8 devices in a mesh: inner: 4 (over z, y, x), data: 2 (over core).
Axes of the slice: x: 2, y: 2, z: 1, core: 2. Of those that a mesh axis runs over, the one named last changes fastest.
Arguments:
- x_t: bfloat16 [8, 576, 192], P(('inner', 'data'))
- labels_t: int32 [8], P(('inner', 'data'))
- x_next: bfloat16 [8, 576, 192], P(('inner', 'data'))
- w_in: float32 [8, 192, 768], replicated
- w_out: float32 [8, 768, 192], replicated
- w_head: float32 [192, 1000], replicated
- mom_in: float32 [8, 192, 768], replicated
- mom_out: float32 [8, 768, 192], replicated
- mom_head: float32 [192, 1000], replicated
- learn_rate: float32 [], replicated
- mom_coef: float32 [], replicated
Outputs:
- output 1: float32 [8, 1000], P(('inner', 'data'))
- output 2: float32 [8, 192, 768], replicated
- output 3: float32 [8, 768, 192], replicated
- output 4: float32 [192, 1000], replicated
- output 5: float32 [8, 192, 768], replicated
- output 6: float32 [8, 768, 192], replicated
- output 7: float32 [192, 1000], replicated
All inputs are finite; a program needn't handle non-finite values.
Results may differ from the reference program's by a relative error of at most 0.0121227.
Values are sent between devices in bfloat16 or wider.
A program may use at most 1 GiB of HBM per device.

```python
import jax
import jax.numpy as jnp
from jax import lax

BATCH_DEV = 1
DEVICES = 8
LAYERS = 8
TOKENS = 576
MODEL_DIM = 192
MLP_DIM = 768
CLASSES = 1000
BATCH_TOTAL = BATCH_DEV * DEVICES
LN_EPS = 1e-6


def layer_norm(stream):
    mean_val = jnp.mean(stream, axis=-1, keepdims=True)
    centered = stream - mean_val
    variance = jnp.mean(centered * centered, axis=-1, keepdims=True)
    return centered * lax.rsqrt(variance + LN_EPS)


def as_bf16(value):
    return value.astype(jnp.bfloat16).astype(jnp.float32)


def forward_logits(tokens, w_in, w_out, w_head):
    def mlp_block(stream, layer_w):
        act_in = as_bf16(layer_norm(stream))
        pre_act = jnp.einsum("bsd,df->bsf", act_in, as_bf16(layer_w[0]))
        hidden = as_bf16(jax.nn.gelu(pre_act, approximate=True))
        return stream + jnp.einsum("bsf,fd->bsd", hidden, as_bf16(layer_w[1])), None

    stream = lax.scan(mlp_block, tokens.astype(jnp.float32), (w_in, w_out))[0]
    pooled = jnp.mean(stream, axis=1).astype(jnp.bfloat16)
    return jnp.dot(pooled, w_head.astype(jnp.bfloat16), preferred_element_type=jnp.float32)


def shard_loss(params, tokens, labels):
    logits = forward_logits(tokens, params[0], params[1], params[2])
    log_norm = jax.nn.logsumexp(logits, axis=-1)
    picked = jnp.take_along_axis(logits, labels[:, None], axis=-1)[:, 0]
    return jnp.sum(log_norm - picked) / BATCH_TOTAL


def setup_inputs(seed: int = 0) -> dict:
    keys = jax.random.split(jax.random.key(seed), 13)
    batch_scale = BATCH_TOTAL ** -0.5

    def images(key_image, key_token):
        image_part = jax.random.normal(key_image, (BATCH_TOTAL, 1, MODEL_DIM), jnp.float32)
        token_part = jax.random.normal(key_token, (BATCH_TOTAL, TOKENS, MODEL_DIM), jnp.float32)
        return ((image_part + token_part) * 0.7071).astype(jnp.bfloat16)

    in_shape = (LAYERS, MODEL_DIM, MLP_DIM)
    out_shape = (LAYERS, MLP_DIM, MODEL_DIM)
    head_shape = (MODEL_DIM, CLASSES)
    return {
        "x_t": images(keys[0], keys[1]),
        "labels_t": jax.random.randint(keys[2], (BATCH_TOTAL,), 0, CLASSES, dtype=jnp.int32),
        "x_next": images(keys[3], keys[4]),
        "w_in": jax.random.normal(keys[5], in_shape, jnp.float32) * MODEL_DIM ** -0.5,
        "w_out": jax.random.normal(keys[6], out_shape, jnp.float32) * MLP_DIM ** -0.5,
        "w_head": jax.random.normal(keys[7], head_shape, jnp.float32) * MODEL_DIM ** -0.5,
        "mom_in": jax.random.normal(keys[8], in_shape, jnp.float32) * (0.5 * MODEL_DIM ** -0.5 * batch_scale),
        "mom_out": jax.random.normal(keys[9], out_shape, jnp.float32) * (0.5 * MLP_DIM ** -0.5 * batch_scale),
        "mom_head": jax.random.normal(keys[10], head_shape, jnp.float32) * (0.5 * MODEL_DIM ** -0.5 * batch_scale),
        "learn_rate": jax.random.uniform(keys[11], (), jnp.float32, 0.4, 0.8) * BATCH_TOTAL ** 0.5,
        "mom_coef": jax.random.uniform(keys[12], (), jnp.float32, 0.6, 0.95),
    }


def reference(x_t, labels_t, x_next, w_in, w_out, w_head, mom_in, mom_out, mom_head, learn_rate, mom_coef):
    params = (w_in, w_out, w_head)
    shard_grad = jax.grad(shard_loss)

    def accumulate(grad_sums, shard):
        local_grads = shard_grad(params, shard[0], shard[1])
        return tuple(running + contrib for running, contrib in zip(grad_sums, local_grads)), None

    zero_sums = tuple(jnp.zeros_like(weight) for weight in params)
    x_shards = x_t.reshape(DEVICES, BATCH_DEV, TOKENS, MODEL_DIM)
    label_shards = labels_t.reshape(DEVICES, BATCH_DEV)
    grad_sums = lax.scan(accumulate, zero_sums, (x_shards, label_shards))[0]
    new_moms = tuple(mom_coef * moment + grad_sum for moment, grad_sum in zip((mom_in, mom_out, mom_head), grad_sums))
    new_weights = tuple(weight - learn_rate * moment for weight, moment in zip(params, new_moms))

    def next_shard(tokens):
        return forward_logits(tokens, new_weights[0], new_weights[1], new_weights[2])

    next_shards = x_next.reshape(DEVICES, BATCH_DEV, TOKENS, MODEL_DIM)
    logits_next = lax.map(next_shard, next_shards).reshape(BATCH_TOTAL, CLASSES)
    return (logits_next, new_weights[0], new_weights[1], new_weights[2], new_moms[0], new_moms[1], new_moms[2])
```

```python
import functools

import jax
import jax.numpy as jnp
from jax import lax
from jax.experimental import pallas as pl
from jax.experimental.pallas import tpu as pltpu
from jax.sharding import PartitionSpec as P

LN_EPS = 1e-6
BATCH_AXES = ("inner", "data")
MESH = pl.DeviceIdType.MESH
LANES = 128
GELU_SCALE = 0.7978845608028654
GELU_CUBIC = 0.044715
F32 = jnp.float32
BF16 = jnp.bfloat16
NT = (((1,), (1,)), ((), ()))
NN = (((1,), (0,)), ((), ()))
TN = (((0,), (0,)), ((), ()))
VMEM_BYTES = 66 * 1000 * 1000


def dot(a, b, dims):
    return lax.dot_general(a, b, dims, preferred_element_type=F32)


def normalize(stream):
    mean_val = jnp.mean(stream, axis=-1, keepdims=True)
    centered = stream - mean_val
    variance = jnp.mean(centered * centered, axis=-1, keepdims=True)
    rstd = lax.rsqrt(variance + LN_EPS)
    return centered * rstd, rstd


def step_kernel(n_shards, rows,
                x_ref, label_ref, w_in_hbm, w_out_hbm, w_head_ref,
                sums_hbm, head_sum_ref,
                stream, d_stream, x_hat, rstds, acts, hidden, d_gelu, d_branch, d_pre,
                w_in_f32, w_out_f32, w_in, w_out,
                grads, recv0, recv1, recv2, sums, head_send, head_recv,
                load_sem, store_sem, send_sem, recv_sem, head_send_sem, head_recv_sem):
    layers, tokens, mlp_dim = hidden.shape
    dim = stream.shape[1]
    classes = w_head_ref.shape[1]
    chunks = mlp_dim // LANES
    weight_rows = chunks * dim
    half = weight_rows
    quarter, eighth = half // 4, half // 8
    inner, core = lax.axis_index("inner"), lax.axis_index("data")
    y, x = inner // 2, inner % 2
    peer_core = (inner, 1 - core)
    peer_x = (inner + 1 - 2 * x, core)
    peer_y = (inner + 2 - 4 * y, core)
    barrier = pltpu.get_barrier_semaphore()
    me = inner * 2 + core
    for step in range(1, n_shards):
        other = (me + step) % n_shards
        pl.semaphore_signal(barrier, inc=1, device_id=(other // 2, other % 2), device_id_type=MESH)

    def load(layer, slot):
        return (pltpu.make_async_copy(w_in_hbm.at[layer], w_in_f32.at[slot], load_sem.at[slot, 0]),
                pltpu.make_async_copy(w_out_hbm.at[layer], w_out_f32.at[slot], load_sem.at[slot, 1]))

    for copy in load(0, 0):
        copy.start()
    stream[...] = x_ref[0].astype(F32).T

    def forward(layer, carry):
        slot = layer % 2

        @pl.when(layer + 1 < layers)
        def _():
            for copy in load(layer + 1, 1 - slot):
                copy.start()

        for copy in load(layer, slot):
            copy.wait()
        w_in[layer] = w_in_f32[slot].astype(BF16)
        w_out[layer] = w_out_f32[slot].astype(BF16)
        for start in range(0, tokens, rows):
            part = slice(start, start + rows)
            stream_in = stream[part]
            normed, rstd = normalize(stream_in)
            act = normed.astype(BF16)
            x_hat[layer, part] = normed
            rstds[layer, part] = rstd
            acts[layer, part] = act
            pre = dot(act, w_in[layer], NN)
            square = pre * pre
            tanh_val = jnp.tanh(pre * (GELU_SCALE + (GELU_SCALE * GELU_CUBIC) * square))
            cdf = 0.5 + 0.5 * tanh_val
            out = (pre * cdf).astype(BF16)
            slope = (0.5 * GELU_SCALE) + (1.5 * GELU_SCALE * GELU_CUBIC) * square
            d_gelu[layer, part] = cdf + (pre * slope) * (1.0 - tanh_val * tanh_val)
            hidden[layer, part] = out
            stream[part] = stream_in + dot(out, w_out[layer], NT)
        return carry

    lax.fori_loop(0, layers, forward, 0)

    pooled = (jnp.sum(stream[...], axis=0, keepdims=True) * (1.0 / tokens)).astype(BF16)
    w_head = w_head_ref[...].astype(BF16)
    pooled_rows = jnp.broadcast_to(pooled.astype(F32), (16, dim)).astype(BF16)
    logits = dot(pooled_rows, w_head, NN)
    peak = jnp.max(logits, axis=-1, keepdims=True)
    expd = jnp.exp(logits - peak)
    probs = expd / jnp.sum(expd, axis=-1, keepdims=True)
    class_ids = lax.broadcasted_iota(jnp.int32, logits.shape, 1)
    targets = jnp.where(class_ids == label_ref[0], 1.0, 0.0)
    d_logits = ((probs - targets) * (1.0 / n_shards)).astype(BF16)
    d_pooled = dot(d_logits, w_head, NT).astype(BF16).astype(F32) / tokens
    d_stream[...] = jnp.broadcast_to(d_pooled[0:1], d_stream.shape)
    head_send[...] = jnp.zeros_like(head_send)
    d_logits = d_logits.astype(F32)
    for chunk in range(8):
        wide = min(LANES, classes - chunk * LANES)
        head_send[chunk:chunk + 1, 0:wide] = d_logits[0:1, chunk * LANES:chunk * LANES + wide]
    pooled = pooled.astype(F32)
    head_send[8:9, :] = pooled[:, 0:LANES]
    head_send[9:10, 0:dim - LANES] = pooled[:, LANES:dim]
    head_recv[0] = head_send[...]

    pl.semaphore_wait(barrier, n_shards - 1)

    def head_copy(step):
        other = (me + step) % n_shards
        return pltpu.make_async_remote_copy(
            src_ref=head_send, dst_ref=head_recv.at[step], send_sem=head_send_sem.at[step],
            recv_sem=head_recv_sem.at[step], device_id=(other // 2, other % 2), device_id_type=MESH)

    for step in range(1, n_shards):
        head_copy(step).start()

    mine = half * core
    place_a, place_b = mine, mine + half // 2

    def remote(src, dst, layer, sem, device):
        return pltpu.make_async_remote_copy(
            src_ref=src, dst_ref=dst, send_sem=send_sem.at[layer, sem], recv_sem=recv_sem.at[layer, sem],
            device_id=device, device_id_type=MESH)

    def copies(stage, layer):
        def grad(start, size):
            return grads.at[layer, pl.ds(start, size)]

        def total(start, size):
            return sums.at[layer, pl.ds(start, size)]

        if stage == 0:
            return [remote(grad(half * (1 - core), half), recv0.at[layer], layer, 0, peer_core)]
        if stage == 1:
            return [remote(grad(place_a + quarter * (1 - x), quarter), recv1.at[layer, 0], layer, 1, peer_x),
                    remote(grad(place_b + quarter * (1 - y), quarter), recv1.at[layer, 1], layer, 2, peer_y)]
        if stage == 2:
            return [remote(grad(place_a + quarter * x + eighth * (1 - y), eighth), recv2.at[layer, 0], layer, 3, peer_y),
                    remote(grad(place_b + quarter * y + eighth * (1 - x), eighth), recv2.at[layer, 1], layer, 4, peer_x)]
        if stage == 3:
            spot_a = total(place_a + quarter * x + eighth * y, eighth)
            spot_b = total(place_b + quarter * y + eighth * x, eighth)
            return [remote(spot_a, spot_a, layer, 5, peer_y), remote(spot_b, spot_b, layer, 6, peer_x)]
        if stage == 4:
            spot_a = total(place_a + quarter * x, quarter)
            spot_b = total(place_b + quarter * y, quarter)
            return [remote(spot_a, spot_a, layer, 7, peer_x), remote(spot_b, spot_b, layer, 8, peer_y)]
        spot = total(mine, half)
        return [remote(spot, spot, layer, 9, peer_core)]

    def add(layer, dst, start, size, other):
        dst[layer, pl.ds(start, size)] = (
            grads[layer, pl.ds(start, size)].astype(F32) + other[...].astype(F32)).astype(BF16)

    def start(stage, layer):
        for copy in copies(stage, layer):
            copy.start()

    def finish(stage, layer):
        for copy in copies(stage, layer):
            copy.wait_recv()
        if stage == 0:
            add(layer, grads, mine, half, recv0.at[layer])
        elif stage == 1:
            add(layer, grads, place_a + quarter * x, quarter, recv1.at[layer, 0])
            add(layer, grads, place_b + quarter * y, quarter, recv1.at[layer, 1])
        elif stage == 2:
            add(layer, sums, place_a + quarter * x + eighth * y, eighth, recv2.at[layer, 0])
            add(layer, sums, place_b + quarter * y + eighth * x, eighth, recv2.at[layer, 1])

    def store(layer):
        return pltpu.make_async_copy(sums.at[layer], sums_hbm.at[layer], store_sem.at[layer])

    last_stage = 5

    def tick(turn):
        for stage in range(last_stage, -1, -1):
            source = turn - 1 - stage

            @pl.when((source >= 0) & (source < layers))
            def _():
                layer = layers - 1 - source
                finish(stage, layer)
                if stage < last_stage:
                    start(stage + 1, layer)
                else:
                    store(layer).start()

    def backward(turn, carry):
        layer = layers - 1 - turn
        for begin in range(0, tokens, rows):
            part = slice(begin, begin + rows)
            branch = d_stream[part].astype(BF16)
            d_branch[part] = branch
            d_hidden = dot(branch, w_out[layer], NN).astype(BF16).astype(F32)
            d_pre_part = (d_hidden * d_gelu[layer, part]).astype(BF16)
            d_pre[part] = d_pre_part
            d_act = dot(d_pre_part, w_in[layer], NT).astype(BF16).astype(F32)
            normed = x_hat[layer, part]
            mean_d = jnp.mean(d_act, axis=-1, keepdims=True)
            mean_dx = jnp.mean(d_act * normed, axis=-1, keepdims=True)
            d_stream[part] = d_stream[part] + rstds[layer, part] * (d_act - mean_d - normed * mean_dx)
        g_in = dot(acts[layer], d_pre[...], TN).astype(BF16)
        g_out = dot(d_branch[...], hidden[layer], TN).astype(BF16)
        for chunk in range(chunks):
            grads[layer, chunk * dim:(chunk + 1) * dim] = g_in[:, chunk * LANES:(chunk + 1) * LANES]
            grads[layer, half + chunk * dim:half + (chunk + 1) * dim] = g_out[:, chunk * LANES:(chunk + 1) * LANES]
        tick(turn)
        start(0, layer)
        return carry

    lax.fori_loop(0, layers, backward, 0)

    for step in range(1, n_shards):
        head_copy(step).wait_recv()
    columns = []
    for device in range(n_shards):
        turned = head_recv[device, 8:16, :].T
        columns.append(jnp.concatenate([turned[:, 0:1], turned[0:dim - LANES, 1:2]], axis=0))
    for chunk in range(8):
        wide = min(LANES, classes - chunk * LANES)
        total_head = None
        for device in range(n_shards):
            product = columns[device] * head_recv[device, chunk:chunk + 1, 0:wide]
            product = product.astype(BF16).astype(F32)
            total_head = product if total_head is None else total_head + product
        head_sum_ref[:, chunk * LANES:chunk * LANES + wide] = total_head

    def drain(turn, carry):
        tick(turn)
        return carry

    lax.fori_loop(layers, layers + last_stage + 1, drain, 0)

    def finish_all(layer, carry):
        for stage in range(last_stage + 1):
            for copy in copies(stage, layer):
                copy.wait_send()
        store(layer).wait()
        return carry

    lax.fori_loop(0, layers, finish_all, 0)
    for step in range(1, n_shards):
        head_copy(step).wait_send()


def update_kernel(rows, x_ref, rate_ref, w_in_ref, m_in_ref, w_out_ref, m_out_ref, sums_ref,
                  w_head_ref, m_head_ref, head_sum_ref,
                  logits_ref, w_in_new, m_in_new, w_out_new, m_out_new, w_head_new, m_head_new,
                  stream, w_in, w_out):
    layer, layers = pl.program_id(0), pl.num_programs(0)
    dim, tokens = x_ref.shape[1:]
    chunks = w_in.shape[1] // LANES
    half = chunks * dim
    rate, coef = rate_ref[0], rate_ref[1]

    @pl.when(layer == 0)
    def _():
        stream[...] = x_ref[0].astype(F32).T

    for chunk in range(chunks):
        columns = slice(chunk * LANES, (chunk + 1) * LANES)
        for base, w_ref, m_ref, w_new, m_new, w_bf in (
                (0, w_in_ref, m_in_ref, w_in_new, m_in_new, w_in),
                (half, w_out_ref, m_out_ref, w_out_new, m_out_new, w_out)):
            grad = sums_ref[0, base + chunk * dim:base + (chunk + 1) * dim].astype(F32)
            moment = coef * m_ref[0, :, columns] + grad
            m_new[0, :, columns] = moment
            weight = w_ref[0, :, columns] - rate * moment
            w_new[0, :, columns] = weight
            w_bf[:, columns] = weight.astype(BF16)

    for start in range(0, tokens, rows):
        part = slice(start, start + rows)
        stream_in = stream[part]
        act = normalize(stream_in)[0].astype(BF16)
        pre = dot(act, w_in[...], NN)
        tanh_val = jnp.tanh(pre * (GELU_SCALE + (GELU_SCALE * GELU_CUBIC) * (pre * pre)))
        out = (pre * (0.5 + 0.5 * tanh_val)).astype(BF16)
        stream[part] = stream_in + dot(out, w_out[...], NT)

    @pl.when(layer == layers - 1)
    def _():
        moment = coef * m_head_ref[...] + head_sum_ref[...]
        m_head_new[...] = moment
        weight = w_head_ref[...] - rate * moment
        w_head_new[...] = weight
        pooled = jnp.sum(stream[...], axis=0, keepdims=True) * (1.0 / tokens)
        pooled = jnp.broadcast_to(pooled, (16, dim)).astype(BF16)
        logits_ref[...] = dot(pooled, weight.astype(BF16), NN)[0:1]


def solution(mesh):
    batch_spec = P(BATCH_AXES)
    repl_spec = P()
    n_shards = mesh.shape["inner"] * mesh.shape["data"]

    def device_step(x_t, labels_t, x_next, w_in, w_out, w_head, mom_in, mom_out, mom_head, learn_rate, mom_coef):
        layers, dim, mlp_dim = w_in.shape
        tokens = x_t.shape[1]
        classes = w_head.shape[1]
        w_out_t = w_out.transpose(0, 2, 1)
        mom_out_t = mom_out.transpose(0, 2, 1)
        weight_rows = mlp_dim // LANES * dim
        vmem = pl.BlockSpec(memory_space=pltpu.VMEM)
        smem = pl.BlockSpec(memory_space=pltpu.SMEM)
        hbm = pl.BlockSpec(memory_space=pl.ANY)
        sums, head_sum = pl.pallas_call(
            functools.partial(step_kernel, n_shards, 192),
            out_shape=(jax.ShapeDtypeStruct((layers, 2 * weight_rows, LANES), BF16),
                       jax.ShapeDtypeStruct((dim, classes), F32)),
            in_specs=[vmem, smem, hbm, hbm, vmem],
            out_specs=(hbm, vmem),
            scratch_shapes=[
                pltpu.VMEM((tokens, dim), F32),
                pltpu.VMEM((tokens, dim), F32),
                pltpu.VMEM((layers, tokens, dim), F32),
                pltpu.VMEM((layers, tokens, 1), F32),
                pltpu.VMEM((layers, tokens, dim), BF16),
                pltpu.VMEM((layers, tokens, mlp_dim), BF16),
                pltpu.VMEM((layers, tokens, mlp_dim), F32),
                pltpu.VMEM((tokens, dim), BF16),
                pltpu.VMEM((tokens, mlp_dim), BF16),
                pltpu.VMEM((2, dim, mlp_dim), F32),
                pltpu.VMEM((2, dim, mlp_dim), F32),
                pltpu.VMEM((layers, dim, mlp_dim), BF16),
                pltpu.VMEM((layers, dim, mlp_dim), BF16),
                pltpu.VMEM((layers, 2 * weight_rows, LANES), BF16),
                pltpu.VMEM((layers, weight_rows, LANES), BF16),
                pltpu.VMEM((layers, 2, weight_rows // 4, LANES), BF16),
                pltpu.VMEM((layers, 2, weight_rows // 8, LANES), BF16),
                pltpu.VMEM((layers, 2 * weight_rows, LANES), BF16),
                pltpu.VMEM((16, LANES), F32),
                pltpu.VMEM((n_shards, 16, LANES), F32),
                pltpu.SemaphoreType.DMA((2, 2)),
                pltpu.SemaphoreType.DMA((layers,)),
                pltpu.SemaphoreType.DMA((layers, 10)),
                pltpu.SemaphoreType.DMA((layers, 10)),
                pltpu.SemaphoreType.DMA((n_shards,)),
                pltpu.SemaphoreType.DMA((n_shards,)),
            ],
            compiler_params=pltpu.CompilerParams(collective_id=0, has_side_effects=True, vmem_limit_bytes=VMEM_BYTES),
            name="step_kernel",
        )(x_t.transpose(0, 2, 1), labels_t, w_in, w_out_t, w_head)

        def per_layer(shape):
            return pl.BlockSpec((1,) + shape, lambda l: (l, 0, 0))

        def whole(shape):
            return pl.BlockSpec(shape, lambda l: (0,) * len(shape))

        weight_block = per_layer((dim, mlp_dim))
        head_block = whole((dim, classes))
        stacked = jax.ShapeDtypeStruct((layers, dim, mlp_dim), F32)
        head_shape = jax.ShapeDtypeStruct((dim, classes), F32)
        rates = jnp.stack([learn_rate, mom_coef])
        logits, w_in_new, m_in_new, w_out_new, m_out_new, w_head_new, m_head_new = pl.pallas_call(
            functools.partial(update_kernel, 192),
            grid=(layers,),
            out_shape=(jax.ShapeDtypeStruct((1, classes), F32), stacked, stacked, stacked, stacked, head_shape, head_shape),
            in_specs=[whole((1, dim, tokens)), smem, weight_block, weight_block, weight_block, weight_block,
                      per_layer((2 * weight_rows, LANES)), head_block, head_block, head_block],
            out_specs=(whole((1, classes)), weight_block, weight_block, weight_block, weight_block, head_block, head_block),
            scratch_shapes=[
                pltpu.VMEM((tokens, dim), F32),
                pltpu.VMEM((dim, mlp_dim), BF16),
                pltpu.VMEM((dim, mlp_dim), BF16),
            ],
            compiler_params=pltpu.CompilerParams(vmem_limit_bytes=VMEM_BYTES),
            name="update_kernel",
        )(x_next.transpose(0, 2, 1), rates, w_in, mom_in, w_out_t, mom_out_t, sums, w_head, mom_head, head_sum)
        return (logits, w_in_new, w_out_new.transpose(0, 2, 1), w_head_new,
                m_in_new, m_out_new.transpose(0, 2, 1), m_head_new)

    return jax.shard_map(device_step, mesh=mesh, in_specs=(batch_spec, batch_spec, batch_spec) + (repl_spec,) * 8, out_specs=(batch_spec,) + (repl_spec,) * 6, check_vma=False)
```

```python
import functools

import jax
import jax.numpy as jnp
from jax import lax
from jax.experimental import pallas as pl
from jax.experimental.pallas import tpu as pltpu
from jax.sharding import PartitionSpec as P

LN_EPS = 1e-6
BATCH_AXES = ("inner", "data")
MESH = pl.DeviceIdType.MESH
LANES = 128
GELU_SCALE = 0.7978845608028654
GELU_CUBIC = 0.044715
F32 = jnp.float32
BF16 = jnp.bfloat16
NT = (((1,), (1,)), ((), ()))
NN = (((1,), (0,)), ((), ()))
TN = (((0,), (0,)), ((), ()))
VMEM_BYTES = 45 * 1000 * 1000
ROWS = 192


def dot(a, b, dims):
    return lax.dot_general(a, b, dims, preferred_element_type=F32)


def normalize(stream):
    mean_val = jnp.mean(stream, axis=-1, keepdims=True)
    centered = stream - mean_val
    variance = jnp.mean(centered * centered, axis=-1, keepdims=True)
    rstd = lax.rsqrt(variance + LN_EPS)
    return centered * rstd, rstd


def gelu_parts(pre):
    inner = GELU_SCALE + (GELU_SCALE * GELU_CUBIC) * (pre * pre)
    return inner, 0.5 + 0.5 * jnp.tanh(pre * inner)


def step_kernel(n_shards,
                x_ref, x_next_ref, label_ref, rate_ref, coef_ref, w_in_hbm, w_out_hbm, w_head_hbm, m_in_hbm, m_out_hbm, m_head_hbm,
                w_in_ref, w_out_ref, w_head_ref, m_in_ref, m_out_ref, m_head_ref, logits_ref,
                stream, d_stream, x_hat, acts, hidden, d_branch, d_pre, w_in, w_out,
                grads, recv0, recv1, recv2, sums, head_send, head_recv,
                load_sem, mom_sem, send_sem, recv_sem, head_send_sem, head_recv_sem):
    layers, tokens, mlp_dim = hidden.shape
    dim = stream.shape[1]
    classes = w_head_ref.shape[1]
    chunks = mlp_dim // LANES
    half = chunks * dim
    quarter, eighth = half // 4, half // 8
    parts = [slice(start, start + ROWS) for start in range(0, tokens, ROWS)]
    inner, core = lax.axis_index("inner"), lax.axis_index("data")
    y, x = inner // 2, inner % 2
    peer_core = (inner, 1 - core)
    peer_x = (inner + 1 - 2 * x, core)
    peer_y = (inner + 2 - 4 * y, core)
    barrier = pltpu.get_barrier_semaphore()
    me = inner * 2 + core

    def load(layer):
        return (pltpu.make_async_copy(w_in_hbm.at[layer], w_in_ref.at[layer], load_sem.at[layer, 0]),
                pltpu.make_async_copy(w_out_hbm.at[layer], w_out_ref.at[layer], load_sem.at[layer, 1]))

    mom_loads = (pltpu.make_async_copy(w_head_hbm, w_head_ref, mom_sem.at[0]),
                 pltpu.make_async_copy(m_head_hbm, m_head_ref, mom_sem.at[1]),
                 pltpu.make_async_copy(m_in_hbm, m_in_ref, mom_sem.at[2]),
                 pltpu.make_async_copy(m_out_hbm, m_out_ref, mom_sem.at[3]))

    for copy in load(0) + load(1):
        copy.start()
    for step in range(1, n_shards):
        other = (me + step) % n_shards
        pl.semaphore_signal(barrier, inc=1, device_id=(other // 2, other % 2), device_id_type=MESH)
    stream[...] = x_ref[0].astype(F32).T

    def forward(layer, carry):
        @pl.when(layer + 2 < layers)
        def _():
            for copy in load(layer + 2):
                copy.start()

        @pl.when(layer == layers - 2)
        def _():
            for copy in mom_loads:
                copy.start()

        for copy in load(layer):
            copy.wait()
        w_in[layer] = w_in_ref[layer].astype(BF16)
        w_out[layer] = w_out_ref[layer].astype(BF16)
        for part in parts:
            stream_in = stream[part]
            normed, rstd = normalize(stream_in)
            x_hat[layer, part, 0:dim] = normed
            x_hat[layer, part, dim:dim + 1] = rstd
            pre = dot(normed.astype(BF16), w_in[layer], NN)
            out = (pre * gelu_parts(pre)[1]).astype(BF16)
            hidden[layer, part] = out
            stream[part] = stream_in + dot(out, w_out[layer], NT)
        return carry

    lax.fori_loop(0, layers, forward, 0)

    pooled = (jnp.sum(stream[...], axis=0, keepdims=True) * (1.0 / tokens)).astype(BF16)
    mom_loads[0].wait()
    w_head = w_head_ref[...].astype(BF16)
    pooled_rows = jnp.broadcast_to(pooled.astype(F32), (16, dim)).astype(BF16)
    logits = dot(pooled_rows, w_head, NN)
    peak = jnp.max(logits, axis=-1, keepdims=True)
    expd = jnp.exp(logits - peak)
    probs = expd / jnp.sum(expd, axis=-1, keepdims=True)
    class_ids = lax.broadcasted_iota(jnp.int32, logits.shape, 1)
    targets = jnp.where(class_ids == label_ref[0], 1.0, 0.0)
    d_logits = ((probs - targets) * (1.0 / n_shards)).astype(BF16)
    d_pooled = dot(d_logits, w_head, NT).astype(BF16).astype(F32) / tokens
    d_stream[...] = jnp.broadcast_to(d_pooled[0:1], d_stream.shape)
    head_send[...] = jnp.zeros_like(head_send)
    d_logits = d_logits.astype(F32)
    for chunk in range(8):
        wide = min(LANES, classes - chunk * LANES)
        head_send[chunk:chunk + 1, 0:wide] = d_logits[0:1, chunk * LANES:chunk * LANES + wide]
    pooled = pooled.astype(F32)
    head_send[8:9, :] = pooled[:, 0:LANES]
    head_send[9:10, 0:dim - LANES] = pooled[:, LANES:dim]
    head_recv[0] = head_send[...]

    pl.semaphore_wait(barrier, n_shards - 1)

    def head_copy(step):
        other = (me + step) % n_shards
        return pltpu.make_async_remote_copy(
            src_ref=head_send, dst_ref=head_recv.at[step], send_sem=head_send_sem.at[step],
            recv_sem=head_recv_sem.at[step], device_id=(other // 2, other % 2), device_id_type=MESH)

    for step in range(1, n_shards):
        head_copy(step).start()

    mine = half * core
    place_a, place_b = mine, mine + half // 2

    def remote(src, dst, layer, sem, device):
        return pltpu.make_async_remote_copy(
            src_ref=src, dst_ref=dst, send_sem=send_sem.at[layer, sem], recv_sem=recv_sem.at[layer, sem],
            device_id=device, device_id_type=MESH)

    def copies(stage, layer):
        def grad(start, size):
            return grads.at[layer, pl.ds(start, size)]

        def total(start, size):
            return sums.at[layer, pl.ds(start, size)]

        if stage == 0:
            return [remote(grad(half * (1 - core), half), recv0.at[layer], layer, 0, peer_core)]
        if stage == 1:
            return [remote(grad(place_a + quarter * (1 - x), quarter), recv1.at[layer, 0], layer, 1, peer_x),
                    remote(grad(place_b + quarter * (1 - y), quarter), recv1.at[layer, 1], layer, 2, peer_y)]
        if stage == 2:
            return [remote(grad(place_a + quarter * x + eighth * (1 - y), eighth), recv2.at[layer, 0], layer, 3, peer_y),
                    remote(grad(place_b + quarter * y + eighth * (1 - x), eighth), recv2.at[layer, 1], layer, 4, peer_x)]
        if stage == 3:
            spot_a = total(place_a + quarter * x + eighth * y, eighth)
            spot_b = total(place_b + quarter * y + eighth * x, eighth)
            return [remote(spot_a, spot_a, layer, 5, peer_y), remote(spot_b, spot_b, layer, 6, peer_x)]
        if stage == 4:
            spot_a = total(place_a + quarter * x, quarter)
            spot_b = total(place_b + quarter * y, quarter)
            return [remote(spot_a, spot_a, layer, 7, peer_x), remote(spot_b, spot_b, layer, 8, peer_y)]
        spot = total(mine, half)
        return [remote(spot, spot, layer, 9, peer_core)]

    def add(layer, dst, start, size, other):
        dst[layer, pl.ds(start, size)] = (
            grads[layer, pl.ds(start, size)].astype(F32) + other[...].astype(F32)).astype(BF16)

    def start(stage, turn):
        for copy in copies(stage, layers - 1 - turn):
            copy.start()

    def advance(stage, turn):
        layer = layers - 1 - turn
        for copy in copies(stage, layer):
            copy.wait_recv()
        if stage == 0:
            add(layer, grads, mine, half, recv0.at[layer])
        elif stage == 1:
            add(layer, grads, place_a + quarter * x, quarter, recv1.at[layer, 0])
            add(layer, grads, place_b + quarter * y, quarter, recv1.at[layer, 1])
        elif stage == 2:
            add(layer, sums, place_a + quarter * x + eighth * y, eighth, recv2.at[layer, 0])
            add(layer, sums, place_b + quarter * y + eighth * x, eighth, recv2.at[layer, 1])
        if stage < 5:
            start(stage + 1, turn)

    def backward(turn, carry):
        layer = layers - 1 - turn
        for part in parts:
            branch = d_stream[part].astype(BF16)
            d_branch[part] = branch
            normed = x_hat[layer, part, 0:dim]
            act = normed.astype(BF16)
            acts[part] = act
            pre = dot(act, w_in[layer], NN)
            inner_val, cdf = gelu_parts(pre)
            slope = cdf + ((cdf - cdf * cdf) * pre) * (6.0 * inner_val - 4.0 * GELU_SCALE)
            d_hidden = dot(branch, w_out[layer], NN).astype(BF16).astype(F32)
            d_pre_part = (d_hidden * slope).astype(BF16)
            d_pre[part] = d_pre_part
            d_act = dot(d_pre_part, w_in[layer], NT).astype(BF16).astype(F32)
            mean_d = jnp.mean(d_act, axis=-1, keepdims=True)
            mean_dx = jnp.mean(d_act * normed, axis=-1, keepdims=True)
            d_stream[part] = d_stream[part] + x_hat[layer, part, dim:dim + 1] * (d_act - mean_d - normed * mean_dx)
        g_in = dot(acts[...], d_pre[...], TN).astype(BF16)
        g_out = dot(d_branch[...], hidden[layer], TN).astype(BF16)
        for chunk in range(chunks):
            grads[layer, chunk * dim:(chunk + 1) * dim] = g_in[:, chunk * LANES:(chunk + 1) * LANES]
            grads[layer, half + chunk * dim:half + (chunk + 1) * dim] = g_out[:, chunk * LANES:(chunk + 1) * LANES]
        start(0, turn)
        pl.when(turn >= 1)(lambda: advance(0, turn - 1))
        pl.when(turn >= 3)(lambda: advance(1, turn - 3))
        return carry

    lax.fori_loop(0, layers, backward, 0)
    last = layers - 1
    advance(0, last)
    advance(1, last - 2)

    rate, coef = rate_ref[0], coef_ref[0]
    for step in range(1, n_shards):
        head_copy(step).wait_recv()
    for copy in mom_loads[1:]:
        copy.wait()
    columns = []
    for device in range(n_shards):
        turned = head_recv[device, 8:16, :].T
        columns.append(jnp.concatenate([turned[:, 0:1], turned[0:dim - LANES, 1:2]], axis=0))
    for chunk in range(8):
        wide = min(LANES, classes - chunk * LANES)
        lanes = slice(chunk * LANES, chunk * LANES + wide)
        total_head = None
        for device in range(n_shards):
            product = columns[device] * head_recv[device, chunk:chunk + 1, 0:wide]
            product = product.astype(BF16).astype(F32)
            total_head = product if total_head is None else total_head + product
        moment = coef * m_head_ref[:, lanes] + total_head
        m_head_ref[:, lanes] = moment
        w_head_ref[:, lanes] = w_head_ref[:, lanes] - rate * moment
    stream[...] = x_next_ref[0].astype(F32).T

    for stage, turn in ((2, 0), (2, 1), (1, last - 1), (2, 2), (2, 3), (1, last), (2, 4), (2, 5), (2, last - 1),
                        (3, 0), (2, last), (3, 1), (3, last), (3, last - 1), (3, 5), (3, 4), (3, 3), (3, 2), (4, last)):
        advance(stage, turn)

    def next_forward(layer, carry):
        advance(5, last - layer)
        for chunk in range(chunks):
            lanes = slice(chunk * LANES, (chunk + 1) * LANES)
            for base, w_ref, m_ref, w_bf in ((0, w_in_ref, m_in_ref, w_in), (half, w_out_ref, m_out_ref, w_out)):
                grad = sums[layer, base + chunk * dim:base + (chunk + 1) * dim].astype(F32)
                moment = coef * m_ref[layer, :, lanes] + grad
                m_ref[layer, :, lanes] = moment
                weight = w_ref[layer, :, lanes] - rate * moment
                w_ref[layer, :, lanes] = weight
                w_bf[layer, :, lanes] = weight.astype(BF16)
        pl.when(layer < last)(lambda: advance(4, last - 1 - layer))
        for part in parts:
            stream_in = stream[part]
            pre = dot(normalize(stream_in)[0].astype(BF16), w_in[layer], NN)
            out = (pre * gelu_parts(pre)[1]).astype(BF16)
            stream[part] = stream_in + dot(out, w_out[layer], NT)
        return carry

    lax.fori_loop(0, layers, next_forward, 0)
    pooled = jnp.sum(stream[...], axis=0, keepdims=True) * (1.0 / tokens)
    pooled = jnp.broadcast_to(pooled, (16, dim)).astype(BF16)
    logits_ref[...] = dot(pooled, w_head_ref[...].astype(BF16), NN)[0:1]

    def finish_all(layer, carry):
        for stage in range(6):
            for copy in copies(stage, layer):
                copy.wait_send()
        return carry

    lax.fori_loop(0, layers, finish_all, 0)
    for step in range(1, n_shards):
        head_copy(step).wait_send()


def store_kernel(*refs):
    count = (len(refs) - 1) // 2
    copies = [pltpu.make_async_copy(refs[i], refs[count + i], refs[-1].at[i]) for i in range(count)]
    for copy in copies:
        copy.start()
    for copy in copies:
        copy.wait()


def solution(mesh):
    batch_spec = P(BATCH_AXES)
    repl_spec = P()
    n_shards = mesh.shape["inner"] * mesh.shape["data"]

    def device_step(x_t, labels_t, x_next, w_in, w_out, w_head, mom_in, mom_out, mom_head, learn_rate, mom_coef):
        layers, dim, mlp_dim = w_in.shape
        tokens = x_t.shape[1]
        classes = w_head.shape[1]
        half = mlp_dim // LANES * dim
        vmem = pl.BlockSpec(memory_space=pltpu.VMEM)
        smem = pl.BlockSpec(memory_space=pltpu.SMEM)
        hbm = pl.BlockSpec(memory_space=pl.ANY)
        shapes = [(layers, dim, mlp_dim), (layers, dim, mlp_dim), (dim, classes)] * 2 + [(1, classes)]
        results = pl.pallas_call(
            functools.partial(step_kernel, n_shards),
            out_shape=tuple(pltpu.VMEM(shape, F32) for shape in shapes),
            in_specs=[vmem, vmem, smem, smem, smem] + [hbm] * 6,
            out_specs=(vmem,) * 7,
            scratch_shapes=[
                pltpu.VMEM((tokens, dim), F32),
                pltpu.VMEM((tokens, dim), F32),
                pltpu.VMEM((layers, tokens, dim + 1), F32),
                pltpu.VMEM((tokens, dim), BF16),
                pltpu.VMEM((layers, tokens, mlp_dim), BF16),
                pltpu.VMEM((tokens, dim), BF16),
                pltpu.VMEM((tokens, mlp_dim), BF16),
                pltpu.VMEM((layers, dim, mlp_dim), BF16),
                pltpu.VMEM((layers, dim, mlp_dim), BF16),
                pltpu.VMEM((layers, 2 * half, LANES), BF16),
                pltpu.VMEM((layers, half, LANES), BF16),
                pltpu.VMEM((layers, 2, half // 4, LANES), BF16),
                pltpu.VMEM((layers, 2, half // 8, LANES), BF16),
                pltpu.VMEM((layers, 2 * half, LANES), BF16),
                pltpu.VMEM((16, LANES), F32),
                pltpu.VMEM((n_shards, 16, LANES), F32),
                pltpu.SemaphoreType.DMA((layers, 2)),
                pltpu.SemaphoreType.DMA((4,)),
                pltpu.SemaphoreType.DMA((layers, 10)),
                pltpu.SemaphoreType.DMA((layers, 10)),
                pltpu.SemaphoreType.DMA((n_shards,)),
                pltpu.SemaphoreType.DMA((n_shards,)),
            ],
            compiler_params=pltpu.CompilerParams(collective_id=0, has_side_effects=True, vmem_limit_bytes=VMEM_BYTES),
            name="step_kernel",
        )(x_t.transpose(0, 2, 1), x_next.transpose(0, 2, 1), labels_t, learn_rate.reshape(1), mom_coef.reshape(1),
          w_in, w_out.transpose(0, 2, 1), w_head, mom_in, mom_out.transpose(0, 2, 1), mom_head)
        stored = pl.pallas_call(
            store_kernel,
            out_shape=tuple(jax.ShapeDtypeStruct(shape, F32) for shape in shapes),
            in_specs=[vmem] * 7,
            out_specs=(hbm,) * 7,
            scratch_shapes=[pltpu.SemaphoreType.DMA((7,))],
            compiler_params=pltpu.CompilerParams(vmem_limit_bytes=1000 * 1000),
            name="store_kernel",
        )(*results)
        w_in_new, w_out_new, w_head_new, m_in_new, m_out_new, m_head_new, logits = stored
        return (logits, w_in_new, w_out_new.transpose(0, 2, 1), w_head_new,
                m_in_new, m_out_new.transpose(0, 2, 1), m_head_new)

    return jax.shard_map(device_step, mesh=mesh, in_specs=(batch_spec, batch_spec, batch_spec) + (repl_spec,) * 8, out_specs=(batch_spec,) + (repl_spec,) * 6, check_vma=False)
```

```python
import functools

import jax
import jax.numpy as jnp
from jax import lax
from jax.experimental import pallas as pl
from jax.experimental.pallas import tpu as pltpu
from jax.sharding import PartitionSpec as P

LN_EPS = 1e-6
BATCH_AXES = ("inner", "data")
MESH = pl.DeviceIdType.MESH
LANES = 128
GELU_SCALE = 0.7978845608028654
GELU_CUBIC = 0.044715
F32 = jnp.float32
BF16 = jnp.bfloat16
NT = (((1,), (1,)), ((), ()))
NN = (((1,), (0,)), ((), ()))
TN = (((0,), (0,)), ((), ()))
VMEM_BYTES = 46 * 1000 * 1000
ROWS = 192


def dot(a, b, dims):
    return lax.dot_general(a, b, dims, preferred_element_type=F32)


def normalize(stream):
    mean_val = jnp.mean(stream, axis=-1, keepdims=True)
    centered = stream - mean_val
    variance = jnp.mean(centered * centered, axis=-1, keepdims=True)
    rstd = lax.rsqrt(variance + LN_EPS)
    return centered * rstd, rstd


def gelu_parts(pre):
    inner = GELU_SCALE + (GELU_SCALE * GELU_CUBIC) * (pre * pre)
    return inner, 0.5 + 0.5 * jnp.tanh(pre * inner)


AFTER_BACKWARD = [[], [(0, 0)], [(0, 1)], [(0, 2)], [(1, 0), (0, 3)], [(1, 1), (0, 4)], [(0, 5)], []]
BEFORE_HEAD = [(0, 6), (0, 7), (2, 1), (1, 5), (1, 4), (1, 6), (2, 0), (1, 7), (1, 3), (1, 2), (2, 5), (2, 6), (2, 7), (2, 4), (2, 3), (2, 2), (3, 5), (3, 7), (3, 6)]
AFTER_HEAD = [(4, 5), (3, 4), (5, 5), (3, 3), (3, 2), (4, 7), (4, 6), (5, 7)]
BEFORE_UPDATE = [[], [(5, 6)], [], [(5, 4), (4, 3)], [(4, 2), (5, 3)], [(5, 2), (4, 1)], [(4, 0), (5, 1)], [(5, 0)]]
AFTER_UPDATE = [[(3, 1), (3, 0)], [(4, 4)], [], [], [], [], [], []]


def step_kernel(n_shards,
                x_ref, x_next_ref, label_ref, rate_ref, coef_ref, w_in_hbm, w_out_hbm, w_head_hbm, m_in_hbm, m_out_hbm, m_head_hbm,
                w_in_ref, w_out_ref, w_head_ref, m_in_ref, m_out_ref, m_head_ref, logits_ref,
                stream, d_stream, x_hat, acts, pre_acts, hidden, d_branch, d_pre, w_in, w_out,
                grads, recv0, recv1, recv2, sums, head_send, head_recv,
                load_sem, mom_sem, send_sem, recv_sem, head_send_sem, head_recv_sem):
    layers, tokens, mlp_dim = pre_acts.shape
    dim = stream.shape[1]
    classes = w_head_ref.shape[1]
    chunks = mlp_dim // LANES
    half = chunks * dim
    quarter, eighth = half // 4, half // 8
    parts = [slice(start, start + ROWS) for start in range(0, tokens, ROWS)]
    inner, core = lax.axis_index("inner"), lax.axis_index("data")
    y, x = inner // 2, inner % 2
    peer_core = (inner, 1 - core)
    peer_x = (inner + 1 - 2 * x, core)
    peer_y = (inner + 2 - 4 * y, core)
    barrier = pltpu.get_barrier_semaphore()
    me = inner * 2 + core

    def load(layer):
        return (pltpu.make_async_copy(w_in_hbm.at[layer], w_in_ref.at[layer], load_sem.at[layer, 0]),
                pltpu.make_async_copy(w_out_hbm.at[layer], w_out_ref.at[layer], load_sem.at[layer, 1]))

    mom_loads = (pltpu.make_async_copy(w_head_hbm, w_head_ref, mom_sem.at[0]),
                 pltpu.make_async_copy(m_head_hbm, m_head_ref, mom_sem.at[1]),
                 pltpu.make_async_copy(m_in_hbm, m_in_ref, mom_sem.at[2]),
                 pltpu.make_async_copy(m_out_hbm, m_out_ref, mom_sem.at[3]))

    for copy in load(0) + load(1):
        copy.start()
    for step in range(1, n_shards):
        other = (me + step) % n_shards
        pl.semaphore_signal(barrier, inc=1, device_id=(other // 2, other % 2), device_id_type=MESH)
    stream[...] = x_ref[0].astype(F32).T

    def forward(layer, carry):
        @pl.when(layer + 2 < layers)
        def _():
            for copy in load(layer + 2):
                copy.start()

        @pl.when(layer == layers - 2)
        def _():
            for copy in mom_loads:
                copy.start()

        for copy in load(layer):
            copy.wait()
        w_in[layer] = w_in_ref[layer].astype(BF16)
        w_out[layer] = w_out_ref[layer].astype(BF16)
        for part in parts:
            stream_in = stream[part]
            normed, rstd = normalize(stream_in)
            x_hat[layer, part, 0:dim] = normed
            x_hat[layer, part, dim:dim + 1] = rstd
            pre = dot(normed.astype(BF16), w_in[layer], NN)
            pre_acts[layer, part] = pre
            out = (pre * gelu_parts(pre)[1]).astype(BF16)
            stream[part] = stream_in + dot(out, w_out[layer], NT)
        return carry

    lax.fori_loop(0, layers, forward, 0)

    pooled = (jnp.sum(stream[...], axis=0, keepdims=True) * (1.0 / tokens)).astype(BF16)
    mom_loads[0].wait()
    w_head = w_head_ref[...].astype(BF16)
    pooled_rows = jnp.broadcast_to(pooled.astype(F32), (16, dim)).astype(BF16)
    logits = dot(pooled_rows, w_head, NN)
    peak = jnp.max(logits, axis=-1, keepdims=True)
    expd = jnp.exp(logits - peak)
    probs = expd / jnp.sum(expd, axis=-1, keepdims=True)
    class_ids = lax.broadcasted_iota(jnp.int32, logits.shape, 1)
    targets = jnp.where(class_ids == label_ref[0], 1.0, 0.0)
    d_logits = ((probs - targets) * (1.0 / n_shards)).astype(BF16)
    d_pooled = dot(d_logits, w_head, NT).astype(BF16).astype(F32) / tokens
    d_stream[...] = jnp.broadcast_to(d_pooled[0:1], d_stream.shape)
    head_send[...] = jnp.zeros_like(head_send)
    d_logits = d_logits.astype(F32)
    for chunk in range(8):
        wide = min(LANES, classes - chunk * LANES)
        head_send[chunk:chunk + 1, 0:wide] = d_logits[0:1, chunk * LANES:chunk * LANES + wide]
    pooled = pooled.astype(F32)
    head_send[8:9, :] = pooled[:, 0:LANES]
    head_send[9:10, 0:dim - LANES] = pooled[:, LANES:dim]
    head_recv[0] = head_send[...]

    pl.semaphore_wait(barrier, n_shards - 1)

    def head_copy(step):
        other = (me + step) % n_shards
        return pltpu.make_async_remote_copy(
            src_ref=head_send, dst_ref=head_recv.at[step], send_sem=head_send_sem.at[step],
            recv_sem=head_recv_sem.at[step], device_id=(other // 2, other % 2), device_id_type=MESH)

    for step in range(1, n_shards):
        head_copy(step).start()

    mine = half * core
    place_a, place_b = mine, mine + half // 2

    def remote(src, dst, layer, sem, device):
        return pltpu.make_async_remote_copy(
            src_ref=src, dst_ref=dst, send_sem=send_sem.at[layer, sem], recv_sem=recv_sem.at[layer, sem],
            device_id=device, device_id_type=MESH)

    def copies(stage, layer):
        def grad(start, size):
            return grads.at[layer, pl.ds(start, size)]

        def total(start, size):
            return sums.at[layer, pl.ds(start, size)]

        if stage == 0:
            return [remote(grad(half * (1 - core), half), recv0.at[layer], layer, 0, peer_core)]
        if stage == 1:
            return [remote(grad(place_a + quarter * (1 - x), quarter), recv1.at[layer, 0], layer, 1, peer_x),
                    remote(grad(place_b + quarter * (1 - y), quarter), recv1.at[layer, 1], layer, 2, peer_y)]
        if stage == 2:
            return [remote(grad(place_a + quarter * x + eighth * (1 - y), eighth), recv2.at[layer, 0], layer, 3, peer_y),
                    remote(grad(place_b + quarter * y + eighth * (1 - x), eighth), recv2.at[layer, 1], layer, 4, peer_x)]
        if stage == 3:
            spot_a = total(place_a + quarter * x + eighth * y, eighth)
            spot_b = total(place_b + quarter * y + eighth * x, eighth)
            return [remote(spot_a, spot_a, layer, 5, peer_y), remote(spot_b, spot_b, layer, 6, peer_x)]
        if stage == 4:
            spot_a = total(place_a + quarter * x, quarter)
            spot_b = total(place_b + quarter * y, quarter)
            return [remote(spot_a, spot_a, layer, 7, peer_x), remote(spot_b, spot_b, layer, 8, peer_y)]
        spot = total(mine, half)
        return [remote(spot, spot, layer, 9, peer_core)]

    def add(layer, dst, start, size, other):
        dst[layer, pl.ds(start, size)] = (
            grads[layer, pl.ds(start, size)].astype(F32) + other[...].astype(F32)).astype(BF16)

    def start(stage, turn):
        for copy in copies(stage, layers - 1 - turn):
            copy.start()

    def advance(stage, turn):
        layer = layers - 1 - turn
        for copy in copies(stage, layer):
            copy.wait_recv()
        if stage == 0:
            add(layer, grads, mine, half, recv0.at[layer])
        elif stage == 1:
            add(layer, grads, place_a + quarter * x, quarter, recv1.at[layer, 0])
            add(layer, grads, place_b + quarter * y, quarter, recv1.at[layer, 1])
        elif stage == 2:
            add(layer, sums, place_a + quarter * x + eighth * y, eighth, recv2.at[layer, 0])
            add(layer, sums, place_b + quarter * y + eighth * x, eighth, recv2.at[layer, 1])
        if stage < 5:
            start(stage + 1, turn)

    def run(steps):
        for step in steps:
            advance(*step)

    def run_at(index, table):
        for at, steps in enumerate(table):
            if steps:
                pl.when(index == at)(functools.partial(run, steps))

    def backward(turn, carry):
        layer = layers - 1 - turn
        for part in parts:
            branch = d_stream[part].astype(BF16)
            d_branch[part] = branch
            normed = x_hat[layer, part, 0:dim]
            acts[part] = normed.astype(BF16)
            pre = pre_acts[layer, part]
            inner_val, cdf = gelu_parts(pre)
            hidden[part] = (pre * cdf).astype(BF16)
            slope = cdf + ((cdf - cdf * cdf) * pre) * (6.0 * inner_val - 4.0 * GELU_SCALE)
            d_hidden = dot(branch, w_out[layer], NN).astype(BF16).astype(F32)
            d_pre_part = (d_hidden * slope).astype(BF16)
            d_pre[part] = d_pre_part
            d_act = dot(d_pre_part, w_in[layer], NT).astype(BF16).astype(F32)
            mean_d = jnp.mean(d_act, axis=-1, keepdims=True)
            mean_dx = jnp.mean(d_act * normed, axis=-1, keepdims=True)
            d_stream[part] = d_stream[part] + x_hat[layer, part, dim:dim + 1] * (d_act - mean_d - normed * mean_dx)
        g_in = dot(acts[...], d_pre[...], TN).astype(BF16)
        g_out = dot(d_branch[...], hidden[...], TN).astype(BF16)
        for chunk in range(chunks):
            grads[layer, chunk * dim:(chunk + 1) * dim] = g_in[:, chunk * LANES:(chunk + 1) * LANES]
            grads[layer, half + chunk * dim:half + (chunk + 1) * dim] = g_out[:, chunk * LANES:(chunk + 1) * LANES]
        start(0, turn)
        run_at(turn, AFTER_BACKWARD)
        return carry

    lax.fori_loop(0, layers, backward, 0)
    last = layers - 1
    run(BEFORE_HEAD)

    rate, coef = rate_ref[0], coef_ref[0]
    for step in range(1, n_shards):
        head_copy(step).wait_recv()
    for copy in mom_loads[1:]:
        copy.wait()
    columns = []
    for device in range(n_shards):
        turned = head_recv[device, 8:16, :].T
        columns.append(jnp.concatenate([turned[:, 0:1], turned[0:dim - LANES, 1:2]], axis=0))
    for chunk in range(8):
        wide = min(LANES, classes - chunk * LANES)
        lanes = slice(chunk * LANES, chunk * LANES + wide)
        total_head = None
        for device in range(n_shards):
            product = columns[device] * head_recv[device, chunk:chunk + 1, 0:wide]
            product = product.astype(BF16).astype(F32)
            total_head = product if total_head is None else total_head + product
        moment = coef * m_head_ref[:, lanes] + total_head
        m_head_ref[:, lanes] = moment
        w_head_ref[:, lanes] = w_head_ref[:, lanes] - rate * moment
    stream[...] = x_next_ref[0].astype(F32).T

    run(AFTER_HEAD)

    def next_forward(layer, carry):
        run_at(layer, BEFORE_UPDATE)
        for chunk in range(chunks):
            lanes = slice(chunk * LANES, (chunk + 1) * LANES)
            for base, w_ref, m_ref, w_bf in ((0, w_in_ref, m_in_ref, w_in), (half, w_out_ref, m_out_ref, w_out)):
                grad = sums[layer, base + chunk * dim:base + (chunk + 1) * dim].astype(F32)
                moment = coef * m_ref[layer, :, lanes] + grad
                m_ref[layer, :, lanes] = moment
                weight = w_ref[layer, :, lanes] - rate * moment
                w_ref[layer, :, lanes] = weight
                w_bf[layer, :, lanes] = weight.astype(BF16)
        run_at(layer, AFTER_UPDATE)
        for part in parts:
            stream_in = stream[part]
            pre = dot(normalize(stream_in)[0].astype(BF16), w_in[layer], NN)
            out = (pre * gelu_parts(pre)[1]).astype(BF16)
            stream[part] = stream_in + dot(out, w_out[layer], NT)
        return carry

    lax.fori_loop(0, layers, next_forward, 0)
    pooled = jnp.sum(stream[...], axis=0, keepdims=True) * (1.0 / tokens)
    pooled = jnp.broadcast_to(pooled, (16, dim)).astype(BF16)
    logits_ref[...] = dot(pooled, w_head_ref[...].astype(BF16), NN)[0:1]

    def finish_all(layer, carry):
        for stage in range(6):
            for copy in copies(stage, layer):
                copy.wait_send()
        return carry

    lax.fori_loop(0, layers, finish_all, 0)
    for step in range(1, n_shards):
        head_copy(step).wait_send()


def store_kernel(*refs):
    count = (len(refs) - 1) // 2
    copies = [pltpu.make_async_copy(refs[i], refs[count + i], refs[-1].at[i]) for i in range(count)]
    for copy in copies:
        copy.start()
    for copy in copies:
        copy.wait()


def solution(mesh):
    batch_spec = P(BATCH_AXES)
    repl_spec = P()
    n_shards = mesh.shape["inner"] * mesh.shape["data"]

    def device_step(x_t, labels_t, x_next, w_in, w_out, w_head, mom_in, mom_out, mom_head, learn_rate, mom_coef):
        layers, dim, mlp_dim = w_in.shape
        tokens = x_t.shape[1]
        classes = w_head.shape[1]
        half = mlp_dim // LANES * dim
        vmem = pl.BlockSpec(memory_space=pltpu.VMEM)
        smem = pl.BlockSpec(memory_space=pltpu.SMEM)
        hbm = pl.BlockSpec(memory_space=pl.ANY)
        shapes = [(layers, dim, mlp_dim), (layers, dim, mlp_dim), (dim, classes)] * 2 + [(1, classes)]
        results = pl.pallas_call(
            functools.partial(step_kernel, n_shards),
            out_shape=tuple(pltpu.VMEM(shape, F32) for shape in shapes),
            in_specs=[vmem, vmem, smem, smem, smem] + [hbm] * 6,
            out_specs=(vmem,) * 7,
            scratch_shapes=[
                pltpu.VMEM((tokens, dim), F32),
                pltpu.VMEM((tokens, dim), F32),
                pltpu.VMEM((layers, tokens, dim + 1), F32),
                pltpu.VMEM((tokens, dim), BF16),
                pltpu.VMEM((layers, tokens, mlp_dim), F32),
                pltpu.VMEM((tokens, mlp_dim), BF16),
                pltpu.VMEM((tokens, dim), BF16),
                pltpu.VMEM((tokens, mlp_dim), BF16),
                pltpu.VMEM((layers, dim, mlp_dim), BF16),
                pltpu.VMEM((layers, dim, mlp_dim), BF16),
                pltpu.VMEM((layers, 2 * half, LANES), BF16),
                pltpu.VMEM((layers, half, LANES), BF16),
                pltpu.VMEM((layers, 2, half // 4, LANES), BF16),
                pltpu.VMEM((layers, 2, half // 8, LANES), BF16),
                pltpu.VMEM((layers, 2 * half, LANES), BF16),
                pltpu.VMEM((16, LANES), F32),
                pltpu.VMEM((n_shards, 16, LANES), F32),
                pltpu.SemaphoreType.DMA((layers, 2)),
                pltpu.SemaphoreType.DMA((4,)),
                pltpu.SemaphoreType.DMA((layers, 10)),
                pltpu.SemaphoreType.DMA((layers, 10)),
                pltpu.SemaphoreType.DMA((n_shards,)),
                pltpu.SemaphoreType.DMA((n_shards,)),
            ],
            compiler_params=pltpu.CompilerParams(collective_id=0, has_side_effects=True, vmem_limit_bytes=VMEM_BYTES),
            name="step_kernel",
        )(x_t.transpose(0, 2, 1), x_next.transpose(0, 2, 1), labels_t, learn_rate.reshape(1), mom_coef.reshape(1),
          w_in, w_out.transpose(0, 2, 1), w_head, mom_in, mom_out.transpose(0, 2, 1), mom_head)
        stored = pl.pallas_call(
            store_kernel,
            out_shape=tuple(jax.ShapeDtypeStruct(shape, F32) for shape in shapes),
            in_specs=[vmem] * 7,
            out_specs=(hbm,) * 7,
            scratch_shapes=[pltpu.SemaphoreType.DMA((7,))],
            compiler_params=pltpu.CompilerParams(vmem_limit_bytes=1000 * 1000),
            name="store_kernel",
        )(*results)
        w_in_new, w_out_new, w_head_new, m_in_new, m_out_new, m_head_new, logits = stored
        return (logits, w_in_new, w_out_new.transpose(0, 2, 1), w_head_new,
                m_in_new, m_out_new.transpose(0, 2, 1), m_head_new)

    return jax.shard_map(device_step, mesh=mesh, in_specs=(batch_spec, batch_spec, batch_spec) + (repl_spec,) * 8, out_specs=(batch_spec,) + (repl_spec,) * 6, check_vma=False)
```

```python
import functools

import jax
import jax.numpy as jnp
from jax import lax
from jax.experimental import pallas as pl
from jax.experimental.pallas import tpu as pltpu
from jax.sharding import PartitionSpec as P

LN_EPS = 1e-6
BATCH_AXES = ("inner", "data")
MESH = pl.DeviceIdType.MESH
LANES = 128
GELU_SCALE = 0.7978845608028654
GELU_CUBIC = 0.044715
F32 = jnp.float32
BF16 = jnp.bfloat16
NT = (((1,), (1,)), ((), ()))
NN = (((1,), (0,)), ((), ()))
TN = (((0,), (0,)), ((), ()))
VMEM_BYTES = 46 * 1000 * 1000
ROWS = 192


def dot(a, b, dims):
    return lax.dot_general(a, b, dims, preferred_element_type=F32)


def normalize(stream):
    mean_val = jnp.mean(stream, axis=-1, keepdims=True)
    centered = stream - mean_val
    variance = jnp.mean(centered * centered, axis=-1, keepdims=True)
    rstd = lax.rsqrt(variance + LN_EPS)
    return centered * rstd, rstd


def gelu_parts(pre):
    inner = GELU_SCALE + (GELU_SCALE * GELU_CUBIC) * (pre * pre)
    return inner, 0.5 + 0.5 * jnp.tanh(pre * inner)


AFTER_BACKWARD = [[], [(0, 0)], [(0, 1)], [(0, 2)], [(1, 0), (0, 3)], [(1, 1), (0, 4)], [(0, 5)], []]
BEFORE_HEAD = [(0, 6), (0, 7), (2, 1), (1, 5), (1, 4), (1, 6), (2, 0), (1, 7), (1, 3), (1, 2), (2, 5), (2, 6), (2, 7), (2, 4), (2, 3), (2, 2), (3, 5), (3, 7), (3, 6)]
AFTER_HEAD = [(4, 5), (3, 4), (5, 5), (3, 3), (3, 2), (4, 7), (4, 6), (5, 7)]
BEFORE_UPDATE = [[], [(5, 6)], [], [(5, 4), (4, 3)], [(4, 2), (5, 3)], [(5, 2), (4, 1)], [(4, 0), (5, 1)], [(5, 0)]]
AFTER_UPDATE = [[(3, 1), (3, 0)], [(4, 4)], [], [], [], [], [], []]


def step_kernel(n_shards,
                x_ref, x_next_ref, label_ref, rate_ref, coef_ref, w_in_hbm, w_out_hbm, w_head_hbm, m_in_hbm, m_out_hbm, m_head_hbm,
                w_in_ref, w_out_ref, w_head_ref, m_in_ref, m_out_ref, m_head_ref, logits_ref,
                stream, d_stream, x_hat, acts, pre_acts, hidden, d_branch, d_pre, w_in, w_out,
                grads, recv0, recv1, recv2, sums, head_send, head_recv,
                load_sem, mom_sem, send_sem, recv_sem, head_send_sem, head_recv_sem):
    layers, tokens, mlp_dim = pre_acts.shape
    dim = stream.shape[1]
    classes = w_head_ref.shape[1]
    chunks = mlp_dim // LANES
    half = chunks * dim
    quarter, eighth = half // 4, half // 8
    parts = [slice(start, start + ROWS) for start in range(0, tokens, ROWS)]
    inner, core = lax.axis_index("inner"), lax.axis_index("data")
    y, x = inner // 2, inner % 2
    peer_core = (inner, 1 - core)
    peer_x = (inner + 1 - 2 * x, core)
    peer_y = (inner + 2 - 4 * y, core)
    barrier = pltpu.get_barrier_semaphore()
    me = inner * 2 + core

    def load(layer):
        return (pltpu.make_async_copy(w_in_hbm.at[layer], w_in_ref.at[layer], load_sem.at[layer, 0]),
                pltpu.make_async_copy(w_out_hbm.at[layer], w_out_ref.at[layer], load_sem.at[layer, 1]))

    mom_loads = (pltpu.make_async_copy(w_head_hbm, w_head_ref, mom_sem.at[0]),
                 pltpu.make_async_copy(m_head_hbm, m_head_ref, mom_sem.at[1]),
                 pltpu.make_async_copy(m_in_hbm, m_in_ref, mom_sem.at[2]),
                 pltpu.make_async_copy(m_out_hbm, m_out_ref, mom_sem.at[3]))

    for copy in load(0) + load(1):
        copy.start()
    for step in range(1, n_shards):
        other = (me + step) % n_shards
        pl.semaphore_signal(barrier, inc=1, device_id=(other // 2, other % 2), device_id_type=MESH)
    stream[...] = x_ref[0].astype(F32).T

    def forward(layer, carry):
        @pl.when(layer + 2 < layers)
        def _():
            for copy in load(layer + 2):
                copy.start()

        @pl.when(layer == layers - 2)
        def _():
            for copy in mom_loads:
                copy.start()

        for copy in load(layer):
            copy.wait()
        w_in[layer] = w_in_ref[layer].astype(BF16)
        w_out[layer] = w_out_ref[layer].astype(BF16)
        for part in parts:
            stream_in = stream[part]
            normed, rstd = normalize(stream_in)
            x_hat[layer, part, 0:dim] = normed
            x_hat[layer, part, dim:dim + 1] = rstd
            pre = dot(normed.astype(BF16), w_in[layer], NN)
            pre_acts[layer, part] = pre
            out = (pre * gelu_parts(pre)[1]).astype(BF16)
            stream[part] = stream_in + dot(out, w_out[layer], NT)
        return carry

    lax.fori_loop(0, layers, forward, 0)

    pooled = (jnp.sum(stream[...], axis=0, keepdims=True) * (1.0 / tokens)).astype(BF16)
    mom_loads[0].wait()
    w_head = w_head_ref[...].astype(BF16)
    pooled_rows = jnp.broadcast_to(pooled.astype(F32), (16, dim)).astype(BF16)
    logits = dot(pooled_rows, w_head, NN)
    peak = jnp.max(logits, axis=-1, keepdims=True)
    expd = jnp.exp(logits - peak)
    probs = expd / jnp.sum(expd, axis=-1, keepdims=True)
    class_ids = lax.broadcasted_iota(jnp.int32, logits.shape, 1)
    targets = jnp.where(class_ids == label_ref[...], 1.0, 0.0)
    d_logits = ((probs - targets) * (1.0 / n_shards)).astype(BF16)
    d_pooled = dot(d_logits, w_head, NT).astype(BF16).astype(F32) / tokens
    d_stream[...] = jnp.broadcast_to(d_pooled[0:1], d_stream.shape)
    head_send[...] = jnp.zeros_like(head_send)
    d_logits = d_logits.astype(F32)
    for chunk in range(8):
        wide = min(LANES, classes - chunk * LANES)
        head_send[chunk:chunk + 1, 0:wide] = d_logits[0:1, chunk * LANES:chunk * LANES + wide]
    pooled = pooled.astype(F32)
    head_send[8:9, :] = pooled[:, 0:LANES]
    head_send[9:10, 0:dim - LANES] = pooled[:, LANES:dim]
    head_recv[0] = head_send[...]

    pl.semaphore_wait(barrier, n_shards - 1)

    def head_copy(step):
        other = (me + step) % n_shards
        return pltpu.make_async_remote_copy(
            src_ref=head_send, dst_ref=head_recv.at[step], send_sem=head_send_sem.at[step],
            recv_sem=head_recv_sem.at[step], device_id=(other // 2, other % 2), device_id_type=MESH)

    for step in range(1, n_shards):
        head_copy(step).start()

    mine = half * core
    place_a, place_b = mine, mine + half // 2

    def remote(src, dst, layer, sem, device):
        return pltpu.make_async_remote_copy(
            src_ref=src, dst_ref=dst, send_sem=send_sem.at[layer, sem], recv_sem=recv_sem.at[layer, sem],
            device_id=device, device_id_type=MESH)

    def copies(stage, layer):
        def grad(start, size):
            return grads.at[layer, pl.ds(start, size)]

        def total(start, size):
            return sums.at[layer, pl.ds(start, size)]

        if stage == 0:
            return [remote(grad(half * (1 - core), half), recv0.at[layer], layer, 0, peer_core)]
        if stage == 1:
            return [remote(grad(place_a + quarter * (1 - x), quarter), recv1.at[layer, 0], layer, 1, peer_x),
                    remote(grad(place_b + quarter * (1 - y), quarter), recv1.at[layer, 1], layer, 2, peer_y)]
        if stage == 2:
            return [remote(grad(place_a + quarter * x + eighth * (1 - y), eighth), recv2.at[layer, 0], layer, 3, peer_y),
                    remote(grad(place_b + quarter * y + eighth * (1 - x), eighth), recv2.at[layer, 1], layer, 4, peer_x)]
        if stage == 3:
            spot_a = total(place_a + quarter * x + eighth * y, eighth)
            spot_b = total(place_b + quarter * y + eighth * x, eighth)
            return [remote(spot_a, spot_a, layer, 5, peer_y), remote(spot_b, spot_b, layer, 6, peer_x)]
        if stage == 4:
            spot_a = total(place_a + quarter * x, quarter)
            spot_b = total(place_b + quarter * y, quarter)
            return [remote(spot_a, spot_a, layer, 7, peer_x), remote(spot_b, spot_b, layer, 8, peer_y)]
        spot = total(mine, half)
        return [remote(spot, spot, layer, 9, peer_core)]

    def add(layer, dst, start, size, other):
        dst[layer, pl.ds(start, size)] = (
            grads[layer, pl.ds(start, size)].astype(F32) + other[...].astype(F32)).astype(BF16)

    def start(stage, turn):
        for copy in copies(stage, layers - 1 - turn):
            copy.start()

    def advance(stage, turn):
        layer = layers - 1 - turn
        for copy in copies(stage, layer):
            copy.wait_recv()
        if stage == 0:
            add(layer, grads, mine, half, recv0.at[layer])
        elif stage == 1:
            add(layer, grads, place_a + quarter * x, quarter, recv1.at[layer, 0])
            add(layer, grads, place_b + quarter * y, quarter, recv1.at[layer, 1])
        elif stage == 2:
            add(layer, sums, place_a + quarter * x + eighth * y, eighth, recv2.at[layer, 0])
            add(layer, sums, place_b + quarter * y + eighth * x, eighth, recv2.at[layer, 1])
        if stage < 5:
            start(stage + 1, turn)

    def run(steps):
        for step in steps:
            advance(*step)

    def run_at(index, table):
        for at, steps in enumerate(table):
            if steps:
                pl.when(index == at)(functools.partial(run, steps))

    def backward(turn, carry):
        layer = layers - 1 - turn
        for part in (slice(0, tokens),):
            branch = d_stream[part].astype(BF16)
            d_branch[part] = branch
            normed = x_hat[layer, part, 0:dim]
            acts[part] = normed.astype(BF16)
            pre = pre_acts[layer, part]
            inner_val, cdf = gelu_parts(pre)
            hidden[part] = (pre * cdf).astype(BF16)
            slope = cdf + ((cdf - cdf * cdf) * pre) * (6.0 * inner_val - 4.0 * GELU_SCALE)
            d_hidden = dot(branch, w_out[layer], NN).astype(BF16).astype(F32)
            d_pre_part = (d_hidden * slope).astype(BF16)
            d_pre[part] = d_pre_part
            d_act = dot(d_pre_part, w_in[layer], NT).astype(BF16).astype(F32)
            mean_d = jnp.mean(d_act, axis=-1, keepdims=True)
            mean_dx = jnp.mean(d_act * normed, axis=-1, keepdims=True)
            d_stream[part] = d_stream[part] + x_hat[layer, part, dim:dim + 1] * (d_act - mean_d - normed * mean_dx)
        g_in = dot(acts[...], d_pre[...], TN).astype(BF16)
        g_out = dot(d_branch[...], hidden[...], TN).astype(BF16)
        for chunk in range(chunks):
            grads[layer, chunk * dim:(chunk + 1) * dim] = g_in[:, chunk * LANES:(chunk + 1) * LANES]
            grads[layer, half + chunk * dim:half + (chunk + 1) * dim] = g_out[:, chunk * LANES:(chunk + 1) * LANES]
        start(0, turn)
        run_at(turn, AFTER_BACKWARD)
        return carry

    lax.fori_loop(0, layers, backward, 0)
    last = layers - 1
    run(BEFORE_HEAD)

    rate, coef = rate_ref[...], coef_ref[...]
    for step in range(1, n_shards):
        head_copy(step).wait_recv()
    for copy in mom_loads[1:]:
        copy.wait()
    columns = []
    for device in range(n_shards):
        turned = head_recv[device, 8:16, :].T
        columns.append(jnp.concatenate([turned[:, 0:1], turned[0:dim - LANES, 1:2]], axis=0))
    for chunk in range(8):
        wide = min(LANES, classes - chunk * LANES)
        lanes = slice(chunk * LANES, chunk * LANES + wide)
        total_head = None
        for device in range(n_shards):
            product = columns[device] * head_recv[device, chunk:chunk + 1, 0:wide]
            product = product.astype(BF16).astype(F32)
            total_head = product if total_head is None else total_head + product
        moment = coef * m_head_ref[:, lanes] + total_head
        m_head_ref[:, lanes] = moment
        w_head_ref[:, lanes] = w_head_ref[:, lanes] - rate * moment
    stream[...] = x_next_ref[0].astype(F32).T

    run(AFTER_HEAD)

    def next_forward(layer, carry):
        run_at(layer, BEFORE_UPDATE)
        for chunk in range(chunks):
            lanes = slice(chunk * LANES, (chunk + 1) * LANES)
            for base, w_ref, m_ref, w_bf in ((0, w_in_ref, m_in_ref, w_in), (half, w_out_ref, m_out_ref, w_out)):
                grad = sums[layer, base + chunk * dim:base + (chunk + 1) * dim].astype(F32)
                moment = coef * m_ref[layer, :, lanes] + grad
                m_ref[layer, :, lanes] = moment
                weight = w_ref[layer, :, lanes] - rate * moment
                w_ref[layer, :, lanes] = weight
                w_bf[layer, :, lanes] = weight.astype(BF16)
        run_at(layer, AFTER_UPDATE)
        for part in parts:
            stream_in = stream[part]
            pre = dot(normalize(stream_in)[0].astype(BF16), w_in[layer], NN)
            out = (pre * gelu_parts(pre)[1]).astype(BF16)
            stream[part] = stream_in + dot(out, w_out[layer], NT)
        return carry

    lax.fori_loop(0, layers, next_forward, 0)
    pooled = jnp.sum(stream[...], axis=0, keepdims=True) * (1.0 / tokens)
    pooled = jnp.broadcast_to(pooled, (16, dim)).astype(BF16)
    logits_ref[...] = dot(pooled, w_head_ref[...].astype(BF16), NN)[0:1]

    def finish_all(layer, carry):
        for stage in range(6):
            for copy in copies(stage, layer):
                copy.wait_send()
        return carry

    lax.fori_loop(0, layers, finish_all, 0)
    for step in range(1, n_shards):
        head_copy(step).wait_send()


def store_kernel(*refs):
    count = (len(refs) - 1) // 2
    copies = [pltpu.make_async_copy(refs[i], refs[count + i], refs[-1].at[i]) for i in range(count)]
    for copy in copies:
        copy.start()
    for copy in copies:
        copy.wait()


def solution(mesh):
    batch_spec = P(BATCH_AXES)
    repl_spec = P()
    n_shards = mesh.shape["inner"] * mesh.shape["data"]

    def device_step(x_t, labels_t, x_next, w_in, w_out, w_head, mom_in, mom_out, mom_head, learn_rate, mom_coef):
        layers, dim, mlp_dim = w_in.shape
        tokens = x_t.shape[1]
        classes = w_head.shape[1]
        half = mlp_dim // LANES * dim
        vmem = pl.BlockSpec(memory_space=pltpu.VMEM)
        hbm = pl.BlockSpec(memory_space=pl.ANY)
        shapes = [(layers, dim, mlp_dim), (layers, dim, mlp_dim), (dim, classes)] * 2 + [(1, classes)]
        results = pl.pallas_call(
            functools.partial(step_kernel, n_shards),
            out_shape=tuple(pltpu.VMEM(shape, F32) for shape in shapes),
            in_specs=[vmem] * 5 + [hbm] * 6,
            out_specs=(vmem,) * 7,
            scratch_shapes=[
                pltpu.VMEM((tokens, dim), F32),
                pltpu.VMEM((tokens, dim), F32),
                pltpu.VMEM((layers, tokens, dim + 1), F32),
                pltpu.VMEM((tokens, dim), BF16),
                pltpu.VMEM((layers, tokens, mlp_dim), F32),
                pltpu.VMEM((tokens, mlp_dim), BF16),
                pltpu.VMEM((tokens, dim), BF16),
                pltpu.VMEM((tokens, mlp_dim), BF16),
                pltpu.VMEM((layers, dim, mlp_dim), BF16),
                pltpu.VMEM((layers, dim, mlp_dim), BF16),
                pltpu.VMEM((layers, 2 * half, LANES), BF16),
                pltpu.VMEM((layers, half, LANES), BF16),
                pltpu.VMEM((layers, 2, half // 4, LANES), BF16),
                pltpu.VMEM((layers, 2, half // 8, LANES), BF16),
                pltpu.VMEM((layers, 2 * half, LANES), BF16),
                pltpu.VMEM((16, LANES), F32),
                pltpu.VMEM((n_shards, 16, LANES), F32),
                pltpu.SemaphoreType.DMA((layers, 2)),
                pltpu.SemaphoreType.DMA((4,)),
                pltpu.SemaphoreType.DMA((layers, 10)),
                pltpu.SemaphoreType.DMA((layers, 10)),
                pltpu.SemaphoreType.DMA((n_shards,)),
                pltpu.SemaphoreType.DMA((n_shards,)),
            ],
            compiler_params=pltpu.CompilerParams(collective_id=0, has_side_effects=True, vmem_limit_bytes=VMEM_BYTES),
            name="step_kernel",
        )(x_t.transpose(0, 2, 1), x_next.transpose(0, 2, 1), labels_t.reshape(1, 1), learn_rate.reshape(1, 1), mom_coef.reshape(1, 1),
          w_in, w_out.transpose(0, 2, 1), w_head, mom_in, mom_out.transpose(0, 2, 1), mom_head)
        stored = pl.pallas_call(
            store_kernel,
            out_shape=tuple(jax.ShapeDtypeStruct(shape, F32) for shape in shapes),
            in_specs=[vmem] * 7,
            out_specs=(hbm,) * 7,
            scratch_shapes=[pltpu.SemaphoreType.DMA((7,))],
            compiler_params=pltpu.CompilerParams(vmem_limit_bytes=1000 * 1000),
            name="store_kernel",
        )(*results)
        w_in_new, w_out_new, w_head_new, m_in_new, m_out_new, m_head_new, logits = stored
        return (logits, w_in_new, w_out_new.transpose(0, 2, 1), w_head_new,
                m_in_new, m_out_new.transpose(0, 2, 1), m_head_new)

    return jax.shard_map(device_step, mesh=mesh, in_specs=(batch_spec, batch_spec, batch_spec) + (repl_spec,) * 8, out_specs=(batch_spec,) + (repl_spec,) * 6, check_vma=False)
```

```python
import functools

import jax
import jax.numpy as jnp
from jax import lax
from jax.experimental import pallas as pl
from jax.experimental.pallas import tpu as pltpu
from jax.sharding import PartitionSpec as P

LN_EPS = 1e-6
BATCH_AXES = ("inner", "data")
MESH = pl.DeviceIdType.MESH
LANES = 128
GELU_SCALE = 0.7978845608028654
GELU_CUBIC = 0.044715
F32 = jnp.float32
BF16 = jnp.bfloat16
NT = (((1,), (1,)), ((), ()))
NN = (((1,), (0,)), ((), ()))
TN = (((0,), (0,)), ((), ()))
VMEM_BYTES = 46 * 1000 * 1000
ROWS = 192


def dot(a, b, dims):
    return lax.dot_general(a, b, dims, preferred_element_type=F32)


def normalize(stream):
    mean_val = jnp.mean(stream, axis=-1, keepdims=True)
    centered = stream - mean_val
    variance = jnp.mean(centered * centered, axis=-1, keepdims=True)
    rstd = lax.rsqrt(variance + LN_EPS)
    return centered * rstd, rstd


def gelu_parts(pre):
    inner = GELU_SCALE + (GELU_SCALE * GELU_CUBIC) * (pre * pre)
    return inner, 0.5 + 0.5 * jnp.tanh(pre * inner)


AFTER_BACKWARD = [[], [(0, 0)], [(0, 1)], [(0, 2)], [(1, 0), (0, 3)], [(1, 1), (0, 4)], [(0, 5)], []]
BEFORE_HEAD = [(0, 6), (0, 7), (2, 1), (1, 5), (1, 4), (1, 6), (2, 0), (1, 7), (1, 3), (1, 2), (2, 5), (2, 6), (2, 7), (2, 4), (2, 3), (2, 2), (3, 5), (3, 7), (3, 6)]
AFTER_HEAD = [(4, 5), (3, 4), (5, 5), (3, 3), (3, 2), (4, 7), (4, 6), (5, 7)]
BEFORE_UPDATE = [[], [(5, 6)], [], [(5, 4), (4, 3)], [(4, 2), (5, 3)], [(5, 2), (4, 1)], [(4, 0), (5, 1)], [(5, 0)]]
AFTER_UPDATE = [[(3, 1), (3, 0)], [(4, 4)], [], [], [], [], [], []]


def step_kernel(n_shards,
                x_hbm, x_next_hbm, label_hbm, rate_hbm, coef_hbm, w_in_hbm, w_out_hbm, w_head_hbm, m_in_hbm, m_out_hbm, m_head_hbm,
                w_in_ref, w_out_ref, w_head_ref, m_in_ref, m_out_ref, m_head_ref, logits_ref,
                stream, d_stream, x_hat, acts, pre_acts, hidden, d_branch, d_pre, w_in, w_out,
                grads, recv0, recv1, recv2, sums, head_send, head_recv,
                x_ref, x_next_ref, label_ref, rate_ref, coef_ref,
                load_sem, mom_sem, small_sem, send_sem, recv_sem, head_send_sem, head_recv_sem):
    layers, tokens, mlp_dim = pre_acts.shape
    dim = stream.shape[1]
    classes = w_head_ref.shape[1]
    chunks = mlp_dim // LANES
    half = chunks * dim
    quarter, eighth = half // 4, half // 8
    parts = [slice(start, start + ROWS) for start in range(0, tokens, ROWS)]
    inner, core = lax.axis_index("inner"), lax.axis_index("data")
    y, x = inner // 2, inner % 2
    peer_core = (inner, 1 - core)
    peer_x = (inner + 1 - 2 * x, core)
    peer_y = (inner + 2 - 4 * y, core)
    barrier = pltpu.get_barrier_semaphore()
    me = inner * 2 + core

    def load(layer):
        return (pltpu.make_async_copy(w_in_hbm.at[layer], w_in_ref.at[layer], load_sem.at[layer, 0]),
                pltpu.make_async_copy(w_out_hbm.at[layer], w_out_ref.at[layer], load_sem.at[layer, 1]))

    mom_loads = (pltpu.make_async_copy(w_head_hbm, w_head_ref, mom_sem.at[0]),
                 pltpu.make_async_copy(m_head_hbm, m_head_ref, mom_sem.at[1]),
                 pltpu.make_async_copy(m_in_hbm, m_in_ref, mom_sem.at[2]),
                 pltpu.make_async_copy(m_out_hbm, m_out_ref, mom_sem.at[3]))

    small_loads = [pltpu.make_async_copy(src, dst, small_sem.at[i]) for i, (src, dst) in enumerate(
        ((x_hbm, x_ref), (label_hbm, label_ref), (rate_hbm, rate_ref), (coef_hbm, coef_ref), (x_next_hbm, x_next_ref)))]

    small_loads[0].start()
    for layer in range(layers):
        for copy in load(layer):
            copy.start()
    for copy in small_loads[1:] + [mom_loads[0]]:
        copy.start()
    for step in range(1, n_shards):
        other = (me + step) % n_shards
        pl.semaphore_signal(barrier, inc=1, device_id=(other // 2, other % 2), device_id_type=MESH)
    small_loads[0].wait()
    stream[...] = x_ref[0].astype(F32).T

    def forward(layer, carry):
        for copy in load(layer):
            copy.wait()
        w_in[layer] = w_in_ref[layer].astype(BF16)
        w_out[layer] = w_out_ref[layer].astype(BF16)
        for part in parts:
            stream_in = stream[part]
            normed, rstd = normalize(stream_in)
            x_hat[layer, part, 0:dim] = normed
            x_hat[layer, part, dim:dim + 1] = rstd
            pre = dot(normed.astype(BF16), w_in[layer], NN)
            pre_acts[layer, part] = pre
            out = (pre * gelu_parts(pre)[1]).astype(BF16)
            stream[part] = stream_in + dot(out, w_out[layer], NT)
        return carry

    lax.fori_loop(0, layers, forward, 0)
    for copy in mom_loads[1:]:
        copy.start()

    pooled = (jnp.sum(stream[...], axis=0, keepdims=True) * (1.0 / tokens)).astype(BF16)
    for copy in small_loads[1:] + [mom_loads[0]]:
        copy.wait()
    w_head = w_head_ref[...].astype(BF16)
    pooled_rows = jnp.broadcast_to(pooled.astype(F32), (16, dim)).astype(BF16)
    logits = dot(pooled_rows, w_head, NN)
    peak = jnp.max(logits, axis=-1, keepdims=True)
    expd = jnp.exp(logits - peak)
    probs = expd / jnp.sum(expd, axis=-1, keepdims=True)
    class_ids = lax.broadcasted_iota(jnp.int32, logits.shape, 1)
    targets = jnp.where(class_ids == label_ref[...], 1.0, 0.0)
    d_logits = ((probs - targets) * (1.0 / n_shards)).astype(BF16)
    d_pooled = dot(d_logits, w_head, NT).astype(BF16).astype(F32) / tokens
    d_stream[...] = jnp.broadcast_to(d_pooled[0:1], d_stream.shape)
    head_send[...] = jnp.zeros_like(head_send)
    d_logits = d_logits.astype(F32)
    for chunk in range(8):
        wide = min(LANES, classes - chunk * LANES)
        head_send[chunk:chunk + 1, 0:wide] = d_logits[0:1, chunk * LANES:chunk * LANES + wide]
    pooled = pooled.astype(F32)
    head_send[8:9, :] = pooled[:, 0:LANES]
    head_send[9:10, 0:dim - LANES] = pooled[:, LANES:dim]
    head_recv[0] = head_send[...]

    pl.semaphore_wait(barrier, n_shards - 1)

    def head_copy(step):
        other = (me + step) % n_shards
        return pltpu.make_async_remote_copy(
            src_ref=head_send, dst_ref=head_recv.at[step], send_sem=head_send_sem.at[step],
            recv_sem=head_recv_sem.at[step], device_id=(other // 2, other % 2), device_id_type=MESH)

    for step in range(1, n_shards):
        head_copy(step).start()

    mine = half * core
    place_a, place_b = mine, mine + half // 2

    def remote(src, dst, layer, sem, device):
        return pltpu.make_async_remote_copy(
            src_ref=src, dst_ref=dst, send_sem=send_sem.at[layer, sem], recv_sem=recv_sem.at[layer, sem],
            device_id=device, device_id_type=MESH)

    def copies(stage, layer):
        def grad(start, size):
            return grads.at[layer, pl.ds(start, size)]

        def total(start, size):
            return sums.at[layer, pl.ds(start, size)]

        if stage == 0:
            return [remote(grad(half * (1 - core), half), recv0.at[layer], layer, 0, peer_core)]
        if stage == 1:
            return [remote(grad(place_a + quarter * (1 - x), quarter), recv1.at[layer, 0], layer, 1, peer_x),
                    remote(grad(place_b + quarter * (1 - y), quarter), recv1.at[layer, 1], layer, 2, peer_y)]
        if stage == 2:
            return [remote(grad(place_a + quarter * x + eighth * (1 - y), eighth), recv2.at[layer, 0], layer, 3, peer_y),
                    remote(grad(place_b + quarter * y + eighth * (1 - x), eighth), recv2.at[layer, 1], layer, 4, peer_x)]
        if stage == 3:
            spot_a = total(place_a + quarter * x + eighth * y, eighth)
            spot_b = total(place_b + quarter * y + eighth * x, eighth)
            return [remote(spot_a, spot_a, layer, 5, peer_y), remote(spot_b, spot_b, layer, 6, peer_x)]
        if stage == 4:
            spot_a = total(place_a + quarter * x, quarter)
            spot_b = total(place_b + quarter * y, quarter)
            return [remote(spot_a, spot_a, layer, 7, peer_x), remote(spot_b, spot_b, layer, 8, peer_y)]
        spot = total(mine, half)
        return [remote(spot, spot, layer, 9, peer_core)]

    def add(layer, dst, start, size, other):
        dst[layer, pl.ds(start, size)] = (
            grads[layer, pl.ds(start, size)].astype(F32) + other[...].astype(F32)).astype(BF16)

    def start(stage, turn):
        for copy in copies(stage, layers - 1 - turn):
            copy.start()

    def advance(stage, turn):
        layer = layers - 1 - turn
        for copy in copies(stage, layer):
            copy.wait_recv()
        if stage == 0:
            add(layer, grads, mine, half, recv0.at[layer])
        elif stage == 1:
            add(layer, grads, place_a + quarter * x, quarter, recv1.at[layer, 0])
            add(layer, grads, place_b + quarter * y, quarter, recv1.at[layer, 1])
        elif stage == 2:
            add(layer, sums, place_a + quarter * x + eighth * y, eighth, recv2.at[layer, 0])
            add(layer, sums, place_b + quarter * y + eighth * x, eighth, recv2.at[layer, 1])
        if stage < 5:
            start(stage + 1, turn)

    def run(steps):
        for step in steps:
            advance(*step)

    def run_at(index, table):
        for at, steps in enumerate(table):
            if steps:
                pl.when(index == at)(functools.partial(run, steps))

    def backward(turn, carry):
        layer = layers - 1 - turn
        for part in (slice(0, tokens),):
            branch = d_stream[part].astype(BF16)
            d_branch[part] = branch
            normed = x_hat[layer, part, 0:dim]
            acts[part] = normed.astype(BF16)
            pre = pre_acts[layer, part]
            inner_val, cdf = gelu_parts(pre)
            hidden[part] = (pre * cdf).astype(BF16)
            slope = cdf + ((cdf - cdf * cdf) * pre) * (6.0 * inner_val - 4.0 * GELU_SCALE)
            d_hidden = dot(branch, w_out[layer], NN).astype(BF16).astype(F32)
            d_pre_part = (d_hidden * slope).astype(BF16)
            d_pre[part] = d_pre_part
            d_act = dot(d_pre_part, w_in[layer], NT).astype(BF16).astype(F32)
            mean_d = jnp.mean(d_act, axis=-1, keepdims=True)
            mean_dx = jnp.mean(d_act * normed, axis=-1, keepdims=True)
            d_stream[part] = d_stream[part] + x_hat[layer, part, dim:dim + 1] * (d_act - mean_d - normed * mean_dx)
        g_in = dot(acts[...], d_pre[...], TN).astype(BF16)
        g_out = dot(d_branch[...], hidden[...], TN).astype(BF16)
        for chunk in range(chunks):
            grads[layer, chunk * dim:(chunk + 1) * dim] = g_in[:, chunk * LANES:(chunk + 1) * LANES]
            grads[layer, half + chunk * dim:half + (chunk + 1) * dim] = g_out[:, chunk * LANES:(chunk + 1) * LANES]
        start(0, turn)
        run_at(turn, AFTER_BACKWARD)
        return carry

    lax.fori_loop(0, layers, backward, 0)
    last = layers - 1
    run(BEFORE_HEAD)

    rate, coef = rate_ref[...], coef_ref[...]
    for step in range(1, n_shards):
        head_copy(step).wait_recv()
    for copy in mom_loads[1:]:
        copy.wait()
    columns = []
    for device in range(n_shards):
        turned = head_recv[device, 8:16, :].T
        columns.append(jnp.concatenate([turned[:, 0:1], turned[0:dim - LANES, 1:2]], axis=0))
    for chunk in range(8):
        wide = min(LANES, classes - chunk * LANES)
        lanes = slice(chunk * LANES, chunk * LANES + wide)
        total_head = None
        for device in range(n_shards):
            product = columns[device] * head_recv[device, chunk:chunk + 1, 0:wide]
            product = product.astype(BF16).astype(F32)
            total_head = product if total_head is None else total_head + product
        moment = coef * m_head_ref[:, lanes] + total_head
        m_head_ref[:, lanes] = moment
        w_head_ref[:, lanes] = w_head_ref[:, lanes] - rate * moment
    stream[...] = x_next_ref[0].astype(F32).T

    run(AFTER_HEAD)

    def next_forward(layer, carry):
        run_at(layer, BEFORE_UPDATE)
        for chunk in range(chunks):
            lanes = slice(chunk * LANES, (chunk + 1) * LANES)
            for base, w_ref, m_ref, w_bf in ((0, w_in_ref, m_in_ref, w_in), (half, w_out_ref, m_out_ref, w_out)):
                grad = sums[layer, base + chunk * dim:base + (chunk + 1) * dim].astype(F32)
                moment = coef * m_ref[layer, :, lanes] + grad
                m_ref[layer, :, lanes] = moment
                weight = w_ref[layer, :, lanes] - rate * moment
                w_ref[layer, :, lanes] = weight
                w_bf[layer, :, lanes] = weight.astype(BF16)
        run_at(layer, AFTER_UPDATE)
        for part in parts:
            stream_in = stream[part]
            pre = dot(normalize(stream_in)[0].astype(BF16), w_in[layer], NN)
            out = (pre * gelu_parts(pre)[1]).astype(BF16)
            stream[part] = stream_in + dot(out, w_out[layer], NT)
        return carry

    lax.fori_loop(0, layers, next_forward, 0)
    pooled = jnp.sum(stream[...], axis=0, keepdims=True) * (1.0 / tokens)
    pooled = jnp.broadcast_to(pooled, (16, dim)).astype(BF16)
    logits_ref[...] = dot(pooled, w_head_ref[...].astype(BF16), NN)[0:1]

    def finish_all(layer, carry):
        for stage in range(6):
            for copy in copies(stage, layer):
                copy.wait_send()
        return carry

    lax.fori_loop(0, layers, finish_all, 0)
    for step in range(1, n_shards):
        head_copy(step).wait_send()


def store_kernel(*refs):
    count = (len(refs) - 1) // 2
    copies = [pltpu.make_async_copy(refs[i], refs[count + i], refs[-1].at[i]) for i in range(count)]
    for copy in copies:
        copy.start()
    for copy in copies:
        copy.wait()


def solution(mesh):
    batch_spec = P(BATCH_AXES)
    repl_spec = P()
    n_shards = mesh.shape["inner"] * mesh.shape["data"]

    def device_step(x_t, labels_t, x_next, w_in, w_out, w_head, mom_in, mom_out, mom_head, learn_rate, mom_coef):
        layers, dim, mlp_dim = w_in.shape
        tokens = x_t.shape[1]
        classes = w_head.shape[1]
        half = mlp_dim // LANES * dim
        vmem = pl.BlockSpec(memory_space=pltpu.VMEM)
        hbm = pl.BlockSpec(memory_space=pl.ANY)
        shapes = [(layers, dim, mlp_dim), (layers, dim, mlp_dim), (dim, classes)] * 2 + [(1, classes)]
        results = pl.pallas_call(
            functools.partial(step_kernel, n_shards),
            out_shape=tuple(pltpu.VMEM(shape, F32) for shape in shapes),
            in_specs=[hbm] * 11,
            out_specs=(vmem,) * 7,
            scratch_shapes=[
                pltpu.VMEM((tokens, dim), F32),
                pltpu.VMEM((tokens, dim), F32),
                pltpu.VMEM((layers, tokens, dim + 1), F32),
                pltpu.VMEM((tokens, dim), BF16),
                pltpu.VMEM((layers, tokens, mlp_dim), F32),
                pltpu.VMEM((tokens, mlp_dim), BF16),
                pltpu.VMEM((tokens, dim), BF16),
                pltpu.VMEM((tokens, mlp_dim), BF16),
                pltpu.VMEM((layers, dim, mlp_dim), BF16),
                pltpu.VMEM((layers, dim, mlp_dim), BF16),
                pltpu.VMEM((layers, 2 * half, LANES), BF16),
                pltpu.VMEM((layers, half, LANES), BF16),
                pltpu.VMEM((layers, 2, half // 4, LANES), BF16),
                pltpu.VMEM((layers, 2, half // 8, LANES), BF16),
                pltpu.VMEM((layers, 2 * half, LANES), BF16),
                pltpu.VMEM((16, LANES), F32),
                pltpu.VMEM((n_shards, 16, LANES), F32),
                pltpu.VMEM((1, dim, tokens), BF16),
                pltpu.VMEM((1, dim, tokens), BF16),
                pltpu.VMEM((1, 1), jnp.int32),
                pltpu.VMEM((1, 1), F32),
                pltpu.VMEM((1, 1), F32),
                pltpu.SemaphoreType.DMA((layers, 2)),
                pltpu.SemaphoreType.DMA((4,)),
                pltpu.SemaphoreType.DMA((5,)),
                pltpu.SemaphoreType.DMA((layers, 10)),
                pltpu.SemaphoreType.DMA((layers, 10)),
                pltpu.SemaphoreType.DMA((n_shards,)),
                pltpu.SemaphoreType.DMA((n_shards,)),
            ],
            compiler_params=pltpu.CompilerParams(collective_id=0, has_side_effects=True, vmem_limit_bytes=VMEM_BYTES),
            name="step_kernel",
        )(x_t.transpose(0, 2, 1), x_next.transpose(0, 2, 1), labels_t.reshape(1, 1), learn_rate.reshape(1, 1), mom_coef.reshape(1, 1),
          w_in, w_out.transpose(0, 2, 1), w_head, mom_in, mom_out.transpose(0, 2, 1), mom_head)
        stored = pl.pallas_call(
            store_kernel,
            out_shape=tuple(jax.ShapeDtypeStruct(shape, F32) for shape in shapes),
            in_specs=[vmem] * 7,
            out_specs=(hbm,) * 7,
            scratch_shapes=[pltpu.SemaphoreType.DMA((7,))],
            compiler_params=pltpu.CompilerParams(vmem_limit_bytes=1000 * 1000),
            name="store_kernel",
        )(*results)
        w_in_new, w_out_new, w_head_new, m_in_new, m_out_new, m_head_new, logits = stored
        return (logits, w_in_new, w_out_new.transpose(0, 2, 1), w_head_new,
                m_in_new, m_out_new.transpose(0, 2, 1), m_head_new)

    return jax.shard_map(device_step, mesh=mesh, in_specs=(batch_spec, batch_spec, batch_spec) + (repl_spec,) * 8, out_specs=(batch_spec,) + (repl_spec,) * 6, check_vma=False)
```

```python
import functools

import jax
import jax.numpy as jnp
from jax import lax
from jax.experimental import pallas as pl
from jax.experimental.pallas import tpu as pltpu
from jax.sharding import PartitionSpec as P

LN_EPS = 1e-6
BATCH_AXES = ("inner", "data")
MESH = pl.DeviceIdType.MESH
LANES = 128
GELU_SCALE = 0.7978845608028654
GELU_CUBIC = 0.044715
F32 = jnp.float32
BF16 = jnp.bfloat16
NT = (((1,), (1,)), ((), ()))
NN = (((1,), (0,)), ((), ()))
TN = (((0,), (0,)), ((), ()))
VMEM_BYTES = 46 * 1000 * 1000
ROWS = 192


def dot(a, b, dims):
    return lax.dot_general(a, b, dims, preferred_element_type=F32)


def normalize(stream):
    mean_val = jnp.mean(stream, axis=-1, keepdims=True)
    centered = stream - mean_val
    variance = jnp.mean(centered * centered, axis=-1, keepdims=True)
    rstd = lax.rsqrt(variance + LN_EPS)
    return centered * rstd, rstd


def gelu_parts(pre):
    inner = GELU_SCALE + (GELU_SCALE * GELU_CUBIC) * (pre * pre)
    return inner, 0.5 + 0.5 * jnp.tanh(pre * inner)


AFTER_BACKWARD = [[], [(0, 0)], [(0, 1)], [(0, 2)], [(1, 0), (0, 3)], [(1, 1), (0, 4)], [(0, 5)], []]
BEFORE_HEAD = [(0, 6), (0, 7), (2, 1), (1, 5), (1, 4), (1, 6), (2, 0), (1, 7), (1, 3), (1, 2), (2, 5), (2, 6), (2, 7), (2, 4), (2, 3), (2, 2), (3, 5), (3, 7), (3, 6)]
AFTER_HEAD = [(4, 5), (3, 4), (5, 5), (3, 3), (3, 2), (4, 7), (4, 6), (5, 7)]
BEFORE_UPDATE = [[], [(5, 6)], [], [(5, 4), (4, 3)], [(4, 2), (5, 3)], [(5, 2), (4, 1)], [(4, 0), (5, 1)], [(5, 0)]]
AFTER_UPDATE = [[(3, 1), (3, 0)], [(4, 4)], [], [], [], [], [], []]


def step_kernel(n_shards,
                x_hbm, x_next_hbm, label_hbm, rate_hbm, coef_hbm, w_in_hbm, w_out_hbm, w_head_hbm, m_in_hbm, m_out_hbm, m_head_hbm,
                w_in_ref, w_out_ref, w_head_ref, m_in_ref, m_out_ref, m_head_ref, logits_ref,
                stream, d_stream, x_hat, acts, pre_acts, hidden, d_branch, d_pre, w_in, w_out,
                grads, recv0, recv1, recv2, sums, head_send, head_recv,
                x_ref, x_next_ref, label_ref, rate_ref, coef_ref,
                load_sem, mom_sem, small_sem, send_sem, recv_sem, head_send_sem, head_recv_sem):
    layers, tokens, mlp_dim = pre_acts.shape
    dim = stream.shape[1]
    classes = w_head_ref.shape[1]
    chunks = mlp_dim // LANES
    half = chunks * dim
    quarter, eighth = half // 4, half // 8
    parts = [slice(start, start + ROWS) for start in range(0, tokens, ROWS)]
    inner, core = lax.axis_index("inner"), lax.axis_index("data")
    y, x = inner // 2, inner % 2
    peer_core = (inner, 1 - core)
    peer_x = (inner + 1 - 2 * x, core)
    peer_y = (inner + 2 - 4 * y, core)
    barrier = pltpu.get_barrier_semaphore()
    me = inner * 2 + core

    def load(layer):
        return (pltpu.make_async_copy(w_in_hbm.at[layer], w_in_ref.at[layer], load_sem.at[layer, 0]),
                pltpu.make_async_copy(w_out_hbm.at[layer], w_out_ref.at[layer], load_sem.at[layer, 1]))

    mom_loads = (pltpu.make_async_copy(w_head_hbm, w_head_ref, mom_sem.at[0]),
                 pltpu.make_async_copy(m_head_hbm, m_head_ref, mom_sem.at[1]),
                 pltpu.make_async_copy(m_in_hbm, m_in_ref, mom_sem.at[2]),
                 pltpu.make_async_copy(m_out_hbm, m_out_ref, mom_sem.at[3]))

    small_loads = [pltpu.make_async_copy(src, dst, small_sem.at[i]) for i, (src, dst) in enumerate(
        ((x_hbm, x_ref), (label_hbm, label_ref), (rate_hbm, rate_ref), (coef_hbm, coef_ref), (x_next_hbm, x_next_ref)))]

    small_loads[0].start()
    for copy in load(0) + load(1):
        copy.start()
    for step in range(1, n_shards):
        other = (me + step) % n_shards
        pl.semaphore_signal(barrier, inc=1, device_id=(other // 2, other % 2), device_id_type=MESH)
    small_loads[0].wait()
    stream[...] = x_ref[0].astype(F32).T

    def forward(layer, carry):
        for copy in load(layer):
            copy.wait()

        @pl.when(layer + 2 < layers)
        def _():
            for copy in load(layer + 2):
                copy.start()

        @pl.when(layer == layers - 2)
        def _():
            for copy in small_loads[1:] + [mom_loads[0]]:
                copy.start()

        w_in[layer] = w_in_ref[layer].astype(BF16)
        w_out[layer] = w_out_ref[layer].astype(BF16)
        for part in parts:
            stream_in = stream[part]
            normed, rstd = normalize(stream_in)
            x_hat[layer, part, 0:dim] = normed
            x_hat[layer, part, dim:dim + 1] = rstd
            pre = dot(normed.astype(BF16), w_in[layer], NN)
            pre_acts[layer, part] = pre
            out = (pre * gelu_parts(pre)[1]).astype(BF16)
            stream[part] = stream_in + dot(out, w_out[layer], NT)
        return carry

    lax.fori_loop(0, layers, forward, 0)
    for copy in mom_loads[1:]:
        copy.start()

    pooled = (jnp.sum(stream[...], axis=0, keepdims=True) * (1.0 / tokens)).astype(BF16)
    for copy in small_loads[1:] + [mom_loads[0]]:
        copy.wait()
    w_head = w_head_ref[...].astype(BF16)
    pooled_rows = jnp.broadcast_to(pooled.astype(F32), (16, dim)).astype(BF16)
    logits = dot(pooled_rows, w_head, NN)
    peak = jnp.max(logits, axis=-1, keepdims=True)
    expd = jnp.exp(logits - peak)
    probs = expd / jnp.sum(expd, axis=-1, keepdims=True)
    class_ids = lax.broadcasted_iota(jnp.int32, logits.shape, 1)
    targets = jnp.where(class_ids == label_ref[...], 1.0, 0.0)
    d_logits = ((probs - targets) * (1.0 / n_shards)).astype(BF16)
    d_pooled = dot(d_logits, w_head, NT).astype(BF16).astype(F32) / tokens
    d_stream[...] = jnp.broadcast_to(d_pooled[0:1], d_stream.shape)
    head_send[...] = jnp.zeros_like(head_send)
    d_logits = d_logits.astype(F32)
    for chunk in range(8):
        wide = min(LANES, classes - chunk * LANES)
        head_send[chunk:chunk + 1, 0:wide] = d_logits[0:1, chunk * LANES:chunk * LANES + wide]
    pooled = pooled.astype(F32)
    head_send[8:9, :] = pooled[:, 0:LANES]
    head_send[9:10, 0:dim - LANES] = pooled[:, LANES:dim]
    head_recv[0] = head_send[...]

    pl.semaphore_wait(barrier, n_shards - 1)

    def head_copy(step):
        other = (me + step) % n_shards
        return pltpu.make_async_remote_copy(
            src_ref=head_send, dst_ref=head_recv.at[step], send_sem=head_send_sem.at[step],
            recv_sem=head_recv_sem.at[step], device_id=(other // 2, other % 2), device_id_type=MESH)

    for step in range(1, n_shards):
        head_copy(step).start()

    mine = half * core
    place_a, place_b = mine, mine + half // 2

    def remote(src, dst, layer, sem, device):
        return pltpu.make_async_remote_copy(
            src_ref=src, dst_ref=dst, send_sem=send_sem.at[layer, sem], recv_sem=recv_sem.at[layer, sem],
            device_id=device, device_id_type=MESH)

    def copies(stage, layer):
        def grad(start, size):
            return grads.at[layer, pl.ds(start, size)]

        def total(start, size):
            return sums.at[layer, pl.ds(start, size)]

        if stage == 0:
            return [remote(grad(half * (1 - core), half), recv0.at[layer], layer, 0, peer_core)]
        if stage == 1:
            return [remote(grad(place_a + quarter * (1 - x), quarter), recv1.at[layer, 0], layer, 1, peer_x),
                    remote(grad(place_b + quarter * (1 - y), quarter), recv1.at[layer, 1], layer, 2, peer_y)]
        if stage == 2:
            return [remote(grad(place_a + quarter * x + eighth * (1 - y), eighth), recv2.at[layer, 0], layer, 3, peer_y),
                    remote(grad(place_b + quarter * y + eighth * (1 - x), eighth), recv2.at[layer, 1], layer, 4, peer_x)]
        if stage == 3:
            spot_a = total(place_a + quarter * x + eighth * y, eighth)
            spot_b = total(place_b + quarter * y + eighth * x, eighth)
            return [remote(spot_a, spot_a, layer, 5, peer_y), remote(spot_b, spot_b, layer, 6, peer_x)]
        if stage == 4:
            spot_a = total(place_a + quarter * x, quarter)
            spot_b = total(place_b + quarter * y, quarter)
            return [remote(spot_a, spot_a, layer, 7, peer_x), remote(spot_b, spot_b, layer, 8, peer_y)]
        spot = total(mine, half)
        return [remote(spot, spot, layer, 9, peer_core)]

    def add(layer, dst, start, size, other):
        dst[layer, pl.ds(start, size)] = (
            grads[layer, pl.ds(start, size)].astype(F32) + other[...].astype(F32)).astype(BF16)

    def start(stage, turn):
        for copy in copies(stage, layers - 1 - turn):
            copy.start()

    def advance(stage, turn):
        layer = layers - 1 - turn
        for copy in copies(stage, layer):
            copy.wait_recv()
        if stage == 0:
            add(layer, grads, mine, half, recv0.at[layer])
        elif stage == 1:
            add(layer, grads, place_a + quarter * x, quarter, recv1.at[layer, 0])
            add(layer, grads, place_b + quarter * y, quarter, recv1.at[layer, 1])
        elif stage == 2:
            add(layer, sums, place_a + quarter * x + eighth * y, eighth, recv2.at[layer, 0])
            add(layer, sums, place_b + quarter * y + eighth * x, eighth, recv2.at[layer, 1])
        if stage < 5:
            start(stage + 1, turn)

    def run(steps):
        for step in steps:
            advance(*step)

    def run_at(index, table):
        for at, steps in enumerate(table):
            if steps:
                pl.when(index == at)(functools.partial(run, steps))

    def backward(turn, carry):
        layer = layers - 1 - turn
        for part in (slice(0, tokens),):
            branch = d_stream[part].astype(BF16)
            d_branch[part] = branch
            normed = x_hat[layer, part, 0:dim]
            acts[part] = normed.astype(BF16)
            pre = pre_acts[layer, part]
            inner_val, cdf = gelu_parts(pre)
            hidden[part] = (pre * cdf).astype(BF16)
            slope = cdf + ((cdf - cdf * cdf) * pre) * (6.0 * inner_val - 4.0 * GELU_SCALE)
            d_hidden = dot(branch, w_out[layer], NN).astype(BF16).astype(F32)
            d_pre_part = (d_hidden * slope).astype(BF16)
            d_pre[part] = d_pre_part
            d_act = dot(d_pre_part, w_in[layer], NT).astype(BF16).astype(F32)
            mean_d = jnp.mean(d_act, axis=-1, keepdims=True)
            mean_dx = jnp.mean(d_act * normed, axis=-1, keepdims=True)
            d_stream[part] = d_stream[part] + x_hat[layer, part, dim:dim + 1] * (d_act - mean_d - normed * mean_dx)
        g_in = dot(acts[...], d_pre[...], TN).astype(BF16)
        g_out = dot(d_branch[...], hidden[...], TN).astype(BF16)
        for chunk in range(chunks):
            grads[layer, chunk * dim:(chunk + 1) * dim] = g_in[:, chunk * LANES:(chunk + 1) * LANES]
            grads[layer, half + chunk * dim:half + (chunk + 1) * dim] = g_out[:, chunk * LANES:(chunk + 1) * LANES]
        start(0, turn)
        run_at(turn, AFTER_BACKWARD)
        return carry

    lax.fori_loop(0, layers, backward, 0)
    last = layers - 1
    run(BEFORE_HEAD)

    rate, coef = rate_ref[...], coef_ref[...]
    for step in range(1, n_shards):
        head_copy(step).wait_recv()
    for copy in mom_loads[1:]:
        copy.wait()
    columns = []
    for device in range(n_shards):
        turned = head_recv[device, 8:16, :].T
        columns.append(jnp.concatenate([turned[:, 0:1], turned[0:dim - LANES, 1:2]], axis=0))
    for chunk in range(8):
        wide = min(LANES, classes - chunk * LANES)
        lanes = slice(chunk * LANES, chunk * LANES + wide)
        total_head = None
        for device in range(n_shards):
            product = columns[device] * head_recv[device, chunk:chunk + 1, 0:wide]
            product = product.astype(BF16).astype(F32)
            total_head = product if total_head is None else total_head + product
        moment = coef * m_head_ref[:, lanes] + total_head
        m_head_ref[:, lanes] = moment
        w_head_ref[:, lanes] = w_head_ref[:, lanes] - rate * moment
    stream[...] = x_next_ref[0].astype(F32).T

    run(AFTER_HEAD)

    def next_forward(layer, carry):
        run_at(layer, BEFORE_UPDATE)
        for chunk in range(chunks):
            lanes = slice(chunk * LANES, (chunk + 1) * LANES)
            for base, w_ref, m_ref, w_bf in ((0, w_in_ref, m_in_ref, w_in), (half, w_out_ref, m_out_ref, w_out)):
                grad = sums[layer, base + chunk * dim:base + (chunk + 1) * dim].astype(F32)
                moment = coef * m_ref[layer, :, lanes] + grad
                m_ref[layer, :, lanes] = moment
                weight = w_ref[layer, :, lanes] - rate * moment
                w_ref[layer, :, lanes] = weight
                w_bf[layer, :, lanes] = weight.astype(BF16)
        run_at(layer, AFTER_UPDATE)
        for part in parts:
            stream_in = stream[part]
            pre = dot(normalize(stream_in)[0].astype(BF16), w_in[layer], NN)
            out = (pre * gelu_parts(pre)[1]).astype(BF16)
            stream[part] = stream_in + dot(out, w_out[layer], NT)
        return carry

    lax.fori_loop(0, layers, next_forward, 0)
    pooled = jnp.sum(stream[...], axis=0, keepdims=True) * (1.0 / tokens)
    pooled = jnp.broadcast_to(pooled, (16, dim)).astype(BF16)
    logits_ref[...] = dot(pooled, w_head_ref[...].astype(BF16), NN)[0:1]

    def finish_all(layer, carry):
        for stage in range(6):
            for copy in copies(stage, layer):
                copy.wait_send()
        return carry

    lax.fori_loop(0, layers, finish_all, 0)
    for step in range(1, n_shards):
        head_copy(step).wait_send()


def store_kernel(*refs):
    count = (len(refs) - 1) // 2
    copies = [pltpu.make_async_copy(refs[i], refs[count + i], refs[-1].at[i]) for i in range(count)]
    for copy in copies:
        copy.start()
    for copy in copies:
        copy.wait()


def solution(mesh):
    batch_spec = P(BATCH_AXES)
    repl_spec = P()
    n_shards = mesh.shape["inner"] * mesh.shape["data"]

    def device_step(x_t, labels_t, x_next, w_in, w_out, w_head, mom_in, mom_out, mom_head, learn_rate, mom_coef):
        layers, dim, mlp_dim = w_in.shape
        tokens = x_t.shape[1]
        classes = w_head.shape[1]
        half = mlp_dim // LANES * dim
        vmem = pl.BlockSpec(memory_space=pltpu.VMEM)
        hbm = pl.BlockSpec(memory_space=pl.ANY)
        shapes = [(layers, dim, mlp_dim), (layers, dim, mlp_dim), (dim, classes)] * 2 + [(1, classes)]
        results = pl.pallas_call(
            functools.partial(step_kernel, n_shards),
            out_shape=tuple(pltpu.VMEM(shape, F32) for shape in shapes),
            in_specs=[hbm] * 11,
            out_specs=(vmem,) * 7,
            scratch_shapes=[
                pltpu.VMEM((tokens, dim), F32),
                pltpu.VMEM((tokens, dim), F32),
                pltpu.VMEM((layers, tokens, dim + 1), F32),
                pltpu.VMEM((tokens, dim), BF16),
                pltpu.VMEM((layers, tokens, mlp_dim), F32),
                pltpu.VMEM((tokens, mlp_dim), BF16),
                pltpu.VMEM((tokens, dim), BF16),
                pltpu.VMEM((tokens, mlp_dim), BF16),
                pltpu.VMEM((layers, dim, mlp_dim), BF16),
                pltpu.VMEM((layers, dim, mlp_dim), BF16),
                pltpu.VMEM((layers, 2 * half, LANES), BF16),
                pltpu.VMEM((layers, half, LANES), BF16),
                pltpu.VMEM((layers, 2, half // 4, LANES), BF16),
                pltpu.VMEM((layers, 2, half // 8, LANES), BF16),
                pltpu.VMEM((layers, 2 * half, LANES), BF16),
                pltpu.VMEM((16, LANES), F32),
                pltpu.VMEM((n_shards, 16, LANES), F32),
                pltpu.VMEM((1, dim, tokens), BF16),
                pltpu.VMEM((1, dim, tokens), BF16),
                pltpu.VMEM((1, 1), jnp.int32),
                pltpu.VMEM((1, 1), F32),
                pltpu.VMEM((1, 1), F32),
                pltpu.SemaphoreType.DMA((layers, 2)),
                pltpu.SemaphoreType.DMA((4,)),
                pltpu.SemaphoreType.DMA((5,)),
                pltpu.SemaphoreType.DMA((layers, 10)),
                pltpu.SemaphoreType.DMA((layers, 10)),
                pltpu.SemaphoreType.DMA((n_shards,)),
                pltpu.SemaphoreType.DMA((n_shards,)),
            ],
            compiler_params=pltpu.CompilerParams(collective_id=0, has_side_effects=True, vmem_limit_bytes=VMEM_BYTES),
            name="step_kernel",
        )(x_t.transpose(0, 2, 1), x_next.transpose(0, 2, 1), labels_t.reshape(1, 1), learn_rate.reshape(1, 1), mom_coef.reshape(1, 1),
          w_in, w_out.transpose(0, 2, 1), w_head, mom_in, mom_out.transpose(0, 2, 1), mom_head)
        stored = pl.pallas_call(
            store_kernel,
            out_shape=tuple(jax.ShapeDtypeStruct(shape, F32) for shape in shapes),
            in_specs=[vmem] * 7,
            out_specs=(hbm,) * 7,
            scratch_shapes=[pltpu.SemaphoreType.DMA((7,))],
            compiler_params=pltpu.CompilerParams(vmem_limit_bytes=1000 * 1000),
            name="store_kernel",
        )(*results)
        w_in_new, w_out_new, w_head_new, m_in_new, m_out_new, m_head_new, logits = stored
        return (logits, w_in_new, w_out_new.transpose(0, 2, 1), w_head_new,
                m_in_new, m_out_new.transpose(0, 2, 1), m_head_new)

    return jax.shard_map(device_step, mesh=mesh, in_specs=(batch_spec, batch_spec, batch_spec) + (repl_spec,) * 8, out_specs=(batch_spec,) + (repl_spec,) * 6, check_vma=False)
```

```python
import functools

import jax
import jax.numpy as jnp
from jax import lax
from jax.experimental import pallas as pl
from jax.experimental.pallas import tpu as pltpu
from jax.sharding import PartitionSpec as P

LN_EPS = 1e-6
BATCH_AXES = ("inner", "data")
MESH = pl.DeviceIdType.MESH
LANES = 128
GELU_SCALE = 0.7978845608028654
GELU_CUBIC = 0.044715
F32 = jnp.float32
BF16 = jnp.bfloat16
NT = (((1,), (1,)), ((), ()))
NN = (((1,), (0,)), ((), ()))
TN = (((0,), (0,)), ((), ()))
VMEM_BYTES = 40600 * 1000
ROWS = 192
LATE = 3


def dot(a, b, dims):
    return lax.dot_general(a, b, dims, preferred_element_type=F32)


def normalize(stream):
    mean_val = jnp.mean(stream, axis=-1, keepdims=True)
    centered = stream - mean_val
    variance = jnp.mean(centered * centered, axis=-1, keepdims=True)
    rstd = lax.rsqrt(variance + LN_EPS)
    return centered * rstd, rstd


def gelu_parts(pre):
    inner = GELU_SCALE + (GELU_SCALE * GELU_CUBIC) * (pre * pre)
    return inner, 0.5 + 0.5 * jnp.tanh(pre * inner)


AFTER_BACKWARD = [[], [(0, 0)], [(0, 1)], [(0, 2), (1, 0)], [(1, 1), (0, 3)], [(1, 2), (0, 4)], [(0, 5), (2, 1), (1, 3), (0, 6)], []]
BEFORE_HEAD = [(1, 5), (0, 7), (2, 3), (1, 6), (2, 5), (1, 4), (1, 7), (2, 2), (2, 6), (2, 0), (2, 4), (2, 7), (3, 5), (3, 6), (3, 7)]
AFTER_HEAD = [(3, 4), (3, 3), (4, 7), (3, 1), (4, 5), (4, 4), (3, 2), (5, 7), (4, 6)]
BEFORE_UPDATE = [[], [(5, 4), (5, 5), (3, 0), (5, 6)], [(4, 3), (4, 1)], [(5, 3), (4, 2)], [(4, 0)]]
AFTER_UPDATE = [[], [], [], [], [(5, 2)]]
AT_END = [(5, 1), (5, 0)]


def update(layer, slot, rate, coef, sums, old, new, w_in, w_out):
    dim, mlp_dim = w_in.shape
    half = mlp_dim // LANES * dim
    for start in range(0, mlp_dim, LANES):
        lanes = slice(start, start + LANES)
        for base, w_old, m_old, w_new, m_new, w_bf in (
                (0, old[0], old[1], new[0], new[1], w_in), (half, old[2], old[3], new[2], new[3], w_out)):
            row = base + start // LANES * dim
            moment = coef * m_old[layer, :, lanes] + sums[layer, row:row + dim].astype(F32)
            m_new[slot, :, lanes] = moment
            weight = w_old[layer, :, lanes] - rate * moment
            w_new[slot, :, lanes] = weight
            w_bf[:, lanes] = weight.astype(BF16)


def next_block(stream, w_in, w_out):
    for start in range(0, stream.shape[0], ROWS):
        part = slice(start, start + ROWS)
        stream_in = stream[part]
        pre = dot(normalize(stream_in)[0].astype(BF16), w_in[...], NN)
        out = (pre * gelu_parts(pre)[1]).astype(BF16)
        stream[part] = stream_in + dot(out, w_out[...], NT)


def step_kernel(n_shards,
                x_hbm, x_next_hbm, label_hbm, rate_hbm, coef_hbm, w_in_hbm, w_out_hbm, w_head_hbm, m_in_hbm, m_out_hbm, m_head_hbm,
                w_in_ref, w_out_ref, w_head_ref, m_in_ref, m_out_ref, m_head_ref, sums, stream,
                d_stream, x_hat, acts, pre_acts, hidden, d_branch, d_pre, w_in, w_out,
                grads, recv0, recv1, recv2, head_send, head_recv,
                x_ref, x_next_ref, label_ref, rate_ref, coef_ref,
                load_sem, mom_sem, small_sem, send_sem, recv_sem, head_send_sem, head_recv_sem):
    layers, tokens, mlp_dim = pre_acts.shape
    dim = stream.shape[1]
    classes = w_head_ref.shape[1]
    chunks = mlp_dim // LANES
    half = chunks * dim
    quarter, eighth = half // 4, half // 8
    parts = [slice(start, start + ROWS) for start in range(0, tokens, ROWS)]
    inner, core = lax.axis_index("inner"), lax.axis_index("data")
    y, x = inner // 2, inner % 2
    peer_core = (inner, 1 - core)
    peer_x = (inner + 1 - 2 * x, core)
    peer_y = (inner + 2 - 4 * y, core)
    barrier = pltpu.get_barrier_semaphore()
    me = inner * 2 + core

    def load(layer):
        return (pltpu.make_async_copy(w_in_hbm.at[layer], w_in_ref.at[layer], load_sem.at[layer % 4, 0]),
                pltpu.make_async_copy(w_out_hbm.at[layer], w_out_ref.at[layer], load_sem.at[layer % 4, 1]))

    mom_loads = (pltpu.make_async_copy(w_head_hbm, w_head_ref, mom_sem.at[0]),
                 pltpu.make_async_copy(m_head_hbm, m_head_ref, mom_sem.at[1]),
                 pltpu.make_async_copy(m_in_hbm, m_in_ref, mom_sem.at[2]),
                 pltpu.make_async_copy(m_out_hbm, m_out_ref, mom_sem.at[3]))

    small_loads = [pltpu.make_async_copy(src, dst, small_sem.at[i]) for i, (src, dst) in enumerate(
        ((x_hbm, x_ref), (label_hbm, label_ref), (rate_hbm, rate_ref), (coef_hbm, coef_ref), (x_next_hbm, x_next_ref)))]

    small_loads[0].start()
    for copy in load(0) + load(1):
        copy.start()
    for step in range(1, n_shards):
        other = (me + step) % n_shards
        pl.semaphore_signal(barrier, inc=1, device_id=(other // 2, other % 2), device_id_type=MESH)
    small_loads[0].wait()
    stream[...] = x_ref[0].astype(F32).T

    def forward(layer, carry):
        for copy in load(layer):
            copy.wait()

        @pl.when(layer + 2 < layers)
        def _():
            for copy in load(layer + 2):
                copy.start()

        @pl.when(layer == layers - 2)
        def _():
            for copy in small_loads[1:] + [mom_loads[0]]:
                copy.start()

        w_in[layer] = w_in_ref[layer].astype(BF16)
        w_out[layer] = w_out_ref[layer].astype(BF16)
        for part in parts:
            stream_in = stream[part]
            normed, rstd = normalize(stream_in)
            x_hat[layer, part, 0:dim] = normed
            x_hat[layer, part, dim:dim + 1] = rstd
            pre = dot(normed.astype(BF16), w_in[layer], NN)
            pre_acts[layer, part] = pre
            out = (pre * gelu_parts(pre)[1]).astype(BF16)
            stream[part] = stream_in + dot(out, w_out[layer], NT)
        return carry

    lax.fori_loop(0, layers, forward, 0)
    for copy in mom_loads[1:]:
        copy.start()

    pooled = (jnp.sum(stream[...], axis=0, keepdims=True) * (1.0 / tokens)).astype(BF16)
    for copy in small_loads[1:] + [mom_loads[0]]:
        copy.wait()
    w_head = w_head_ref[...].astype(BF16)
    pooled_rows = jnp.broadcast_to(pooled.astype(F32), (16, dim)).astype(BF16)
    logits = dot(pooled_rows, w_head, NN)
    peak = jnp.max(logits, axis=-1, keepdims=True)
    expd = jnp.exp(logits - peak)
    probs = expd / jnp.sum(expd, axis=-1, keepdims=True)
    class_ids = lax.broadcasted_iota(jnp.int32, logits.shape, 1)
    targets = jnp.where(class_ids == label_ref[...], 1.0, 0.0)
    d_logits = ((probs - targets) * (1.0 / n_shards)).astype(BF16)
    d_pooled = dot(d_logits, w_head, NT).astype(BF16).astype(F32) / tokens
    d_stream[...] = jnp.broadcast_to(d_pooled[0:1], d_stream.shape)
    head_send[...] = jnp.zeros_like(head_send)
    d_logits = d_logits.astype(F32)
    for chunk in range(8):
        wide = min(LANES, classes - chunk * LANES)
        head_send[chunk:chunk + 1, 0:wide] = d_logits[0:1, chunk * LANES:chunk * LANES + wide]
    pooled = pooled.astype(F32)
    head_send[8:9, :] = pooled[:, 0:LANES]
    head_send[9:10, 0:dim - LANES] = pooled[:, LANES:dim]
    head_recv[0] = head_send[...]

    pl.semaphore_wait(barrier, n_shards - 1)

    def head_copy(step):
        other = (me + step) % n_shards
        return pltpu.make_async_remote_copy(
            src_ref=head_send, dst_ref=head_recv.at[step], send_sem=head_send_sem.at[0],
            recv_sem=head_recv_sem.at[0], device_id=(other // 2, other % 2), device_id_type=MESH)

    for step in range(1, n_shards):
        head_copy(step).start()

    def all_head_copies():
        others = head_recv.at[pl.ds(1, n_shards - 1)]
        return pltpu.make_async_remote_copy(
            src_ref=others, dst_ref=others, send_sem=head_send_sem.at[0],
            recv_sem=head_recv_sem.at[0], device_id=peer_core, device_id_type=MESH)

    mine = half * core
    place_a, place_b = mine, mine + half // 2

    def remote(src, dst, layer, stage, device):
        near = 0 if stage in (0, 5) else 1
        return pltpu.make_async_remote_copy(
            src_ref=src, dst_ref=dst, send_sem=send_sem.at[layer, near], recv_sem=recv_sem.at[layer, stage],
            device_id=device, device_id_type=MESH)

    def copies(stage, layer):
        def grad(start, size):
            return grads.at[layer, pl.ds(start, size)]

        def total(start, size):
            return sums.at[layer, pl.ds(start, size)]

        if stage == 0:
            return [remote(grad(half * (1 - core), half), recv0.at[layer], layer, stage, peer_core)]
        if stage == 1:
            return [remote(grad(place_a + quarter * (1 - x), quarter), recv1.at[layer, 0], layer, stage, peer_x),
                    remote(grad(place_b + quarter * (1 - y), quarter), recv1.at[layer, 1], layer, stage, peer_y)]
        if stage == 2:
            return [remote(grad(place_a + quarter * x + eighth * (1 - y), eighth), recv2.at[layer, 0], layer, stage, peer_y),
                    remote(grad(place_b + quarter * y + eighth * (1 - x), eighth), recv2.at[layer, 1], layer, stage, peer_x)]
        if stage == 3:
            spot_a = total(place_a + quarter * x + eighth * y, eighth)
            spot_b = total(place_b + quarter * y + eighth * x, eighth)
            return [remote(spot_a, spot_a, layer, stage, peer_y), remote(spot_b, spot_b, layer, stage, peer_x)]
        if stage == 4:
            spot_a = total(place_a + quarter * x, quarter)
            spot_b = total(place_b + quarter * y, quarter)
            return [remote(spot_a, spot_a, layer, stage, peer_x), remote(spot_b, spot_b, layer, stage, peer_y)]
        spot = total(mine, half)
        return [remote(spot, spot, layer, stage, peer_core)]

    def add(layer, dst, start, size, other):
        dst[layer, pl.ds(start, size)] = (
            grads[layer, pl.ds(start, size)].astype(F32) + other[...].astype(F32)).astype(BF16)

    def start(stage, turn):
        for copy in copies(stage, layers - 1 - turn):
            copy.start()

    def advance(stage, turn):
        layer = layers - 1 - turn
        size = (half, 2 * quarter, 2 * eighth, 2 * eighth, 2 * quarter, half)[stage]
        spot = grads.at[layer, pl.ds(0, size)]
        remote(spot, spot, layer, stage, peer_core).wait_recv()
        if stage == 0:
            add(layer, grads, mine, half, recv0.at[layer])
        elif stage == 1:
            add(layer, grads, place_a + quarter * x, quarter, recv1.at[layer, 0])
            add(layer, grads, place_b + quarter * y, quarter, recv1.at[layer, 1])
        elif stage == 2:
            add(layer, sums, place_a + quarter * x + eighth * y, eighth, recv2.at[layer, 0])
            add(layer, sums, place_b + quarter * y + eighth * x, eighth, recv2.at[layer, 1])
        if stage < 5:
            start(stage + 1, turn)

    def run(steps):
        for step in steps:
            advance(*step)

    def run_at(index, table):
        for at, steps in enumerate(table):
            if steps:
                pl.when(index == at)(functools.partial(run, steps))

    def backward(turn, carry):
        layer = layers - 1 - turn
        for part in (slice(0, tokens),):
            branch = d_stream[part].astype(BF16)
            d_branch[part] = branch
            normed = x_hat[layer, part, 0:dim]
            acts[part] = normed.astype(BF16)
            pre = pre_acts[layer, part]
            inner_val, cdf = gelu_parts(pre)
            hidden[part] = (pre * cdf).astype(BF16)
            slope = cdf + ((cdf - cdf * cdf) * pre) * (6.0 * inner_val - 4.0 * GELU_SCALE)
            d_hidden = dot(branch, w_out[layer], NN).astype(BF16).astype(F32)
            d_pre_part = (d_hidden * slope).astype(BF16)
            d_pre[part] = d_pre_part
            d_act = dot(d_pre_part, w_in[layer], NT).astype(BF16).astype(F32)
            mean_d = jnp.mean(d_act, axis=-1, keepdims=True)
            mean_dx = jnp.mean(d_act * normed, axis=-1, keepdims=True)
            d_stream[part] = d_stream[part] + x_hat[layer, part, dim:dim + 1] * (d_act - mean_d - normed * mean_dx)
        g_in = dot(acts[...], d_pre[...], TN).astype(BF16)
        g_out = dot(d_branch[...], hidden[...], TN).astype(BF16)
        for chunk in range(chunks):
            grads[layer, chunk * dim:(chunk + 1) * dim] = g_in[:, chunk * LANES:(chunk + 1) * LANES]
            grads[layer, half + chunk * dim:half + (chunk + 1) * dim] = g_out[:, chunk * LANES:(chunk + 1) * LANES]
        start(0, turn)
        run_at(turn, AFTER_BACKWARD)
        return carry

    lax.fori_loop(0, layers, backward, 0)
    last = layers - 1
    run(BEFORE_HEAD)

    rate, coef = rate_ref[...], coef_ref[...]
    all_head_copies().wait_recv()
    for copy in mom_loads[1:]:
        copy.wait()
    columns = []
    for device in range(n_shards):
        turned = head_recv[device, 8:16, :].T
        columns.append(jnp.concatenate([turned[:, 0:1], turned[0:dim - LANES, 1:2]], axis=0))
    for chunk in range(8):
        wide = min(LANES, classes - chunk * LANES)
        lanes = slice(chunk * LANES, chunk * LANES + wide)
        total_head = None
        for device in range(n_shards):
            product = columns[device] * head_recv[device, chunk:chunk + 1, 0:wide]
            product = product.astype(BF16).astype(F32)
            total_head = product if total_head is None else total_head + product
        moment = coef * m_head_ref[:, lanes] + total_head
        m_head_ref[:, lanes] = moment
        w_head_ref[:, lanes] = w_head_ref[:, lanes] - rate * moment
    stream[...] = x_next_ref[0].astype(F32).T

    run(AFTER_HEAD)

    def next_forward(layer, carry):
        run_at(layer, BEFORE_UPDATE)
        update(layer, layer, rate, coef, sums, (w_in_ref, m_in_ref, w_out_ref, m_out_ref), (w_in_ref, m_in_ref, w_out_ref, m_out_ref),
               w_in.at[layer], w_out.at[layer])
        run_at(layer, AFTER_UPDATE)
        next_block(stream, w_in.at[layer], w_out.at[layer])
        return carry

    lax.fori_loop(0, layers - LATE, next_forward, 0)
    run(AT_END)

    def finish_all(layer, carry):
        for stage, size in ((0, 2 * half), (1, 3 * half // 2)):
            spot = grads.at[layer, pl.ds(0, size)]
            remote(spot, spot, layer, stage, peer_core).wait_send()
        return carry

    lax.fori_loop(0, layers, finish_all, 0)
    all_head_copies().wait_send()


def store_kernel(rate_ref, coef_ref, w_in_ref, w_out_ref, w_head_ref, m_in_ref, m_out_ref, m_head_ref, sums, stream_ref,
                 w_in_out, w_out_out, w_head_out, m_in_out, m_out_out, m_head_out, logits_out,
                 stream, w_in_late, m_in_late, w_out_late, m_out_late, w_in, w_out, logits, early_sem, late_sem):
    layers = w_in_ref.shape[0]
    tokens, dim = stream.shape
    early = layers - LATE
    rate, coef = rate_ref[...], coef_ref[...]
    old = (w_in_ref, m_in_ref, w_out_ref, m_out_ref)
    new = (w_in_late, m_in_late, w_out_late, m_out_late)
    outs = (w_in_out, m_in_out, w_out_out, m_out_out)
    copies = [pltpu.make_async_copy(src.at[pl.ds(0, early)], dst.at[pl.ds(0, early)], early_sem.at[i])
              for i, (src, dst) in enumerate(zip(old, outs))]
    copies.append(pltpu.make_async_copy(w_head_ref, w_head_out, early_sem.at[4]))
    copies.append(pltpu.make_async_copy(m_head_ref, m_head_out, early_sem.at[5]))
    for copy in copies:
        copy.start()
    stream[...] = stream_ref[...]

    def late_copies(step):
        return [pltpu.make_async_copy(src.at[step], dst.at[early + step], late_sem.at[step, i])
                for i, (src, dst) in enumerate(zip(new, outs))]

    def late_layer(step, carry):
        update(early + step, step, rate, coef, sums, old, new, w_in, w_out)
        for copy in late_copies(step):
            copy.start()
        next_block(stream, w_in, w_out)
        return carry

    lax.fori_loop(0, LATE, late_layer, 0)
    pooled = jnp.sum(stream[...], axis=0, keepdims=True) * (1.0 / tokens)
    pooled = jnp.broadcast_to(pooled, (16, dim)).astype(BF16)
    logits[...] = dot(pooled, w_head_ref[...].astype(BF16), NN)[0:1]
    copies.append(pltpu.make_async_copy(logits, logits_out, early_sem.at[6]))
    copies[-1].start()
    for step in range(LATE):
        copies += late_copies(step)
    for copy in copies:
        copy.wait()


def solution(mesh):
    batch_spec = P(BATCH_AXES)
    repl_spec = P()
    n_shards = mesh.shape["inner"] * mesh.shape["data"]

    def device_step(x_t, labels_t, x_next, w_in, w_out, w_head, mom_in, mom_out, mom_head, learn_rate, mom_coef):
        layers, dim, mlp_dim = w_in.shape
        tokens = x_t.shape[1]
        classes = w_head.shape[1]
        half = mlp_dim // LANES * dim
        vmem = pl.BlockSpec(memory_space=pltpu.VMEM)
        hbm = pl.BlockSpec(memory_space=pl.ANY)
        shapes = [(layers, dim, mlp_dim), (layers, dim, mlp_dim), (dim, classes)] * 2
        rate, coef = learn_rate.reshape(1, 1), mom_coef.reshape(1, 1)
        results = pl.pallas_call(
            functools.partial(step_kernel, n_shards),
            out_shape=tuple(pltpu.VMEM(shape, F32) for shape in shapes) + (pltpu.VMEM((layers, 2 * half, LANES), BF16), pltpu.VMEM((tokens, dim), F32)),
            in_specs=[hbm] * 11,
            out_specs=(vmem,) * 8,
            scratch_shapes=[
                pltpu.VMEM((tokens, dim), F32),
                pltpu.VMEM((layers, tokens, dim + 1), F32),
                pltpu.VMEM((tokens, dim), BF16),
                pltpu.VMEM((layers, tokens, mlp_dim), F32),
                pltpu.VMEM((tokens, mlp_dim), BF16),
                pltpu.VMEM((tokens, dim), BF16),
                pltpu.VMEM((tokens, mlp_dim), BF16),
                pltpu.VMEM((layers, dim, mlp_dim), BF16),
                pltpu.VMEM((layers, dim, mlp_dim), BF16),
                pltpu.VMEM((layers, 2 * half, LANES), BF16),
                pltpu.VMEM((layers, half, LANES), BF16),
                pltpu.VMEM((layers, 2, half // 4, LANES), BF16),
                pltpu.VMEM((layers, 2, half // 8, LANES), BF16),
                pltpu.VMEM((16, LANES), F32),
                pltpu.VMEM((n_shards, 16, LANES), F32),
                pltpu.VMEM((1, dim, tokens), BF16),
                pltpu.VMEM((1, dim, tokens), BF16),
                pltpu.VMEM((1, 1), jnp.int32),
                pltpu.VMEM((1, 1), F32),
                pltpu.VMEM((1, 1), F32),
                pltpu.SemaphoreType.DMA((4, 2)),
                pltpu.SemaphoreType.DMA((4,)),
                pltpu.SemaphoreType.DMA((5,)),
                pltpu.SemaphoreType.DMA((layers, 2)),
                pltpu.SemaphoreType.DMA((layers, 6)),
                pltpu.SemaphoreType.DMA((1,)),
                pltpu.SemaphoreType.DMA((1,)),
            ],
            compiler_params=pltpu.CompilerParams(collective_id=0, has_side_effects=True, vmem_limit_bytes=VMEM_BYTES),
            name="step_kernel",
        )(x_t.transpose(0, 2, 1), x_next.transpose(0, 2, 1), labels_t.reshape(1, 1), rate, coef,
          w_in, w_out.transpose(0, 2, 1), w_head, mom_in, mom_out.transpose(0, 2, 1), mom_head)
        late = pltpu.VMEM((LATE, dim, mlp_dim), F32)
        w_in_new, w_out_new, w_head_new, m_in_new, m_out_new, m_head_new, logits = pl.pallas_call(
            store_kernel,
            out_shape=tuple(jax.ShapeDtypeStruct(shape, F32) for shape in shapes + [(1, classes)]),
            in_specs=[vmem] * 10,
            out_specs=(hbm,) * 7,
            scratch_shapes=[
                pltpu.VMEM((tokens, dim), F32), late, late, late, late,
                pltpu.VMEM((dim, mlp_dim), BF16), pltpu.VMEM((dim, mlp_dim), BF16), pltpu.VMEM((1, classes), F32),
                pltpu.SemaphoreType.DMA((7,)), pltpu.SemaphoreType.DMA((LATE, 4)),
            ],
            compiler_params=pltpu.CompilerParams(vmem_limit_bytes=11 * 1000 * 1000),
            name="store_kernel",
        )(rate, coef, *results)
        return (logits, w_in_new, w_out_new.transpose(0, 2, 1), w_head_new,
                m_in_new, m_out_new.transpose(0, 2, 1), m_head_new)

    return jax.shard_map(device_step, mesh=mesh, in_specs=(batch_spec, batch_spec, batch_spec) + (repl_spec,) * 8, out_specs=(batch_spec,) + (repl_spec,) * 6, check_vma=False)
```

```python
import functools

import jax
import jax.numpy as jnp
from jax import lax
from jax.experimental import pallas as pl
from jax.experimental.pallas import tpu as pltpu
from jax.sharding import PartitionSpec as P

LN_EPS = 1e-6
BATCH_AXES = ("inner", "data")
MESH = pl.DeviceIdType.MESH
LANES = 128
GELU_SCALE = 0.7978845608028654
GELU_CUBIC = 0.044715
F32 = jnp.float32
BF16 = jnp.bfloat16
NT = (((1,), (1,)), ((), ()))
NN = (((1,), (0,)), ((), ()))
TN = (((0,), (0,)), ((), ()))
VMEM_BYTES = 40600 * 1000
ROWS = 192
LATE = 3


def dot(a, b, dims):
    return lax.dot_general(a, b, dims, preferred_element_type=F32)


def normalize(stream):
    mean_val = jnp.mean(stream, axis=-1, keepdims=True)
    centered = stream - mean_val
    variance = jnp.mean(centered * centered, axis=-1, keepdims=True)
    rstd = lax.rsqrt(variance + LN_EPS)
    return centered * rstd, rstd


def gelu_parts(pre_half):
    square = pre_half * pre_half
    tanh_val = jnp.tanh(pre_half * (2.0 * GELU_SCALE + (8.0 * GELU_SCALE * GELU_CUBIC) * square))
    return square, tanh_val, 1.0 + tanh_val


AFTER_BACKWARD = [[], [(0, 0)], [(0, 1)], [(0, 2), (1, 0)], [(1, 1), (0, 3)], [(1, 2), (0, 4)], [(0, 5), (2, 1), (1, 3), (0, 6)], []]
BEFORE_HEAD = [(1, 5), (0, 7), (2, 3), (1, 6), (2, 5), (1, 4), (1, 7), (2, 2), (2, 6), (2, 0), (2, 4), (2, 7), (3, 5), (3, 6), (3, 7)]
AFTER_HEAD = [(3, 4), (3, 3), (4, 7), (3, 1), (4, 5), (4, 4), (3, 2), (5, 7), (4, 6)]
BEFORE_UPDATE = [[], [(5, 4), (5, 5), (3, 0), (5, 6)], [(4, 3), (4, 1)], [(5, 3), (4, 2)], [(4, 0)]]
AFTER_UPDATE = [[], [], [], [], [(5, 2)]]
AT_END = [(5, 1), (5, 0)]


def update(layer, slot, rate, coef, sums, old, new, w_in, w_out):
    dim, mlp_dim = w_in.shape
    half = mlp_dim // LANES * dim
    for start in range(0, mlp_dim, LANES):
        lanes = slice(start, start + LANES)
        for base, w_old, m_old, w_new, m_new, w_bf, scale in (
                (0, old[0], old[1], new[0], new[1], w_in, 0.5), (half, old[2], old[3], new[2], new[3], w_out, 1.0)):
            row = base + start // LANES * dim
            moment = coef * m_old[layer, :, lanes] + sums[layer, row:row + dim].astype(F32)
            m_new[slot, :, lanes] = moment
            weight = w_old[layer, :, lanes] - rate * moment
            w_new[slot, :, lanes] = weight
            w_bf[:, lanes] = (weight * scale).astype(BF16)


def next_block(stream, w_in, w_out):
    for start in range(0, stream.shape[0], ROWS):
        part = slice(start, start + ROWS)
        stream_in = stream[part]
        pre_half = dot(normalize(stream_in)[0].astype(BF16), w_in[...], NN)
        out = (pre_half * gelu_parts(pre_half)[2]).astype(BF16)
        stream[part] = stream_in + dot(out, w_out[...], NT)


def step_kernel(n_shards,
                x_hbm, x_next_hbm, label_hbm, rate_hbm, coef_hbm, w_in_hbm, w_out_hbm, w_head_hbm, m_in_hbm, m_out_hbm, m_head_hbm,
                w_in_ref, w_out_ref, w_head_ref, m_in_ref, m_out_ref, m_head_ref, sums, stream,
                d_stream, x_hat, acts, pre_acts, hidden, d_branch, d_pre, w_in, w_out,
                grads, recv0, recv1, recv2, head_send, head_recv,
                x_ref, x_next_ref, label_ref, rate_ref, coef_ref,
                load_sem, mom_sem, small_sem, send_sem, recv_sem, head_send_sem, head_recv_sem):
    layers, tokens, mlp_dim = pre_acts.shape
    dim = stream.shape[1]
    classes = w_head_ref.shape[1]
    chunks = mlp_dim // LANES
    half = chunks * dim
    quarter, eighth = half // 4, half // 8
    parts = [slice(start, start + ROWS) for start in range(0, tokens, ROWS)]
    inner, core = lax.axis_index("inner"), lax.axis_index("data")
    y, x = inner // 2, inner % 2
    peer_core = (inner, 1 - core)
    peer_x = (inner + 1 - 2 * x, core)
    peer_y = (inner + 2 - 4 * y, core)
    barrier = pltpu.get_barrier_semaphore()
    me = inner * 2 + core

    def load(layer):
        return (pltpu.make_async_copy(w_in_hbm.at[layer], w_in_ref.at[layer], load_sem.at[layer % 4, 0]),
                pltpu.make_async_copy(w_out_hbm.at[layer], w_out_ref.at[layer], load_sem.at[layer % 4, 1]))

    mom_loads = (pltpu.make_async_copy(w_head_hbm, w_head_ref, mom_sem.at[0]),
                 pltpu.make_async_copy(m_head_hbm, m_head_ref, mom_sem.at[1]),
                 pltpu.make_async_copy(m_in_hbm, m_in_ref, mom_sem.at[2]),
                 pltpu.make_async_copy(m_out_hbm, m_out_ref, mom_sem.at[3]))

    small_loads = [pltpu.make_async_copy(src, dst, small_sem.at[i]) for i, (src, dst) in enumerate(
        ((x_hbm, x_ref), (label_hbm, label_ref), (rate_hbm, rate_ref), (coef_hbm, coef_ref), (x_next_hbm, x_next_ref)))]

    small_loads[0].start()
    for copy in load(0) + load(1):
        copy.start()
    for step in range(1, n_shards):
        other = (me + step) % n_shards
        pl.semaphore_signal(barrier, inc=1, device_id=(other // 2, other % 2), device_id_type=MESH)
    small_loads[0].wait()
    stream[...] = x_ref[0].astype(F32).T

    def forward(pair, carry):
        first = 2 * pair
        for copy in load(first) + load(first + 1):
            copy.wait()

        @pl.when(first + 2 < layers)
        def _():
            for copy in load(first + 2) + load(first + 3):
                copy.start()

        @pl.when(first + 2 >= layers)
        def _():
            for copy in small_loads[1:] + [mom_loads[0]]:
                copy.start()

        for layer in (first, first + 1):
            w_in[layer] = (0.5 * w_in_ref[layer]).astype(BF16)
            w_out[layer] = w_out_ref[layer].astype(BF16)
        for layer in (first, first + 1):
            for part in parts:
                stream_in = stream[part]
                normed, rstd = normalize(stream_in)
                x_hat[layer, part, 0:dim] = normed
                x_hat[layer, part, dim:dim + 1] = rstd
                pre_half = dot(normed.astype(BF16), w_in[layer], NN)
                pre_acts[layer, part] = pre_half
                out = (pre_half * gelu_parts(pre_half)[2]).astype(BF16)
                stream[part] = stream_in + dot(out, w_out[layer], NT)
        return carry

    lax.fori_loop(0, layers // 2, forward, 0)
    for copy in mom_loads[1:]:
        copy.start()

    pooled = (jnp.sum(stream[...], axis=0, keepdims=True) * (1.0 / tokens)).astype(BF16)
    for copy in small_loads[1:] + [mom_loads[0]]:
        copy.wait()
    w_head = w_head_ref[...].astype(BF16)
    pooled_rows = jnp.broadcast_to(pooled.astype(F32), (16, dim)).astype(BF16)
    logits = dot(pooled_rows, w_head, NN)
    peak = jnp.max(logits, axis=-1, keepdims=True)
    expd = jnp.exp(logits - peak)
    probs = expd / jnp.sum(expd, axis=-1, keepdims=True)
    class_ids = lax.broadcasted_iota(jnp.int32, logits.shape, 1)
    targets = jnp.where(class_ids == label_ref[...], 1.0, 0.0)
    d_logits = ((probs - targets) * (1.0 / n_shards)).astype(BF16)
    d_pooled = dot(d_logits, w_head, NT).astype(BF16).astype(F32) / tokens
    d_stream[...] = jnp.broadcast_to(d_pooled[0:1], d_stream.shape)
    head_send[...] = jnp.zeros_like(head_send)
    d_logits = d_logits.astype(F32)
    for chunk in range(8):
        wide = min(LANES, classes - chunk * LANES)
        head_send[chunk:chunk + 1, 0:wide] = d_logits[0:1, chunk * LANES:chunk * LANES + wide]
    pooled = pooled.astype(F32)
    head_send[8:9, :] = pooled[:, 0:LANES]
    head_send[9:10, 0:dim - LANES] = pooled[:, LANES:dim]
    head_recv[0] = head_send[...]

    pl.semaphore_wait(barrier, n_shards - 1)

    def head_copy(step):
        other = (me + step) % n_shards
        return pltpu.make_async_remote_copy(
            src_ref=head_send, dst_ref=head_recv.at[step], send_sem=head_send_sem.at[0],
            recv_sem=head_recv_sem.at[0], device_id=(other // 2, other % 2), device_id_type=MESH)

    for step in range(1, n_shards):
        head_copy(step).start()

    def all_head_copies():
        others = head_recv.at[pl.ds(1, n_shards - 1)]
        return pltpu.make_async_remote_copy(
            src_ref=others, dst_ref=others, send_sem=head_send_sem.at[0],
            recv_sem=head_recv_sem.at[0], device_id=peer_core, device_id_type=MESH)

    mine = half * core
    place_a, place_b = mine, mine + half // 2

    def remote(src, dst, layer, stage, device):
        near = 0 if stage in (0, 5) else 1
        return pltpu.make_async_remote_copy(
            src_ref=src, dst_ref=dst, send_sem=send_sem.at[layer, near], recv_sem=recv_sem.at[layer, stage],
            device_id=device, device_id_type=MESH)

    def copies(stage, layer):
        def grad(start, size):
            return grads.at[layer, pl.ds(start, size)]

        def total(start, size):
            return sums.at[layer, pl.ds(start, size)]

        if stage == 0:
            return [remote(grad(half * (1 - core), half), recv0.at[layer], layer, stage, peer_core)]
        if stage == 1:
            return [remote(grad(place_a + quarter * (1 - x), quarter), recv1.at[layer, 0], layer, stage, peer_x),
                    remote(grad(place_b + quarter * (1 - y), quarter), recv1.at[layer, 1], layer, stage, peer_y)]
        if stage == 2:
            return [remote(grad(place_a + quarter * x + eighth * (1 - y), eighth), recv2.at[layer, 0], layer, stage, peer_y),
                    remote(grad(place_b + quarter * y + eighth * (1 - x), eighth), recv2.at[layer, 1], layer, stage, peer_x)]
        if stage == 3:
            spot_a = total(place_a + quarter * x + eighth * y, eighth)
            spot_b = total(place_b + quarter * y + eighth * x, eighth)
            return [remote(spot_a, spot_a, layer, stage, peer_y), remote(spot_b, spot_b, layer, stage, peer_x)]
        if stage == 4:
            spot_a = total(place_a + quarter * x, quarter)
            spot_b = total(place_b + quarter * y, quarter)
            return [remote(spot_a, spot_a, layer, stage, peer_x), remote(spot_b, spot_b, layer, stage, peer_y)]
        spot = total(mine, half)
        return [remote(spot, spot, layer, stage, peer_core)]

    def add(layer, dst, start, size, other):
        dst[layer, pl.ds(start, size)] = (
            grads[layer, pl.ds(start, size)].astype(F32) + other[...].astype(F32)).astype(BF16)

    def start(stage, turn):
        for copy in copies(stage, layers - 1 - turn):
            copy.start()

    def advance(stage, turn):
        layer = layers - 1 - turn
        size = (half, 2 * quarter, 2 * eighth, 2 * eighth, 2 * quarter, half)[stage]
        spot = grads.at[layer, pl.ds(0, size)]
        remote(spot, spot, layer, stage, peer_core).wait_recv()
        if stage == 0:
            add(layer, grads, mine, half, recv0.at[layer])
        elif stage == 1:
            add(layer, grads, place_a + quarter * x, quarter, recv1.at[layer, 0])
            add(layer, grads, place_b + quarter * y, quarter, recv1.at[layer, 1])
        elif stage == 2:
            add(layer, sums, place_a + quarter * x + eighth * y, eighth, recv2.at[layer, 0])
            add(layer, sums, place_b + quarter * y + eighth * x, eighth, recv2.at[layer, 1])
        if stage < 5:
            start(stage + 1, turn)

    def run(steps):
        for step in steps:
            advance(*step)

    def run_at(index, table):
        for at, steps in enumerate(table):
            if steps:
                pl.when(index == at)(functools.partial(run, steps))

    def backward(turn, carry):
        layer = layers - 1 - turn
        for part in (slice(0, tokens),):
            branch = d_stream[part].astype(BF16)
            d_branch[part] = branch
            normed = x_hat[layer, part, 0:dim]
            acts[part] = normed.astype(BF16)
            pre_half = pre_acts[layer, part]
            square, tanh_val, twice_cdf = gelu_parts(pre_half)
            hidden[part] = (pre_half * twice_cdf).astype(BF16)
            slope = twice_cdf + ((1.0 - tanh_val * tanh_val) * pre_half) * (
                2.0 * GELU_SCALE + (24.0 * GELU_SCALE * GELU_CUBIC) * square)
            d_hidden = dot(branch, w_out[layer], NN).astype(BF16).astype(F32)
            d_pre_part = (d_hidden * slope).astype(BF16)
            d_pre[part] = d_pre_part
            d_act = dot(d_pre_part, w_in[layer], NT).astype(BF16).astype(F32)
            mean_d = jnp.mean(d_act, axis=-1, keepdims=True)
            mean_dx = jnp.mean(d_act * normed, axis=-1, keepdims=True)
            d_stream[part] = d_stream[part] + x_hat[layer, part, dim:dim + 1] * (d_act - mean_d - normed * mean_dx)
        g_in = (0.5 * dot(acts[...], d_pre[...], TN)).astype(BF16)
        g_out = dot(d_branch[...], hidden[...], TN).astype(BF16)
        for chunk in range(chunks):
            grads[layer, chunk * dim:(chunk + 1) * dim] = g_in[:, chunk * LANES:(chunk + 1) * LANES]
            grads[layer, half + chunk * dim:half + (chunk + 1) * dim] = g_out[:, chunk * LANES:(chunk + 1) * LANES]
        start(0, turn)
        run_at(turn, AFTER_BACKWARD)
        return carry

    lax.fori_loop(0, layers, backward, 0)
    last = layers - 1
    run(BEFORE_HEAD)

    rate, coef = rate_ref[...], coef_ref[...]
    all_head_copies().wait_recv()
    for copy in mom_loads[1:]:
        copy.wait()
    columns = []
    for device in range(n_shards):
        turned = head_recv[device, 8:16, :].T
        columns.append(jnp.concatenate([turned[:, 0:1], turned[0:dim - LANES, 1:2]], axis=0))
    for chunk in range(8):
        wide = min(LANES, classes - chunk * LANES)
        lanes = slice(chunk * LANES, chunk * LANES + wide)
        total_head = None
        for device in range(n_shards):
            product = columns[device] * head_recv[device, chunk:chunk + 1, 0:wide]
            product = product.astype(BF16).astype(F32)
            total_head = product if total_head is None else total_head + product
        moment = coef * m_head_ref[:, lanes] + total_head
        m_head_ref[:, lanes] = moment
        w_head_ref[:, lanes] = w_head_ref[:, lanes] - rate * moment
    stream[...] = x_next_ref[0].astype(F32).T

    run(AFTER_HEAD)

    def next_forward(layer, carry):
        run_at(layer, BEFORE_UPDATE)
        update(layer, layer, rate, coef, sums, (w_in_ref, m_in_ref, w_out_ref, m_out_ref), (w_in_ref, m_in_ref, w_out_ref, m_out_ref),
               w_in.at[layer], w_out.at[layer])
        run_at(layer, AFTER_UPDATE)
        next_block(stream, w_in.at[layer], w_out.at[layer])
        return carry

    lax.fori_loop(0, layers - LATE, next_forward, 0)
    run(AT_END)

    def finish_all(layer, carry):
        for stage, size in ((0, 2 * half), (1, 3 * half // 2)):
            spot = grads.at[layer, pl.ds(0, size)]
            remote(spot, spot, layer, stage, peer_core).wait_send()
        return carry

    lax.fori_loop(0, layers, finish_all, 0)
    all_head_copies().wait_send()


def store_kernel(rate_ref, coef_ref, w_in_ref, w_out_ref, w_head_ref, m_in_ref, m_out_ref, m_head_ref, sums, stream_ref,
                 w_in_out, w_out_out, w_head_out, m_in_out, m_out_out, m_head_out, logits_out,
                 stream, w_in_late, m_in_late, w_out_late, m_out_late, w_in, w_out, logits, early_sem, late_sem):
    layers = w_in_ref.shape[0]
    tokens, dim = stream.shape
    early = layers - LATE
    rate, coef = rate_ref[...], coef_ref[...]
    old = (w_in_ref, m_in_ref, w_out_ref, m_out_ref)
    new = (w_in_late, m_in_late, w_out_late, m_out_late)
    outs = (w_in_out, m_in_out, w_out_out, m_out_out)
    copies = [pltpu.make_async_copy(src.at[pl.ds(0, early)], dst.at[pl.ds(0, early)], early_sem.at[i])
              for i, (src, dst) in enumerate(zip(old, outs))]
    copies.append(pltpu.make_async_copy(w_head_ref, w_head_out, early_sem.at[4]))
    copies.append(pltpu.make_async_copy(m_head_ref, m_head_out, early_sem.at[5]))
    for copy in copies:
        copy.start()
    stream[...] = stream_ref[...]

    def late_copies(step):
        return [pltpu.make_async_copy(src.at[step], dst.at[early + step], late_sem.at[step, i])
                for i, (src, dst) in enumerate(zip(new, outs))]

    def late_layer(step, carry):
        update(early + step, step, rate, coef, sums, old, new, w_in, w_out)
        for copy in late_copies(step):
            copy.start()
        next_block(stream, w_in, w_out)
        return carry

    lax.fori_loop(0, LATE, late_layer, 0)
    pooled = jnp.sum(stream[...], axis=0, keepdims=True) * (1.0 / tokens)
    pooled = jnp.broadcast_to(pooled, (16, dim)).astype(BF16)
    logits[...] = dot(pooled, w_head_ref[...].astype(BF16), NN)[0:1]
    copies.append(pltpu.make_async_copy(logits, logits_out, early_sem.at[6]))
    copies[-1].start()
    for step in range(LATE):
        copies += late_copies(step)
    for copy in copies:
        copy.wait()


def solution(mesh):
    batch_spec = P(BATCH_AXES)
    repl_spec = P()
    n_shards = mesh.shape["inner"] * mesh.shape["data"]

    def device_step(x_t, labels_t, x_next, w_in, w_out, w_head, mom_in, mom_out, mom_head, learn_rate, mom_coef):
        layers, dim, mlp_dim = w_in.shape
        tokens = x_t.shape[1]
        classes = w_head.shape[1]
        half = mlp_dim // LANES * dim
        vmem = pl.BlockSpec(memory_space=pltpu.VMEM)
        hbm = pl.BlockSpec(memory_space=pl.ANY)
        shapes = [(layers, dim, mlp_dim), (layers, dim, mlp_dim), (dim, classes)] * 2
        rate, coef = learn_rate.reshape(1, 1), mom_coef.reshape(1, 1)
        results = pl.pallas_call(
            functools.partial(step_kernel, n_shards),
            out_shape=tuple(pltpu.VMEM(shape, F32) for shape in shapes) + (pltpu.VMEM((layers, 2 * half, LANES), BF16), pltpu.VMEM((tokens, dim), F32)),
            in_specs=[hbm] * 11,
            out_specs=(vmem,) * 8,
            scratch_shapes=[
                pltpu.VMEM((tokens, dim), F32),
                pltpu.VMEM((layers, tokens, dim + 1), F32),
                pltpu.VMEM((tokens, dim), BF16),
                pltpu.VMEM((layers, tokens, mlp_dim), F32),
                pltpu.VMEM((tokens, mlp_dim), BF16),
                pltpu.VMEM((tokens, dim), BF16),
                pltpu.VMEM((tokens, mlp_dim), BF16),
                pltpu.VMEM((layers, dim, mlp_dim), BF16),
                pltpu.VMEM((layers, dim, mlp_dim), BF16),
                pltpu.VMEM((layers, 2 * half, LANES), BF16),
                pltpu.VMEM((layers, half, LANES), BF16),
                pltpu.VMEM((layers, 2, half // 4, LANES), BF16),
                pltpu.VMEM((layers, 2, half // 8, LANES), BF16),
                pltpu.VMEM((16, LANES), F32),
                pltpu.VMEM((n_shards, 16, LANES), F32),
                pltpu.VMEM((1, dim, tokens), BF16),
                pltpu.VMEM((1, dim, tokens), BF16),
                pltpu.VMEM((1, 1), jnp.int32),
                pltpu.VMEM((1, 1), F32),
                pltpu.VMEM((1, 1), F32),
                pltpu.SemaphoreType.DMA((4, 2)),
                pltpu.SemaphoreType.DMA((4,)),
                pltpu.SemaphoreType.DMA((5,)),
                pltpu.SemaphoreType.DMA((layers, 2)),
                pltpu.SemaphoreType.DMA((layers, 6)),
                pltpu.SemaphoreType.DMA((1,)),
                pltpu.SemaphoreType.DMA((1,)),
            ],
            compiler_params=pltpu.CompilerParams(collective_id=0, has_side_effects=True, vmem_limit_bytes=VMEM_BYTES),
            name="step_kernel",
        )(x_t.transpose(0, 2, 1), x_next.transpose(0, 2, 1), labels_t.reshape(1, 1), rate, coef,
          w_in, w_out.transpose(0, 2, 1), w_head, mom_in, mom_out.transpose(0, 2, 1), mom_head)
        late = pltpu.VMEM((LATE, dim, mlp_dim), F32)
        w_in_new, w_out_new, w_head_new, m_in_new, m_out_new, m_head_new, logits = pl.pallas_call(
            store_kernel,
            out_shape=tuple(jax.ShapeDtypeStruct(shape, F32) for shape in shapes + [(1, classes)]),
            in_specs=[vmem] * 10,
            out_specs=(hbm,) * 7,
            scratch_shapes=[
                pltpu.VMEM((tokens, dim), F32), late, late, late, late,
                pltpu.VMEM((dim, mlp_dim), BF16), pltpu.VMEM((dim, mlp_dim), BF16), pltpu.VMEM((1, classes), F32),
                pltpu.SemaphoreType.DMA((7,)), pltpu.SemaphoreType.DMA((LATE, 4)),
            ],
            compiler_params=pltpu.CompilerParams(vmem_limit_bytes=11 * 1000 * 1000),
            name="store_kernel",
        )(rate, coef, *results)
        return (logits, w_in_new, w_out_new.transpose(0, 2, 1), w_head_new,
                m_in_new, m_out_new.transpose(0, 2, 1), m_head_new)

    return jax.shard_map(device_step, mesh=mesh, in_specs=(batch_spec, batch_spec, batch_spec) + (repl_spec,) * 8, out_specs=(batch_spec,) + (repl_spec,) * 6, check_vma=False)
```

```python
import functools

import jax
import jax.numpy as jnp
from jax import lax
from jax.experimental import pallas as pl
from jax.experimental.pallas import tpu as pltpu
from jax.sharding import PartitionSpec as P

LN_EPS = 1e-6
BATCH_AXES = ("inner", "data")
MESH = pl.DeviceIdType.MESH
LANES = 128
GELU_SCALE = 0.7978845608028654
GELU_CUBIC = 0.044715
F32 = jnp.float32
BF16 = jnp.bfloat16
NT = (((1,), (1,)), ((), ()))
NN = (((1,), (0,)), ((), ()))
TN = (((0,), (0,)), ((), ()))
VMEM_BYTES = 40600 * 1000
ROWS = 192
LATE = 3


def dot(a, b, dims):
    return lax.dot_general(a, b, dims, preferred_element_type=F32)


def normalize(stream):
    mean_val = jnp.mean(stream, axis=-1, keepdims=True)
    centered = stream - mean_val
    variance = jnp.mean(centered * centered, axis=-1, keepdims=True)
    rstd = lax.rsqrt(variance + LN_EPS)
    return centered * rstd, rstd


def gelu_parts(pre_half):
    square = pre_half * pre_half
    tanh_val = jnp.tanh(pre_half * (2.0 * GELU_SCALE + (8.0 * GELU_SCALE * GELU_CUBIC) * square))
    return square, tanh_val, 1.0 + tanh_val


AFTER_BACKWARD = [[], [(0, 0)], [(0, 1)], [(0, 2), (1, 0)], [(1, 1), (0, 3)], [(1, 2), (0, 4)], [(0, 5), (2, 1), (1, 3), (0, 6)], []]
BEFORE_HEAD = [(1, 5), (0, 7), (2, 3), (1, 6), (2, 5), (1, 4), (1, 7), (2, 2), (2, 6), (2, 0), (2, 4), (2, 7), (3, 5), (3, 6), (3, 7)]
AFTER_HEAD = [(3, 4), (3, 3), (4, 7), (3, 1), (4, 5), (4, 4), (3, 2), (5, 7), (4, 6)]
BEFORE_UPDATE = [[], [(5, 4), (5, 5), (3, 0), (5, 6)], [(4, 3), (4, 1)], [(5, 3), (4, 2)], [(4, 0)]]
AFTER_UPDATE = [[], [], [], [], [(5, 2)]]
AT_END = [(5, 1), (5, 0)]


def update(layer, slot, rate, coef, sums, old, new, w_in, w_out):
    dim, mlp_dim = w_in.shape
    half = mlp_dim // LANES * dim
    for start in range(0, mlp_dim, LANES):
        lanes = slice(start, start + LANES)
        for base, w_old, m_old, w_new, m_new, w_bf, scale in (
                (0, old[0], old[1], new[0], new[1], w_in, 0.5), (half, old[2], old[3], new[2], new[3], w_out, 1.0)):
            row = base + start // LANES * dim
            moment = coef * m_old[layer, :, lanes] + sums[layer, row:row + dim].astype(F32)
            m_new[slot, :, lanes] = moment
            weight = w_old[layer, :, lanes] - rate * moment
            w_new[slot, :, lanes] = weight
            w_bf[:, lanes] = (weight * scale).astype(BF16)


def next_block(stream, w_in, w_out):
    for start in range(0, stream.shape[0], ROWS):
        part = slice(start, start + ROWS)
        stream_in = stream[part]
        pre_half = dot(normalize(stream_in)[0].astype(BF16), w_in[...], NN)
        out = (pre_half * gelu_parts(pre_half)[2]).astype(BF16)
        stream[part] = stream_in + dot(out, w_out[...], NT)


def step_kernel(n_shards,
                x_hbm, x_next_hbm, label_hbm, rate_hbm, coef_hbm, w_in_hbm, w_out_hbm, w_head_hbm, m_in_hbm, m_out_hbm, m_head_hbm,
                w_in_ref, w_out_ref, w_head_ref, m_in_ref, m_out_ref, m_head_ref, sums, stream,
                d_stream, x_hat, acts, pre_acts, hidden, d_branch, d_pre, w_in, w_out,
                grads, recv0, recv1, recv2, head_send, head_recv,
                x_ref, x_next_ref, label_ref, rate_ref, coef_ref,
                load_sem, mom_sem, small_sem, send_sem, recv_sem, head_send_sem, head_recv_sem):
    layers, tokens, mlp_dim = pre_acts.shape
    dim = stream.shape[1]
    classes = w_head_ref.shape[1]
    chunks = mlp_dim // LANES
    half = chunks * dim
    quarter, eighth = half // 4, half // 8
    parts = [slice(start, start + ROWS) for start in range(0, tokens, ROWS)]
    inner, core = lax.axis_index("inner"), lax.axis_index("data")
    y, x = inner // 2, inner % 2
    peer_core = (inner, 1 - core)
    peer_x = (inner + 1 - 2 * x, core)
    peer_y = (inner + 2 - 4 * y, core)
    barrier = pltpu.get_barrier_semaphore()
    me = inner * 2 + core

    def load(layer):
        return (pltpu.make_async_copy(w_in_hbm.at[layer], w_in_ref.at[layer], load_sem.at[layer % 4, 0]),
                pltpu.make_async_copy(w_out_hbm.at[layer], w_out_ref.at[layer], load_sem.at[layer % 4, 1]))

    mom_loads = (pltpu.make_async_copy(w_head_hbm, w_head_ref, mom_sem.at[0]),
                 pltpu.make_async_copy(m_head_hbm, m_head_ref, mom_sem.at[1]),
                 pltpu.make_async_copy(m_in_hbm, m_in_ref, mom_sem.at[2]),
                 pltpu.make_async_copy(m_out_hbm, m_out_ref, mom_sem.at[3]))

    small_loads = [pltpu.make_async_copy(src, dst, small_sem.at[i]) for i, (src, dst) in enumerate(
        ((x_hbm, x_ref), (label_hbm, label_ref), (rate_hbm, rate_ref), (coef_hbm, coef_ref), (x_next_hbm, x_next_ref)))]

    small_loads[0].start()
    for copy in load(0) + load(1):
        copy.start()
    for step in range(1, n_shards):
        other = (me + step) % n_shards
        pl.semaphore_signal(barrier, inc=1, device_id=(other // 2, other % 2), device_id_type=MESH)
    small_loads[0].wait()
    stream[...] = x_ref[0].astype(F32).T

    def forward(pair, carry):
        first = 2 * pair
        for copy in load(first) + load(first + 1):
            copy.wait()

        @pl.when(first + 2 < layers)
        def _():
            for copy in load(first + 2) + load(first + 3):
                copy.start()

        @pl.when(first + 2 >= layers)
        def _():
            for copy in small_loads[1:] + [mom_loads[0]]:
                copy.start()

        for layer in (first, first + 1):
            w_in[layer] = (0.5 * w_in_ref[layer]).astype(BF16)
            w_out[layer] = w_out_ref[layer].astype(BF16)
        for layer in (first, first + 1):
            for part in parts:
                stream_in = stream[part]
                normed, rstd = normalize(stream_in)
                x_hat[layer, part, 0:dim] = normed
                x_hat[layer, part, dim:dim + 1] = rstd
                pre_half = dot(normed.astype(BF16), w_in[layer], NN)
                pre_acts[layer, part] = pre_half
                out = (pre_half * gelu_parts(pre_half)[2]).astype(BF16)
                stream[part] = stream_in + dot(out, w_out[layer], NT)
        return carry

    lax.fori_loop(0, layers // 2, forward, 0)
    for copy in mom_loads[1:]:
        copy.start()

    pooled = (jnp.sum(stream[...], axis=0, keepdims=True) * (1.0 / tokens)).astype(BF16)
    for copy in small_loads[1:] + [mom_loads[0]]:
        copy.wait()
    w_head = w_head_ref[...].astype(BF16)
    pooled_rows = jnp.broadcast_to(pooled.astype(F32), (16, dim)).astype(BF16)
    logits = dot(pooled_rows, w_head, NN)
    peak = jnp.max(logits, axis=-1, keepdims=True)
    expd = jnp.exp(logits - peak)
    probs = expd / jnp.sum(expd, axis=-1, keepdims=True)
    class_ids = lax.broadcasted_iota(jnp.int32, logits.shape, 1)
    targets = jnp.where(class_ids == label_ref[...], 1.0, 0.0)
    d_logits = ((probs - targets) * (1.0 / n_shards)).astype(BF16)
    d_pooled = dot(d_logits, w_head, NT).astype(BF16).astype(F32) / tokens
    d_stream[...] = jnp.broadcast_to(d_pooled[0:1], d_stream.shape)
    head_send[...] = jnp.zeros_like(head_send)
    d_logits = d_logits.astype(F32)
    for chunk in range(8):
        wide = min(LANES, classes - chunk * LANES)
        head_send[chunk:chunk + 1, 0:wide] = d_logits[0:1, chunk * LANES:chunk * LANES + wide]
    pooled = pooled.astype(F32)
    head_send[8:9, :] = pooled[:, 0:LANES]
    head_send[9:10, 0:dim - LANES] = pooled[:, LANES:dim]
    head_recv[0] = head_send[...]


    def head_copy(step):
        other = (me + step) % n_shards
        return pltpu.make_async_remote_copy(
            src_ref=head_send, dst_ref=head_recv.at[step], send_sem=head_send_sem.at[0],
            recv_sem=head_recv_sem.at[0], device_id=(other // 2, other % 2), device_id_type=MESH)

    def all_head_copies():
        others = head_recv.at[pl.ds(1, n_shards - 1)]
        return pltpu.make_async_remote_copy(
            src_ref=others, dst_ref=others, send_sem=head_send_sem.at[0],
            recv_sem=head_recv_sem.at[0], device_id=peer_core, device_id_type=MESH)

    mine = half * core
    place_a, place_b = mine, mine + half // 2

    def remote(src, dst, layer, stage, device):
        near = 0 if stage in (0, 5) else 1
        return pltpu.make_async_remote_copy(
            src_ref=src, dst_ref=dst, send_sem=send_sem.at[layer, near], recv_sem=recv_sem.at[layer, stage],
            device_id=device, device_id_type=MESH)

    def copies(stage, layer):
        def grad(start, size):
            return grads.at[layer, pl.ds(start, size)]

        def total(start, size):
            return sums.at[layer, pl.ds(start, size)]

        if stage == 0:
            return [remote(grad(half * (1 - core), half), recv0.at[layer], layer, stage, peer_core)]
        if stage == 1:
            return [remote(grad(place_a + quarter * (1 - x), quarter), recv1.at[layer, 0], layer, stage, peer_x),
                    remote(grad(place_b + quarter * (1 - y), quarter), recv1.at[layer, 1], layer, stage, peer_y)]
        if stage == 2:
            return [remote(grad(place_a + quarter * x + eighth * (1 - y), eighth), recv2.at[layer, 0], layer, stage, peer_y),
                    remote(grad(place_b + quarter * y + eighth * (1 - x), eighth), recv2.at[layer, 1], layer, stage, peer_x)]
        if stage == 3:
            spot_a = total(place_a + quarter * x + eighth * y, eighth)
            spot_b = total(place_b + quarter * y + eighth * x, eighth)
            return [remote(spot_a, spot_a, layer, stage, peer_y), remote(spot_b, spot_b, layer, stage, peer_x)]
        if stage == 4:
            spot_a = total(place_a + quarter * x, quarter)
            spot_b = total(place_b + quarter * y, quarter)
            return [remote(spot_a, spot_a, layer, stage, peer_x), remote(spot_b, spot_b, layer, stage, peer_y)]
        spot = total(mine, half)
        return [remote(spot, spot, layer, stage, peer_core)]

    def add(layer, dst, start, size, other):
        dst[layer, pl.ds(start, size)] = (
            grads[layer, pl.ds(start, size)].astype(F32) + other[...].astype(F32)).astype(BF16)

    def start(stage, turn):
        for copy in copies(stage, layers - 1 - turn):
            copy.start()

    def advance(stage, turn):
        layer = layers - 1 - turn
        size = (half, 2 * quarter, 2 * eighth, 2 * eighth, 2 * quarter, half)[stage]
        spot = grads.at[layer, pl.ds(0, size)]
        remote(spot, spot, layer, stage, peer_core).wait_recv()
        if stage == 0:
            add(layer, grads, mine, half, recv0.at[layer])
        elif stage == 1:
            add(layer, grads, place_a + quarter * x, quarter, recv1.at[layer, 0])
            add(layer, grads, place_b + quarter * y, quarter, recv1.at[layer, 1])
        elif stage == 2:
            add(layer, sums, place_a + quarter * x + eighth * y, eighth, recv2.at[layer, 0])
            add(layer, sums, place_b + quarter * y + eighth * x, eighth, recv2.at[layer, 1])
        if stage < 5:
            start(stage + 1, turn)

    def run(steps):
        for step in steps:
            advance(*step)

    def run_at(index, table):
        for at, steps in enumerate(table):
            if steps:
                pl.when(index == at)(functools.partial(run, steps))

    def block_gradients(layer):
        for part in (slice(0, tokens),):
            branch = d_stream[part].astype(BF16)
            d_branch[part] = branch
            normed = x_hat[layer, part, 0:dim]
            acts[part] = normed.astype(BF16)
            pre_half = pre_acts[layer, part]
            square, tanh_val, twice_cdf = gelu_parts(pre_half)
            hidden[part] = (pre_half * twice_cdf).astype(BF16)
            slope = twice_cdf + ((1.0 - tanh_val * tanh_val) * pre_half) * (
                2.0 * GELU_SCALE + (24.0 * GELU_SCALE * GELU_CUBIC) * square)
            d_hidden = dot(branch, w_out[layer], NN).astype(BF16).astype(F32)
            d_pre_part = (d_hidden * slope).astype(BF16)
            d_pre[part] = d_pre_part
            d_act = dot(d_pre_part, w_in[layer], NT).astype(BF16).astype(F32)
            mean_d = jnp.mean(d_act, axis=-1, keepdims=True)
            mean_dx = jnp.mean(d_act * normed, axis=-1, keepdims=True)
            d_stream[part] = d_stream[part] + x_hat[layer, part, dim:dim + 1] * (d_act - mean_d - normed * mean_dx)
        g_in = (0.5 * dot(acts[...], d_pre[...], TN)).astype(BF16)
        g_out = dot(d_branch[...], hidden[...], TN).astype(BF16)
        for chunk in range(chunks):
            grads[layer, chunk * dim:(chunk + 1) * dim] = g_in[:, chunk * LANES:(chunk + 1) * LANES]
            grads[layer, half + chunk * dim:half + (chunk + 1) * dim] = g_out[:, chunk * LANES:(chunk + 1) * LANES]

    def backward(turn, carry):
        block_gradients(layers - 1 - turn)
        start(0, turn)
        run_at(turn, AFTER_BACKWARD)
        return carry

    block_gradients(layers - 1)
    pl.semaphore_wait(barrier, n_shards - 1)
    start(0, 0)
    for step in range(1, n_shards):
        head_copy(step).start()
    lax.fori_loop(1, layers, backward, 0)
    last = layers - 1
    run(BEFORE_HEAD)

    rate, coef = rate_ref[...], coef_ref[...]
    all_head_copies().wait_recv()
    for copy in mom_loads[1:]:
        copy.wait()
    columns = []
    for device in range(n_shards):
        turned = head_recv[device, 8:16, :].T
        columns.append(jnp.concatenate([turned[:, 0:1], turned[0:dim - LANES, 1:2]], axis=0))
    for chunk in range(8):
        wide = min(LANES, classes - chunk * LANES)
        lanes = slice(chunk * LANES, chunk * LANES + wide)
        total_head = None
        for device in range(n_shards):
            product = columns[device] * head_recv[device, chunk:chunk + 1, 0:wide]
            product = product.astype(BF16).astype(F32)
            total_head = product if total_head is None else total_head + product
        moment = coef * m_head_ref[:, lanes] + total_head
        m_head_ref[:, lanes] = moment
        w_head_ref[:, lanes] = w_head_ref[:, lanes] - rate * moment
    stream[...] = x_next_ref[0].astype(F32).T

    run(AFTER_HEAD)

    def next_forward(layer, carry):
        run_at(layer, BEFORE_UPDATE)
        update(layer, layer, rate, coef, sums, (w_in_ref, m_in_ref, w_out_ref, m_out_ref), (w_in_ref, m_in_ref, w_out_ref, m_out_ref),
               w_in.at[layer], w_out.at[layer])
        run_at(layer, AFTER_UPDATE)
        next_block(stream, w_in.at[layer], w_out.at[layer])
        return carry

    lax.fori_loop(0, layers - LATE, next_forward, 0)
    run(AT_END)

    def finish_all(layer, carry):
        for stage, size in ((0, 2 * half), (1, 3 * half // 2)):
            spot = grads.at[layer, pl.ds(0, size)]
            remote(spot, spot, layer, stage, peer_core).wait_send()
        return carry

    lax.fori_loop(0, layers, finish_all, 0)
    all_head_copies().wait_send()


def store_kernel(rate_ref, coef_ref, w_in_ref, w_out_ref, w_head_ref, m_in_ref, m_out_ref, m_head_ref, sums, stream_ref,
                 w_in_out, w_out_out, w_head_out, m_in_out, m_out_out, m_head_out, logits_out,
                 stream, w_in_late, m_in_late, w_out_late, m_out_late, w_in, w_out, logits, early_sem, late_sem):
    layers = w_in_ref.shape[0]
    tokens, dim = stream.shape
    early = layers - LATE
    rate, coef = rate_ref[...], coef_ref[...]
    old = (w_in_ref, m_in_ref, w_out_ref, m_out_ref)
    new = (w_in_late, m_in_late, w_out_late, m_out_late)
    outs = (w_in_out, m_in_out, w_out_out, m_out_out)
    copies = [pltpu.make_async_copy(src.at[pl.ds(0, early)], dst.at[pl.ds(0, early)], early_sem.at[i])
              for i, (src, dst) in enumerate(zip(old, outs))]
    copies.append(pltpu.make_async_copy(w_head_ref, w_head_out, early_sem.at[4]))
    copies.append(pltpu.make_async_copy(m_head_ref, m_head_out, early_sem.at[5]))
    for copy in copies:
        copy.start()
    stream[...] = stream_ref[...]

    def late_copies(step):
        return [pltpu.make_async_copy(src.at[step], dst.at[early + step], late_sem.at[step, i])
                for i, (src, dst) in enumerate(zip(new, outs))]

    def late_layer(step, carry):
        update(early + step, step, rate, coef, sums, old, new, w_in, w_out)
        for copy in late_copies(step):
            copy.start()
        next_block(stream, w_in, w_out)
        return carry

    lax.fori_loop(0, LATE, late_layer, 0)
    pooled = jnp.sum(stream[...], axis=0, keepdims=True) * (1.0 / tokens)
    pooled = jnp.broadcast_to(pooled, (16, dim)).astype(BF16)
    logits[...] = dot(pooled, w_head_ref[...].astype(BF16), NN)[0:1]
    copies.append(pltpu.make_async_copy(logits, logits_out, early_sem.at[6]))
    copies[-1].start()
    for step in range(LATE):
        copies += late_copies(step)
    for copy in copies:
        copy.wait()


def solution(mesh):
    batch_spec = P(BATCH_AXES)
    repl_spec = P()
    n_shards = mesh.shape["inner"] * mesh.shape["data"]

    def device_step(x_t, labels_t, x_next, w_in, w_out, w_head, mom_in, mom_out, mom_head, learn_rate, mom_coef):
        layers, dim, mlp_dim = w_in.shape
        tokens = x_t.shape[1]
        classes = w_head.shape[1]
        half = mlp_dim // LANES * dim
        vmem = pl.BlockSpec(memory_space=pltpu.VMEM)
        hbm = pl.BlockSpec(memory_space=pl.ANY)
        shapes = [(layers, dim, mlp_dim), (layers, dim, mlp_dim), (dim, classes)] * 2
        rate, coef = learn_rate.reshape(1, 1), mom_coef.reshape(1, 1)
        results = pl.pallas_call(
            functools.partial(step_kernel, n_shards),
            out_shape=tuple(pltpu.VMEM(shape, F32) for shape in shapes) + (pltpu.VMEM((layers, 2 * half, LANES), BF16), pltpu.VMEM((tokens, dim), F32)),
            in_specs=[hbm] * 11,
            out_specs=(vmem,) * 8,
            scratch_shapes=[
                pltpu.VMEM((tokens, dim), F32),
                pltpu.VMEM((layers, tokens, dim + 1), F32),
                pltpu.VMEM((tokens, dim), BF16),
                pltpu.VMEM((layers, tokens, mlp_dim), F32),
                pltpu.VMEM((tokens, mlp_dim), BF16),
                pltpu.VMEM((tokens, dim), BF16),
                pltpu.VMEM((tokens, mlp_dim), BF16),
                pltpu.VMEM((layers, dim, mlp_dim), BF16),
                pltpu.VMEM((layers, dim, mlp_dim), BF16),
                pltpu.VMEM((layers, 2 * half, LANES), BF16),
                pltpu.VMEM((layers, half, LANES), BF16),
                pltpu.VMEM((layers, 2, half // 4, LANES), BF16),
                pltpu.VMEM((layers, 2, half // 8, LANES), BF16),
                pltpu.VMEM((16, LANES), F32),
                pltpu.VMEM((n_shards, 16, LANES), F32),
                pltpu.VMEM((1, dim, tokens), BF16),
                pltpu.VMEM((1, dim, tokens), BF16),
                pltpu.VMEM((1, 1), jnp.int32),
                pltpu.VMEM((1, 1), F32),
                pltpu.VMEM((1, 1), F32),
                pltpu.SemaphoreType.DMA((4, 2)),
                pltpu.SemaphoreType.DMA((4,)),
                pltpu.SemaphoreType.DMA((5,)),
                pltpu.SemaphoreType.DMA((layers, 2)),
                pltpu.SemaphoreType.DMA((layers, 6)),
                pltpu.SemaphoreType.DMA((1,)),
                pltpu.SemaphoreType.DMA((1,)),
            ],
            compiler_params=pltpu.CompilerParams(collective_id=0, has_side_effects=True, vmem_limit_bytes=VMEM_BYTES),
            name="step_kernel",
        )(x_t.transpose(0, 2, 1), x_next.transpose(0, 2, 1), labels_t.reshape(1, 1), rate, coef,
          w_in, w_out.transpose(0, 2, 1), w_head, mom_in, mom_out.transpose(0, 2, 1), mom_head)
        late = pltpu.VMEM((LATE, dim, mlp_dim), F32)
        w_in_new, w_out_new, w_head_new, m_in_new, m_out_new, m_head_new, logits = pl.pallas_call(
            store_kernel,
            out_shape=tuple(jax.ShapeDtypeStruct(shape, F32) for shape in shapes + [(1, classes)]),
            in_specs=[vmem] * 10,
            out_specs=(hbm,) * 7,
            scratch_shapes=[
                pltpu.VMEM((tokens, dim), F32), late, late, late, late,
                pltpu.VMEM((dim, mlp_dim), BF16), pltpu.VMEM((dim, mlp_dim), BF16), pltpu.VMEM((1, classes), F32),
                pltpu.SemaphoreType.DMA((7,)), pltpu.SemaphoreType.DMA((LATE, 4)),
            ],
            compiler_params=pltpu.CompilerParams(vmem_limit_bytes=11 * 1000 * 1000),
            name="store_kernel",
        )(rate, coef, *results)
        return (logits, w_in_new, w_out_new.transpose(0, 2, 1), w_head_new,
                m_in_new, m_out_new.transpose(0, 2, 1), m_head_new)

    return jax.shard_map(device_step, mesh=mesh, in_specs=(batch_spec, batch_spec, batch_spec) + (repl_spec,) * 8, out_specs=(batch_spec,) + (repl_spec,) * 6, check_vma=False)
```

```python
import functools

import jax
import jax.numpy as jnp
from jax import lax
from jax.experimental import pallas as pl
from jax.experimental.pallas import tpu as pltpu
from jax.sharding import PartitionSpec as P

LN_EPS = 1e-6
BATCH_AXES = ("inner", "data")
MESH = pl.DeviceIdType.MESH
LANES = 128
GELU_SCALE = 0.7978845608028654
GELU_CUBIC = 0.044715
F32 = jnp.float32
BF16 = jnp.bfloat16
NT = (((1,), (1,)), ((), ()))
NN = (((1,), (0,)), ((), ()))
TN = (((0,), (0,)), ((), ()))
VMEM_BYTES = 40600 * 1000
ROWS = 192
LATE = 3


def dot(a, b, dims):
    return lax.dot_general(a, b, dims, preferred_element_type=F32)


def normalize(stream):
    mean_val = jnp.mean(stream, axis=-1, keepdims=True)
    centered = stream - mean_val
    variance = jnp.mean(centered * centered, axis=-1, keepdims=True)
    rstd = lax.rsqrt(variance + LN_EPS)
    return centered * rstd, rstd


def gelu_parts(pre_half):
    square = pre_half * pre_half
    tanh_val = jnp.tanh(pre_half * (2.0 * GELU_SCALE + (8.0 * GELU_SCALE * GELU_CUBIC) * square))
    return square, tanh_val, 1.0 + tanh_val


AFTER_BACKWARD = [[], [(0, 0)], [(0, 1)], [(0, 2), (1, 0)], [(1, 1), (0, 3)], [(1, 2), (0, 4)], [(0, 5), (2, 1), (1, 3), (0, 6)], []]
BEFORE_HEAD = [(1, 5), (0, 7), (2, 3), (1, 6), (2, 5), (1, 4), (1, 7), (2, 2), (2, 6), (2, 0), (2, 4), (2, 7), (3, 5), (3, 6), (3, 7)]
AFTER_HEAD = [(3, 4), (3, 3), (4, 7), (3, 1), (4, 5), (4, 4), (3, 2), (5, 7), (4, 6)]
BEFORE_UPDATE = [[], [(5, 4), (5, 5), (3, 0), (5, 6)], [(4, 3), (4, 1)], [(5, 3), (4, 2)], [(4, 0)]]
AFTER_UPDATE = [[], [], [], [], [(5, 2)]]
AT_END = [(5, 1), (5, 0)]


def update(layer, slot, rate, coef, sums, old, new, w_in, w_out):
    dim, mlp_dim = w_in.shape
    half = mlp_dim // LANES * dim
    for start in range(0, mlp_dim, LANES):
        lanes = slice(start, start + LANES)
        for base, w_old, m_old, w_new, m_new, w_bf, scale in (
                (0, old[0], old[1], new[0], new[1], w_in, 0.5), (half, old[2], old[3], new[2], new[3], w_out, 1.0)):
            row = base + start // LANES * dim
            moment = coef * m_old[layer, :, lanes] + sums[layer, row:row + dim].astype(F32)
            m_new[slot, :, lanes] = moment
            weight = w_old[layer, :, lanes] - rate * moment
            w_new[slot, :, lanes] = weight
            w_bf[:, lanes] = (weight * scale).astype(BF16)


def next_block(stream, w_in, w_out):
    for start in range(0, stream.shape[0], ROWS):
        part = slice(start, start + ROWS)
        stream_in = stream[part]
        pre_half = dot(normalize(stream_in)[0].astype(BF16), w_in[...], NN)
        out = (pre_half * gelu_parts(pre_half)[2]).astype(BF16)
        stream[part] = stream_in + dot(out, w_out[...], NT)


def step_kernel(n_shards,
                x_hbm, x_next_hbm, label_hbm, rate_hbm, coef_hbm, w_in_hbm, w_out_hbm, w_head_hbm, m_in_hbm, m_out_hbm, m_head_hbm,
                w_in_ref, w_out_ref, w_head_ref, m_in_ref, m_out_ref, m_head_ref, sums, stream,
                d_stream, x_hat, acts, pre_acts, hidden, d_branch, d_pre, w_in, w_out,
                grads, recv0, recv1, recv2, head_send, head_recv,
                x_ref, x_next_ref, label_ref, rate_ref, coef_ref,
                load_sem, mom_sem, small_sem, send_sem, recv_sem, head_send_sem, head_recv_sem):
    layers, tokens, mlp_dim = pre_acts.shape
    dim = stream.shape[1]
    classes = w_head_ref.shape[1]
    chunks = mlp_dim // LANES
    half = chunks * dim
    quarter, eighth = half // 4, half // 8
    parts = [slice(start, start + ROWS) for start in range(0, tokens, ROWS)]
    inner, core = lax.axis_index("inner"), lax.axis_index("data")
    y, x = inner // 2, inner % 2
    peer_core = (inner, 1 - core)
    peer_x = (inner + 1 - 2 * x, core)
    peer_y = (inner + 2 - 4 * y, core)
    barrier = pltpu.get_barrier_semaphore()
    me = inner * 2 + core

    def load(layer):
        return (pltpu.make_async_copy(w_in_hbm.at[layer], w_in_ref.at[layer], load_sem.at[layer % 4, 0]),
                pltpu.make_async_copy(w_out_hbm.at[layer], w_out_ref.at[layer], load_sem.at[layer % 4, 1]))

    mom_loads = (pltpu.make_async_copy(w_head_hbm, w_head_ref, mom_sem.at[0]),
                 pltpu.make_async_copy(m_head_hbm, m_head_ref, mom_sem.at[1]),
                 pltpu.make_async_copy(m_in_hbm, m_in_ref, mom_sem.at[2]),
                 pltpu.make_async_copy(m_out_hbm, m_out_ref, mom_sem.at[3]))

    small_loads = [pltpu.make_async_copy(src, dst, small_sem.at[i]) for i, (src, dst) in enumerate(
        ((x_hbm, x_ref), (label_hbm, label_ref), (rate_hbm, rate_ref), (coef_hbm, coef_ref), (x_next_hbm, x_next_ref)))]

    small_loads[0].start()
    for copy in load(0) + load(1):
        copy.start()
    for step in range(1, n_shards):
        other = (me + step) % n_shards
        pl.semaphore_signal(barrier, inc=1, device_id=(other // 2, other % 2), device_id_type=MESH)
    small_loads[0].wait()
    stream[...] = x_ref[0].astype(F32).T

    groups = [range(0, 2)] + [range(first, min(first + 3, layers)) for first in range(2, layers, 3)]
    for number, group in enumerate(groups):
        for layer in group:
            for copy in load(layer):
                copy.wait()
        if number + 1 < len(groups):
            for layer in groups[number + 1]:
                for copy in load(layer):
                    copy.start()
        else:
            for copy in small_loads[1:] + [mom_loads[0]]:
                copy.start()
        for layer in group:
            w_in[layer] = (0.5 * w_in_ref[layer]).astype(BF16)
            w_out[layer] = w_out_ref[layer].astype(BF16)
        for layer in group:
            for part in parts:
                stream_in = stream[part]
                normed, rstd = normalize(stream_in)
                x_hat[layer, part, 0:dim] = normed
                x_hat[layer, part, dim:dim + 1] = rstd
                pre_half = dot(normed.astype(BF16), w_in[layer], NN)
                pre_acts[layer, part] = pre_half
                out = (pre_half * gelu_parts(pre_half)[2]).astype(BF16)
                stream[part] = stream_in + dot(out, w_out[layer], NT)
    for copy in mom_loads[1:]:
        copy.start()

    pooled = (jnp.sum(stream[...], axis=0, keepdims=True) * (1.0 / tokens)).astype(BF16)
    for copy in small_loads[1:] + [mom_loads[0]]:
        copy.wait()
    w_head = w_head_ref[...].astype(BF16)
    pooled_rows = jnp.broadcast_to(pooled.astype(F32), (16, dim)).astype(BF16)
    logits = dot(pooled_rows, w_head, NN)
    peak = jnp.max(logits, axis=-1, keepdims=True)
    expd = jnp.exp(logits - peak)
    probs = expd / jnp.sum(expd, axis=-1, keepdims=True)
    class_ids = lax.broadcasted_iota(jnp.int32, logits.shape, 1)
    targets = jnp.where(class_ids == label_ref[...], 1.0, 0.0)
    d_logits = ((probs - targets) * (1.0 / n_shards)).astype(BF16)
    d_pooled = dot(d_logits, w_head, NT).astype(BF16).astype(F32) / tokens
    d_stream[...] = jnp.broadcast_to(d_pooled[0:1], d_stream.shape)
    head_send[...] = jnp.zeros_like(head_send)
    d_logits = d_logits.astype(F32)
    for chunk in range(8):
        wide = min(LANES, classes - chunk * LANES)
        head_send[chunk:chunk + 1, 0:wide] = d_logits[0:1, chunk * LANES:chunk * LANES + wide]
    pooled = pooled.astype(F32)
    head_send[8:9, :] = pooled[:, 0:LANES]
    head_send[9:10, 0:dim - LANES] = pooled[:, LANES:dim]
    head_recv[0] = head_send[...]

    pl.semaphore_wait(barrier, n_shards - 1)

    def head_copy(step):
        other = (me + step) % n_shards
        return pltpu.make_async_remote_copy(
            src_ref=head_send, dst_ref=head_recv.at[step], send_sem=head_send_sem.at[0],
            recv_sem=head_recv_sem.at[0], device_id=(other // 2, other % 2), device_id_type=MESH)

    for step in range(1, n_shards):
        head_copy(step).start()

    def all_head_copies():
        others = head_recv.at[pl.ds(1, n_shards - 1)]
        return pltpu.make_async_remote_copy(
            src_ref=others, dst_ref=others, send_sem=head_send_sem.at[0],
            recv_sem=head_recv_sem.at[0], device_id=peer_core, device_id_type=MESH)

    mine = half * core
    place_a, place_b = mine, mine + half // 2

    def remote(src, dst, layer, stage, device):
        near = 0 if stage in (0, 5) else 1
        return pltpu.make_async_remote_copy(
            src_ref=src, dst_ref=dst, send_sem=send_sem.at[layer, near], recv_sem=recv_sem.at[layer, stage],
            device_id=device, device_id_type=MESH)

    def copies(stage, layer):
        def grad(start, size):
            return grads.at[layer, pl.ds(start, size)]

        def total(start, size):
            return sums.at[layer, pl.ds(start, size)]

        if stage == 0:
            return [remote(grad(half * (1 - core), half), recv0.at[layer], layer, stage, peer_core)]
        if stage == 1:
            return [remote(grad(place_a + quarter * (1 - x), quarter), recv1.at[layer, 0], layer, stage, peer_x),
                    remote(grad(place_b + quarter * (1 - y), quarter), recv1.at[layer, 1], layer, stage, peer_y)]
        if stage == 2:
            return [remote(grad(place_a + quarter * x + eighth * (1 - y), eighth), recv2.at[layer, 0], layer, stage, peer_y),
                    remote(grad(place_b + quarter * y + eighth * (1 - x), eighth), recv2.at[layer, 1], layer, stage, peer_x)]
        if stage == 3:
            spot_a = total(place_a + quarter * x + eighth * y, eighth)
            spot_b = total(place_b + quarter * y + eighth * x, eighth)
            return [remote(spot_a, spot_a, layer, stage, peer_y), remote(spot_b, spot_b, layer, stage, peer_x)]
        if stage == 4:
            spot_a = total(place_a + quarter * x, quarter)
            spot_b = total(place_b + quarter * y, quarter)
            return [remote(spot_a, spot_a, layer, stage, peer_x), remote(spot_b, spot_b, layer, stage, peer_y)]
        spot = total(mine, half)
        return [remote(spot, spot, layer, stage, peer_core)]

    def add(layer, dst, start, size, other):
        dst[layer, pl.ds(start, size)] = (
            grads[layer, pl.ds(start, size)].astype(F32) + other[...].astype(F32)).astype(BF16)

    def start(stage, turn):
        for copy in copies(stage, layers - 1 - turn):
            copy.start()

    def advance(stage, turn):
        layer = layers - 1 - turn
        size = (half, 2 * quarter, 2 * eighth, 2 * eighth, 2 * quarter, half)[stage]
        spot = grads.at[layer, pl.ds(0, size)]
        remote(spot, spot, layer, stage, peer_core).wait_recv()
        if stage == 0:
            add(layer, grads, mine, half, recv0.at[layer])
        elif stage == 1:
            add(layer, grads, place_a + quarter * x, quarter, recv1.at[layer, 0])
            add(layer, grads, place_b + quarter * y, quarter, recv1.at[layer, 1])
        elif stage == 2:
            add(layer, sums, place_a + quarter * x + eighth * y, eighth, recv2.at[layer, 0])
            add(layer, sums, place_b + quarter * y + eighth * x, eighth, recv2.at[layer, 1])
        if stage < 5:
            start(stage + 1, turn)

    def run(steps):
        for step in steps:
            advance(*step)

    def run_at(index, table):
        for at, steps in enumerate(table):
            if steps:
                pl.when(index == at)(functools.partial(run, steps))

    def backward(turn, carry):
        layer = layers - 1 - turn
        for part in (slice(0, tokens),):
            branch = d_stream[part].astype(BF16)
            d_branch[part] = branch
            normed = x_hat[layer, part, 0:dim]
            acts[part] = normed.astype(BF16)
            pre_half = pre_acts[layer, part]
            square, tanh_val, twice_cdf = gelu_parts(pre_half)
            hidden[part] = (pre_half * twice_cdf).astype(BF16)
            slope = twice_cdf + ((1.0 - tanh_val * tanh_val) * pre_half) * (
                2.0 * GELU_SCALE + (24.0 * GELU_SCALE * GELU_CUBIC) * square)
            d_hidden = dot(branch, w_out[layer], NN).astype(BF16).astype(F32)
            d_pre_part = (d_hidden * slope).astype(BF16)
            d_pre[part] = d_pre_part
            d_act = dot(d_pre_part, w_in[layer], NT).astype(BF16).astype(F32)
            mean_d = jnp.mean(d_act, axis=-1, keepdims=True)
            mean_dx = jnp.mean(d_act * normed, axis=-1, keepdims=True)
            d_stream[part] = d_stream[part] + x_hat[layer, part, dim:dim + 1] * (d_act - mean_d - normed * mean_dx)
        g_in = (0.5 * dot(acts[...], d_pre[...], TN)).astype(BF16)
        g_out = dot(d_branch[...], hidden[...], TN).astype(BF16)
        for chunk in range(chunks):
            grads[layer, chunk * dim:(chunk + 1) * dim] = g_in[:, chunk * LANES:(chunk + 1) * LANES]
            grads[layer, half + chunk * dim:half + (chunk + 1) * dim] = g_out[:, chunk * LANES:(chunk + 1) * LANES]
        start(0, turn)
        run_at(turn, AFTER_BACKWARD)
        return carry

    lax.fori_loop(0, layers, backward, 0)
    last = layers - 1
    run(BEFORE_HEAD)

    rate, coef = rate_ref[...], coef_ref[...]
    all_head_copies().wait_recv()
    for copy in mom_loads[1:]:
        copy.wait()
    columns = []
    for device in range(n_shards):
        turned = head_recv[device, 8:16, :].T
        columns.append(jnp.concatenate([turned[:, 0:1], turned[0:dim - LANES, 1:2]], axis=0))
    for chunk in range(8):
        wide = min(LANES, classes - chunk * LANES)
        lanes = slice(chunk * LANES, chunk * LANES + wide)
        total_head = None
        for device in range(n_shards):
            product = columns[device] * head_recv[device, chunk:chunk + 1, 0:wide]
            product = product.astype(BF16).astype(F32)
            total_head = product if total_head is None else total_head + product
        moment = coef * m_head_ref[:, lanes] + total_head
        m_head_ref[:, lanes] = moment
        w_head_ref[:, lanes] = w_head_ref[:, lanes] - rate * moment
    stream[...] = x_next_ref[0].astype(F32).T

    run(AFTER_HEAD)

    def next_forward(layer, carry):
        run_at(layer, BEFORE_UPDATE)
        update(layer, layer, rate, coef, sums, (w_in_ref, m_in_ref, w_out_ref, m_out_ref), (w_in_ref, m_in_ref, w_out_ref, m_out_ref),
               w_in.at[layer], w_out.at[layer])
        run_at(layer, AFTER_UPDATE)
        next_block(stream, w_in.at[layer], w_out.at[layer])
        return carry

    lax.fori_loop(0, layers - LATE, next_forward, 0)
    run(AT_END)

    def finish_all(layer, carry):
        for stage, size in ((0, 2 * half), (1, 3 * half // 2)):
            spot = grads.at[layer, pl.ds(0, size)]
            remote(spot, spot, layer, stage, peer_core).wait_send()
        return carry

    lax.fori_loop(0, layers, finish_all, 0)
    all_head_copies().wait_send()


def store_kernel(rate_ref, coef_ref, w_in_ref, w_out_ref, w_head_ref, m_in_ref, m_out_ref, m_head_ref, sums, stream_ref,
                 w_in_out, w_out_out, w_head_out, m_in_out, m_out_out, m_head_out, logits_out,
                 stream, w_in_late, m_in_late, w_out_late, m_out_late, w_in, w_out, logits, early_sem, late_sem):
    layers = w_in_ref.shape[0]
    tokens, dim = stream.shape
    early = layers - LATE
    rate, coef = rate_ref[...], coef_ref[...]
    old = (w_in_ref, m_in_ref, w_out_ref, m_out_ref)
    new = (w_in_late, m_in_late, w_out_late, m_out_late)
    outs = (w_in_out, m_in_out, w_out_out, m_out_out)
    copies = [pltpu.make_async_copy(src.at[layer], dst.at[layer], early_sem.at[3 + 4 * layer + i])
              for layer in range(early) for i, (src, dst) in enumerate(zip(old, outs))]
    copies.append(pltpu.make_async_copy(w_head_ref, w_head_out, early_sem.at[0]))
    copies.append(pltpu.make_async_copy(m_head_ref, m_head_out, early_sem.at[1]))
    for copy in copies:
        copy.start()
    stream[...] = stream_ref[...]

    def late_copies(step):
        return [pltpu.make_async_copy(src.at[step], dst.at[early + step], late_sem.at[step, i])
                for i, (src, dst) in enumerate(zip(new, outs))]

    def late_layer(step, carry):
        update(early + step, step, rate, coef, sums, old, new, w_in, w_out)
        for copy in late_copies(step):
            copy.start()
        next_block(stream, w_in, w_out)
        return carry

    lax.fori_loop(0, LATE, late_layer, 0)
    pooled = jnp.sum(stream[...], axis=0, keepdims=True) * (1.0 / tokens)
    pooled = jnp.broadcast_to(pooled, (16, dim)).astype(BF16)
    logits[...] = dot(pooled, w_head_ref[...].astype(BF16), NN)[0:1]
    copies.append(pltpu.make_async_copy(logits, logits_out, early_sem.at[2]))
    copies[-1].start()
    for step in range(LATE):
        copies += late_copies(step)
    for copy in copies:
        copy.wait()


def solution(mesh):
    batch_spec = P(BATCH_AXES)
    repl_spec = P()
    n_shards = mesh.shape["inner"] * mesh.shape["data"]

    def device_step(x_t, labels_t, x_next, w_in, w_out, w_head, mom_in, mom_out, mom_head, learn_rate, mom_coef):
        layers, dim, mlp_dim = w_in.shape
        tokens = x_t.shape[1]
        classes = w_head.shape[1]
        half = mlp_dim // LANES * dim
        vmem = pl.BlockSpec(memory_space=pltpu.VMEM)
        hbm = pl.BlockSpec(memory_space=pl.ANY)
        shapes = [(layers, dim, mlp_dim), (layers, dim, mlp_dim), (dim, classes)] * 2
        rate, coef = learn_rate.reshape(1, 1), mom_coef.reshape(1, 1)
        results = pl.pallas_call(
            functools.partial(step_kernel, n_shards),
            out_shape=tuple(pltpu.VMEM(shape, F32) for shape in shapes) + (pltpu.VMEM((layers, 2 * half, LANES), BF16), pltpu.VMEM((tokens, dim), F32)),
            in_specs=[hbm] * 11,
            out_specs=(vmem,) * 8,
            scratch_shapes=[
                pltpu.VMEM((tokens, dim), F32),
                pltpu.VMEM((layers, tokens, dim + 1), F32),
                pltpu.VMEM((tokens, dim), BF16),
                pltpu.VMEM((layers, tokens, mlp_dim), F32),
                pltpu.VMEM((tokens, mlp_dim), BF16),
                pltpu.VMEM((tokens, dim), BF16),
                pltpu.VMEM((tokens, mlp_dim), BF16),
                pltpu.VMEM((layers, dim, mlp_dim), BF16),
                pltpu.VMEM((layers, dim, mlp_dim), BF16),
                pltpu.VMEM((layers, 2 * half, LANES), BF16),
                pltpu.VMEM((layers, half, LANES), BF16),
                pltpu.VMEM((layers, 2, half // 4, LANES), BF16),
                pltpu.VMEM((layers, 2, half // 8, LANES), BF16),
                pltpu.VMEM((16, LANES), F32),
                pltpu.VMEM((n_shards, 16, LANES), F32),
                pltpu.VMEM((1, dim, tokens), BF16),
                pltpu.VMEM((1, dim, tokens), BF16),
                pltpu.VMEM((1, 1), jnp.int32),
                pltpu.VMEM((1, 1), F32),
                pltpu.VMEM((1, 1), F32),
                pltpu.SemaphoreType.DMA((4, 2)),
                pltpu.SemaphoreType.DMA((4,)),
                pltpu.SemaphoreType.DMA((5,)),
                pltpu.SemaphoreType.DMA((layers, 2)),
                pltpu.SemaphoreType.DMA((layers, 6)),
                pltpu.SemaphoreType.DMA((1,)),
                pltpu.SemaphoreType.DMA((1,)),
            ],
            compiler_params=pltpu.CompilerParams(collective_id=0, has_side_effects=True, vmem_limit_bytes=VMEM_BYTES),
            name="step_kernel",
        )(x_t.transpose(0, 2, 1), x_next.transpose(0, 2, 1), labels_t.reshape(1, 1), rate, coef,
          w_in, w_out.transpose(0, 2, 1), w_head, mom_in, mom_out.transpose(0, 2, 1), mom_head)
        late = pltpu.VMEM((LATE, dim, mlp_dim), F32)
        w_in_new, w_out_new, w_head_new, m_in_new, m_out_new, m_head_new, logits = pl.pallas_call(
            store_kernel,
            out_shape=tuple(jax.ShapeDtypeStruct(shape, F32) for shape in shapes + [(1, classes)]),
            in_specs=[vmem] * 10,
            out_specs=(hbm,) * 7,
            scratch_shapes=[
                pltpu.VMEM((tokens, dim), F32), late, late, late, late,
                pltpu.VMEM((dim, mlp_dim), BF16), pltpu.VMEM((dim, mlp_dim), BF16), pltpu.VMEM((1, classes), F32),
                pltpu.SemaphoreType.DMA((3 + 4 * (layers - LATE),)), pltpu.SemaphoreType.DMA((LATE, 4)),
            ],
            compiler_params=pltpu.CompilerParams(vmem_limit_bytes=11 * 1000 * 1000),
            name="store_kernel",
        )(rate, coef, *results)
        return (logits, w_in_new, w_out_new.transpose(0, 2, 1), w_head_new,
                m_in_new, m_out_new.transpose(0, 2, 1), m_head_new)

    return jax.shard_map(device_step, mesh=mesh, in_specs=(batch_spec, batch_spec, batch_spec) + (repl_spec,) * 8, out_specs=(batch_spec,) + (repl_spec,) * 6, check_vma=False)
```

```python
import functools

import jax
import jax.numpy as jnp
from jax import lax
from jax.experimental import pallas as pl
from jax.experimental.pallas import tpu as pltpu
from jax.sharding import PartitionSpec as P

LN_EPS = 1e-6
BATCH_AXES = ("inner", "data")
MESH = pl.DeviceIdType.MESH
LANES = 128
GELU_SCALE = 0.7978845608028654
GELU_CUBIC = 0.044715
F32 = jnp.float32
BF16 = jnp.bfloat16
NT = (((1,), (1,)), ((), ()))
NN = (((1,), (0,)), ((), ()))
TN = (((0,), (0,)), ((), ()))
VMEM_BYTES = 40600 * 1000
ROWS = 192
LATE = 2


def dot(a, b, dims):
    return lax.dot_general(a, b, dims, preferred_element_type=F32)


def normalize(stream):
    mean_val = jnp.mean(stream, axis=-1, keepdims=True)
    centered = stream - mean_val
    variance = jnp.mean(centered * centered, axis=-1, keepdims=True)
    rstd = lax.rsqrt(variance + LN_EPS)
    return centered * rstd, rstd


def gelu_parts(pre_half):
    square = pre_half * pre_half
    tanh_val = jnp.tanh(pre_half * (2.0 * GELU_SCALE + (8.0 * GELU_SCALE * GELU_CUBIC) * square))
    return square, tanh_val, 1.0 + tanh_val


AFTER_BACKWARD = [[], [(0, 0)], [(0, 1)], [(0, 2), (1, 0)], [(1, 1), (0, 3)], [(0, 4)], [(0, 5), (1, 3), (0, 6)], []]
BEFORE_HEAD = [(1, 2), (0, 7), (1, 5)]
AFTER_HEAD = [(1, 6), (1, 4), (2, 3), (1, 7), (2, 5), (2, 6), (2, 0), (2, 1), (2, 7), (2, 2), (2, 4), (3, 6), (3, 7), (3, 5), (3, 2), (4, 7), (4, 6), (3, 4), (5, 7)]
BEFORE_UPDATE = [[], [(3, 0), (3, 1), (4, 5)], [(4, 4), (5, 5)], [(4, 3), (5, 4)], [(5, 3), (4, 0)], [(5, 2)]]
AFTER_UPDATE = [[(5, 6), (3, 3)], [], [(4, 2)], [], [], [(5, 0), (4, 1)]]
AT_END = [(5, 1)]


def update(layer, slot, rate, coef, sums, old, new, w_in, w_out):
    dim, mlp_dim = w_in.shape
    half = mlp_dim // LANES * dim
    for start in range(0, mlp_dim, LANES):
        lanes = slice(start, start + LANES)
        for base, w_old, m_old, w_new, m_new, w_bf, scale in (
                (0, old[0], old[1], new[0], new[1], w_in, 0.5), (half, old[2], old[3], new[2], new[3], w_out, 1.0)):
            row = base + start // LANES * dim
            moment = coef * m_old[layer, :, lanes] + sums[layer, row:row + dim].astype(F32)
            m_new[slot, :, lanes] = moment
            weight = w_old[layer, :, lanes] - rate * moment
            w_new[slot, :, lanes] = weight
            w_bf[:, lanes] = (weight * scale).astype(BF16)


def next_block(stream, w_in, w_out):
    for start in range(0, stream.shape[0], ROWS):
        part = slice(start, start + ROWS)
        stream_in = stream[part]
        pre_half = dot(normalize(stream_in)[0].astype(BF16), w_in[...], NN)
        out = (pre_half * gelu_parts(pre_half)[2]).astype(BF16)
        stream[part] = stream_in + dot(out, w_out[...], NT)


def step_kernel(n_shards,
                x_hbm, x_next_hbm, label_hbm, rate_hbm, coef_hbm, w_in_hbm, w_out_hbm, w_head_hbm, m_in_hbm, m_out_hbm, m_head_hbm,
                w_in_ref, w_out_ref, w_head_ref, m_in_ref, m_out_ref, m_head_ref, sums, stream,
                d_stream, x_hat, acts, pre_acts, hidden, d_branch, d_pre, w_in, w_out,
                grads, recv0, recv1, recv2, head_send, head_recv,
                x_ref, x_next_ref, label_ref, rate_ref, coef_ref,
                load_sem, mom_sem, small_sem, send_sem, recv_sem, head_send_sem, head_recv_sem):
    layers, tokens, mlp_dim = pre_acts.shape
    dim = stream.shape[1]
    classes = w_head_ref.shape[1]
    chunks = mlp_dim // LANES
    half = chunks * dim
    quarter, eighth = half // 4, half // 8
    parts = [slice(start, start + tokens // 2) for start in (0, tokens // 2)]
    inner, core = lax.axis_index("inner"), lax.axis_index("data")
    y, x = inner // 2, inner % 2
    peer_core = (inner, 1 - core)
    peer_x = (inner + 1 - 2 * x, core)
    peer_y = (inner + 2 - 4 * y, core)
    barrier = pltpu.get_barrier_semaphore()
    me = inner * 2 + core

    def load(layer):
        return (pltpu.make_async_copy(w_in_hbm.at[layer], w_in_ref.at[layer], load_sem.at[layer % 4, 0]),
                pltpu.make_async_copy(w_out_hbm.at[layer], w_out_ref.at[layer], load_sem.at[layer % 4, 1]))

    mom_loads = (pltpu.make_async_copy(w_head_hbm, w_head_ref, mom_sem.at[0]),
                 pltpu.make_async_copy(m_head_hbm, m_head_ref, mom_sem.at[1]),
                 pltpu.make_async_copy(m_in_hbm, m_in_ref, mom_sem.at[2]),
                 pltpu.make_async_copy(m_out_hbm, m_out_ref, mom_sem.at[3]))

    small_loads = [pltpu.make_async_copy(src, dst, small_sem.at[i]) for i, (src, dst) in enumerate(
        ((x_hbm, x_ref), (label_hbm, label_ref), (rate_hbm, rate_ref), (coef_hbm, coef_ref), (x_next_hbm, x_next_ref)))]

    small_loads[0].start()
    for copy in load(0) + load(1):
        copy.start()
    for step in range(1, n_shards):
        other = (me + step) % n_shards
        pl.semaphore_signal(barrier, inc=1, device_id=(other // 2, other % 2), device_id_type=MESH)
    small_loads[0].wait()
    stream[...] = x_ref[0].astype(F32).T

    def forward(pair, carry):
        first = 2 * pair
        for copy in load(first) + load(first + 1):
            copy.wait()

        @pl.when(first + 2 < layers)
        def _():
            for copy in load(first + 2) + load(first + 3):
                copy.start()

        @pl.when(first + 2 >= layers)
        def _():
            for copy in small_loads[1:] + [mom_loads[0]]:
                copy.start()

        for layer in (first, first + 1):
            w_in[layer] = (0.5 * w_in_ref[layer]).astype(BF16)
            w_out[layer] = w_out_ref[layer].astype(BF16)
        for layer in (first, first + 1):
            for part in parts:
                stream_in = stream[part]
                normed, rstd = normalize(stream_in)
                x_hat[layer, part, 0:dim] = normed
                x_hat[layer, part, dim:dim + 1] = rstd
                pre_half = dot(normed.astype(BF16), w_in[layer], NN)
                pre_acts[layer, part] = pre_half
                out = (pre_half * gelu_parts(pre_half)[2]).astype(BF16)
                stream[part] = stream_in + dot(out, w_out[layer], NT)
        return carry

    lax.fori_loop(0, layers // 2, forward, 0)
    for copy in mom_loads[1:]:
        copy.start()

    pooled = (jnp.sum(stream[...], axis=0, keepdims=True) * (1.0 / tokens)).astype(BF16)
    for copy in small_loads[1:] + [mom_loads[0]]:
        copy.wait()
    w_head = w_head_ref[...].astype(BF16)
    pooled_rows = jnp.broadcast_to(pooled.astype(F32), (16, dim)).astype(BF16)
    logits = dot(pooled_rows, w_head, NN)
    peak = jnp.max(logits, axis=-1, keepdims=True)
    expd = jnp.exp(logits - peak)
    probs = expd / jnp.sum(expd, axis=-1, keepdims=True)
    class_ids = lax.broadcasted_iota(jnp.int32, logits.shape, 1)
    targets = jnp.where(class_ids == label_ref[...], 1.0, 0.0)
    d_logits = ((probs - targets) * (1.0 / n_shards)).astype(BF16)
    d_pooled = dot(d_logits, w_head, NT).astype(BF16).astype(F32) / tokens
    d_stream[...] = jnp.broadcast_to(d_pooled[0:1], d_stream.shape)
    head_send[...] = jnp.zeros_like(head_send)
    d_logits = d_logits.astype(F32)
    for chunk in range(8):
        wide = min(LANES, classes - chunk * LANES)
        head_send[chunk:chunk + 1, 0:wide] = d_logits[0:1, chunk * LANES:chunk * LANES + wide]
    pooled = pooled.astype(F32)
    head_send[8:9, :] = pooled[:, 0:LANES]
    head_send[9:10, 0:dim - LANES] = pooled[:, LANES:dim]
    head_recv[0] = head_send[...]

    pl.semaphore_wait(barrier, n_shards - 1)

    def head_copy(step):
        other = (me + step) % n_shards
        return pltpu.make_async_remote_copy(
            src_ref=head_send, dst_ref=head_recv.at[step], send_sem=head_send_sem.at[0],
            recv_sem=head_recv_sem.at[0], device_id=(other // 2, other % 2), device_id_type=MESH)

    for step in range(1, n_shards):
        head_copy(step).start()

    def all_head_copies():
        others = head_recv.at[pl.ds(1, n_shards - 1)]
        return pltpu.make_async_remote_copy(
            src_ref=others, dst_ref=others, send_sem=head_send_sem.at[0],
            recv_sem=head_recv_sem.at[0], device_id=peer_core, device_id_type=MESH)

    mine = half * core
    place_a, place_b = mine, mine + half // 2

    def remote(src, dst, layer, stage, device):
        near = 0 if stage in (0, 5) else 1
        return pltpu.make_async_remote_copy(
            src_ref=src, dst_ref=dst, send_sem=send_sem.at[layer, near], recv_sem=recv_sem.at[layer, stage],
            device_id=device, device_id_type=MESH)

    def copies(stage, layer):
        def grad(start, size):
            return grads.at[layer, pl.ds(start, size)]

        def total(start, size):
            return sums.at[layer, pl.ds(start, size)]

        if stage == 0:
            return [remote(grad(half * (1 - core), half), recv0.at[layer], layer, stage, peer_core)]
        if stage == 1:
            return [remote(grad(place_a + quarter * (1 - x), quarter), recv1.at[layer, 0], layer, stage, peer_x),
                    remote(grad(place_b + quarter * (1 - y), quarter), recv1.at[layer, 1], layer, stage, peer_y)]
        if stage == 2:
            return [remote(grad(place_a + quarter * x + eighth * (1 - y), eighth), recv2.at[layer, 0], layer, stage, peer_y),
                    remote(grad(place_b + quarter * y + eighth * (1 - x), eighth), recv2.at[layer, 1], layer, stage, peer_x)]
        if stage == 3:
            spot_a = total(place_a + quarter * x + eighth * y, eighth)
            spot_b = total(place_b + quarter * y + eighth * x, eighth)
            return [remote(spot_a, spot_a, layer, stage, peer_y), remote(spot_b, spot_b, layer, stage, peer_x)]
        if stage == 4:
            spot_a = total(place_a + quarter * x, quarter)
            spot_b = total(place_b + quarter * y, quarter)
            return [remote(spot_a, spot_a, layer, stage, peer_x), remote(spot_b, spot_b, layer, stage, peer_y)]
        spot = total(mine, half)
        return [remote(spot, spot, layer, stage, peer_core)]

    def add(layer, dst, start, size, other):
        dst[layer, pl.ds(start, size)] = (
            grads[layer, pl.ds(start, size)].astype(F32) + other[...].astype(F32)).astype(BF16)

    def start(stage, turn):
        for copy in copies(stage, layers - 1 - turn):
            copy.start()

    def advance(stage, turn):
        layer = layers - 1 - turn
        size = (half, 2 * quarter, 2 * eighth, 2 * eighth, 2 * quarter, half)[stage]
        spot = grads.at[layer, pl.ds(0, size)]
        remote(spot, spot, layer, stage, peer_core).wait_recv()
        if stage == 0:
            add(layer, grads, mine, half, recv0.at[layer])
        elif stage == 1:
            add(layer, grads, place_a + quarter * x, quarter, recv1.at[layer, 0])
            add(layer, grads, place_b + quarter * y, quarter, recv1.at[layer, 1])
        elif stage == 2:
            add(layer, sums, place_a + quarter * x + eighth * y, eighth, recv2.at[layer, 0])
            add(layer, sums, place_b + quarter * y + eighth * x, eighth, recv2.at[layer, 1])
        if stage < 5:
            start(stage + 1, turn)

    def run(steps):
        for step in steps:
            advance(*step)

    def run_at(index, table):
        for at, steps in enumerate(table):
            if steps:
                pl.when(index == at)(functools.partial(run, steps))

    def backward(turn, carry):
        layer = layers - 1 - turn
        for part in (slice(0, tokens),):
            branch = d_stream[part].astype(BF16)
            d_branch[part] = branch
            normed = x_hat[layer, part, 0:dim]
            acts[part] = normed.astype(BF16)
            pre_half = pre_acts[layer, part]
            square, tanh_val, twice_cdf = gelu_parts(pre_half)
            hidden[part] = (pre_half * twice_cdf).astype(BF16)
            slope = twice_cdf + ((1.0 - tanh_val * tanh_val) * pre_half) * (
                2.0 * GELU_SCALE + (24.0 * GELU_SCALE * GELU_CUBIC) * square)
            d_hidden = dot(branch, w_out[layer], NN).astype(BF16).astype(F32)
            d_pre_part = (d_hidden * slope).astype(BF16)
            d_pre[part] = d_pre_part
            d_act = dot(d_pre_part, w_in[layer], NT).astype(BF16).astype(F32)
            mean_d = jnp.mean(d_act, axis=-1, keepdims=True)
            mean_dx = jnp.mean(d_act * normed, axis=-1, keepdims=True)
            d_stream[part] = d_stream[part] + x_hat[layer, part, dim:dim + 1] * (d_act - mean_d - normed * mean_dx)
        g_in = (0.5 * dot(acts[...], d_pre[...], TN)).astype(BF16)
        g_out = dot(d_branch[...], hidden[...], TN).astype(BF16)
        for chunk in range(chunks):
            grads[layer, chunk * dim:(chunk + 1) * dim] = g_in[:, chunk * LANES:(chunk + 1) * LANES]
            grads[layer, half + chunk * dim:half + (chunk + 1) * dim] = g_out[:, chunk * LANES:(chunk + 1) * LANES]
        start(0, turn)
        run_at(turn, AFTER_BACKWARD)
        return carry

    lax.fori_loop(0, layers, backward, 0)
    last = layers - 1
    run(BEFORE_HEAD)

    rate, coef = rate_ref[...], coef_ref[...]
    all_head_copies().wait_recv()
    for copy in mom_loads[1:]:
        copy.wait()
    columns = []
    for device in range(n_shards):
        turned = head_recv[device, 8:16, :].T
        columns.append(jnp.concatenate([turned[:, 0:1], turned[0:dim - LANES, 1:2]], axis=0))
    for chunk in range(8):
        wide = min(LANES, classes - chunk * LANES)
        lanes = slice(chunk * LANES, chunk * LANES + wide)
        total_head = None
        for device in range(n_shards):
            product = columns[device] * head_recv[device, chunk:chunk + 1, 0:wide]
            product = product.astype(BF16).astype(F32)
            total_head = product if total_head is None else total_head + product
        moment = coef * m_head_ref[:, lanes] + total_head
        m_head_ref[:, lanes] = moment
        w_head_ref[:, lanes] = w_head_ref[:, lanes] - rate * moment
    stream[...] = x_next_ref[0].astype(F32).T

    run(AFTER_HEAD)

    def next_forward(layer, carry):
        run_at(layer, BEFORE_UPDATE)
        update(layer, layer, rate, coef, sums, (w_in_ref, m_in_ref, w_out_ref, m_out_ref), (w_in_ref, m_in_ref, w_out_ref, m_out_ref),
               w_in.at[layer], w_out.at[layer])
        run_at(layer, AFTER_UPDATE)
        next_block(stream, w_in.at[layer], w_out.at[layer])
        return carry

    lax.fori_loop(0, layers - LATE, next_forward, 0)
    run(AT_END)

    def finish_all(layer, carry):
        for stage, size in ((0, 2 * half), (1, 3 * half // 2)):
            spot = grads.at[layer, pl.ds(0, size)]
            remote(spot, spot, layer, stage, peer_core).wait_send()
        return carry

    lax.fori_loop(0, layers, finish_all, 0)
    all_head_copies().wait_send()


def store_kernel(rate_ref, coef_ref, w_in_ref, w_out_ref, w_head_ref, m_in_ref, m_out_ref, m_head_ref, sums, stream_ref,
                 w_in_out, w_out_out, w_head_out, m_in_out, m_out_out, m_head_out, logits_out,
                 stream, w_in_late, m_in_late, w_out_late, m_out_late, w_in, w_out, logits, early_sem, late_sem):
    layers = w_in_ref.shape[0]
    tokens, dim = stream.shape
    early = layers - LATE
    rate, coef = rate_ref[...], coef_ref[...]
    old = (w_in_ref, m_in_ref, w_out_ref, m_out_ref)
    new = (w_in_late, m_in_late, w_out_late, m_out_late)
    outs = (w_in_out, m_in_out, w_out_out, m_out_out)
    copies = [pltpu.make_async_copy(src.at[pl.ds(0, early)], dst.at[pl.ds(0, early)], early_sem.at[i])
              for i, (src, dst) in enumerate(zip(old, outs))]
    copies.append(pltpu.make_async_copy(w_head_ref, w_head_out, early_sem.at[4]))
    copies.append(pltpu.make_async_copy(m_head_ref, m_head_out, early_sem.at[5]))
    for copy in copies:
        copy.start()
    stream[...] = stream_ref[...]

    def late_copies(step):
        return [pltpu.make_async_copy(src.at[step], dst.at[early + step], late_sem.at[step, i])
                for i, (src, dst) in enumerate(zip(new, outs))]

    def late_layer(step, carry):
        update(early + step, step, rate, coef, sums, old, new, w_in, w_out)
        for copy in late_copies(step):
            copy.start()
        next_block(stream, w_in, w_out)
        return carry

    lax.fori_loop(0, LATE, late_layer, 0)
    pooled = jnp.sum(stream[...], axis=0, keepdims=True) * (1.0 / tokens)
    pooled = jnp.broadcast_to(pooled, (16, dim)).astype(BF16)
    logits[...] = dot(pooled, w_head_ref[...].astype(BF16), NN)[0:1]
    copies.append(pltpu.make_async_copy(logits, logits_out, early_sem.at[6]))
    copies[-1].start()
    for step in range(LATE):
        copies += late_copies(step)
    for copy in copies:
        copy.wait()


def solution(mesh):
    batch_spec = P(BATCH_AXES)
    repl_spec = P()
    n_shards = mesh.shape["inner"] * mesh.shape["data"]

    def device_step(x_t, labels_t, x_next, w_in, w_out, w_head, mom_in, mom_out, mom_head, learn_rate, mom_coef):
        layers, dim, mlp_dim = w_in.shape
        tokens = x_t.shape[1]
        classes = w_head.shape[1]
        half = mlp_dim // LANES * dim
        vmem = pl.BlockSpec(memory_space=pltpu.VMEM)
        hbm = pl.BlockSpec(memory_space=pl.ANY)
        shapes = [(layers, dim, mlp_dim), (layers, dim, mlp_dim), (dim, classes)] * 2
        rate, coef = learn_rate.reshape(1, 1), mom_coef.reshape(1, 1)
        results = pl.pallas_call(
            functools.partial(step_kernel, n_shards),
            out_shape=tuple(pltpu.VMEM(shape, F32) for shape in shapes) + (pltpu.VMEM((layers, 2 * half, LANES), BF16), pltpu.VMEM((tokens, dim), F32)),
            in_specs=[hbm] * 11,
            out_specs=(vmem,) * 8,
            scratch_shapes=[
                pltpu.VMEM((tokens, dim), F32),
                pltpu.VMEM((layers, tokens, dim + 1), F32),
                pltpu.VMEM((tokens, dim), BF16),
                pltpu.VMEM((layers, tokens, mlp_dim), F32),
                pltpu.VMEM((tokens, mlp_dim), BF16),
                pltpu.VMEM((tokens, dim), BF16),
                pltpu.VMEM((tokens, mlp_dim), BF16),
                pltpu.VMEM((layers, dim, mlp_dim), BF16),
                pltpu.VMEM((layers, dim, mlp_dim), BF16),
                pltpu.VMEM((layers, 2 * half, LANES), BF16),
                pltpu.VMEM((layers, half, LANES), BF16),
                pltpu.VMEM((layers, 2, half // 4, LANES), BF16),
                pltpu.VMEM((layers, 2, half // 8, LANES), BF16),
                pltpu.VMEM((16, LANES), F32),
                pltpu.VMEM((n_shards, 16, LANES), F32),
                pltpu.VMEM((1, dim, tokens), BF16),
                pltpu.VMEM((1, dim, tokens), BF16),
                pltpu.VMEM((1, 1), jnp.int32),
                pltpu.VMEM((1, 1), F32),
                pltpu.VMEM((1, 1), F32),
                pltpu.SemaphoreType.DMA((4, 2)),
                pltpu.SemaphoreType.DMA((4,)),
                pltpu.SemaphoreType.DMA((5,)),
                pltpu.SemaphoreType.DMA((layers, 2)),
                pltpu.SemaphoreType.DMA((layers, 6)),
                pltpu.SemaphoreType.DMA((1,)),
                pltpu.SemaphoreType.DMA((1,)),
            ],
            compiler_params=pltpu.CompilerParams(collective_id=0, has_side_effects=True, vmem_limit_bytes=VMEM_BYTES),
            name="step_kernel",
        )(x_t.transpose(0, 2, 1), x_next.transpose(0, 2, 1), labels_t.reshape(1, 1), rate, coef,
          w_in, w_out.transpose(0, 2, 1), w_head, mom_in, mom_out.transpose(0, 2, 1), mom_head)
        late = pltpu.VMEM((LATE, dim, mlp_dim), F32)
        w_in_new, w_out_new, w_head_new, m_in_new, m_out_new, m_head_new, logits = pl.pallas_call(
            store_kernel,
            out_shape=tuple(jax.ShapeDtypeStruct(shape, F32) for shape in shapes + [(1, classes)]),
            in_specs=[vmem] * 10,
            out_specs=(hbm,) * 7,
            scratch_shapes=[
                pltpu.VMEM((tokens, dim), F32), late, late, late, late,
                pltpu.VMEM((dim, mlp_dim), BF16), pltpu.VMEM((dim, mlp_dim), BF16), pltpu.VMEM((1, classes), F32),
                pltpu.SemaphoreType.DMA((7,)), pltpu.SemaphoreType.DMA((LATE, 4)),
            ],
            compiler_params=pltpu.CompilerParams(vmem_limit_bytes=11 * 1000 * 1000),
            name="store_kernel",
        )(rate, coef, *results)
        return (logits, w_in_new, w_out_new.transpose(0, 2, 1), w_head_new,
                m_in_new, m_out_new.transpose(0, 2, 1), m_head_new)

    return jax.shard_map(device_step, mesh=mesh, in_specs=(batch_spec, batch_spec, batch_spec) + (repl_spec,) * 8, out_specs=(batch_spec,) + (repl_spec,) * 6, check_vma=False)
```

```python
import functools

import jax
import jax.numpy as jnp
from jax import lax
from jax.experimental import pallas as pl
from jax.experimental.pallas import tpu as pltpu
from jax.sharding import PartitionSpec as P

LN_EPS = 1e-6
BATCH_AXES = ("inner", "data")
MESH = pl.DeviceIdType.MESH
LANES = 128
GELU_SCALE = 0.7978845608028654
GELU_CUBIC = 0.044715
F32 = jnp.float32
BF16 = jnp.bfloat16
NT = (((1,), (1,)), ((), ()))
NN = (((1,), (0,)), ((), ()))
TN = (((0,), (0,)), ((), ()))
VMEM_BYTES = 40600 * 1000
ROWS = 192
LATE = 2


def dot(a, b, dims):
    return lax.dot_general(a, b, dims, preferred_element_type=F32)


def normalize(stream):
    mean_val = jnp.mean(stream, axis=-1, keepdims=True)
    centered = stream - mean_val
    variance = jnp.mean(centered * centered, axis=-1, keepdims=True)
    rstd = lax.rsqrt(variance + LN_EPS)
    return centered * rstd, rstd


def gelu_parts(pre_half):
    square = pre_half * pre_half
    tanh_val = jnp.tanh(pre_half * (2.0 * GELU_SCALE + (8.0 * GELU_SCALE * GELU_CUBIC) * square))
    return square, tanh_val, 1.0 + tanh_val


AFTER_BACKWARD = [[], [(0, 0)], [(0, 1)], [(0, 2), (1, 0)], [(1, 1), (0, 3)], [(0, 4)], [(0, 5), (1, 3), (0, 6)], []]
BEFORE_HEAD = [(1, 2), (0, 7), (1, 5)]
AFTER_HEAD = [(1, 6), (1, 4), (2, 3), (1, 7), (2, 5), (2, 6), (2, 0), (2, 1), (2, 7), (2, 2), (2, 4), (3, 6), (3, 7), (3, 5), (3, 2), (4, 7), (4, 6), (3, 4), (5, 7)]
BEFORE_UPDATE = [[], [(3, 0), (3, 1), (4, 5)], [(4, 4), (5, 5)], [(4, 3), (5, 4)], [(5, 3), (4, 0)], [(5, 2)]]
AFTER_UPDATE = [[(5, 6), (3, 3)], [], [(4, 2)], [], [], [(5, 0), (4, 1)]]
AT_END = [(5, 1)]


def update(layer, slot, rate, coef, sums, old, new, w_in, w_out):
    dim, mlp_dim = w_in.shape
    half = mlp_dim // LANES * dim
    for start in range(0, mlp_dim, LANES):
        lanes = slice(start, start + LANES)
        for base, w_old, m_old, w_new, m_new, w_bf, scale in (
                (0, old[0], old[1], new[0], new[1], w_in, 0.5), (half, old[2], old[3], new[2], new[3], w_out, 1.0)):
            row = base + start // LANES * dim
            moment = coef * m_old[layer, :, lanes] + sums[layer, row:row + dim].astype(F32)
            m_new[slot, :, lanes] = moment
            weight = w_old[layer, :, lanes] - rate * moment
            w_new[slot, :, lanes] = weight
            w_bf[:, lanes] = (weight * scale).astype(BF16)


def next_block(stream, w_in, w_out):
    for start in range(0, stream.shape[0], ROWS):
        part = slice(start, start + ROWS)
        stream_in = stream[part]
        pre_half = dot(normalize(stream_in)[0].astype(BF16), w_in[...], NN)
        out = (pre_half * gelu_parts(pre_half)[2]).astype(BF16)
        stream[part] = stream_in + dot(out, w_out[...], NT)


def step_kernel(n_shards,
                x_hbm, x_next_hbm, label_hbm, rate_hbm, coef_hbm, w_in_hbm, w_out_hbm, w_head_hbm, m_in_hbm, m_out_hbm, m_head_hbm,
                w_in_ref, w_out_ref, w_head_ref, m_in_ref, m_out_ref, m_head_ref, sums, stream,
                d_stream, x_hat, acts, pre_acts, hidden, d_branch, d_pre, w_in, w_out,
                grads, recv0, recv1, recv2, head_send, head_recv,
                x_ref, x_next_ref, label_ref, rate_ref, coef_ref,
                load_sem, mom_sem, small_sem, send_sem, recv_sem, head_send_sem, head_recv_sem):
    layers, tokens, mlp_dim = pre_acts.shape
    dim = stream.shape[1]
    classes = w_head_ref.shape[1]
    chunks = mlp_dim // LANES
    half = chunks * dim
    quarter, eighth = half // 4, half // 8
    parts = [slice(start, start + tokens // 2) for start in (0, tokens // 2)]
    inner, core = lax.axis_index("inner"), lax.axis_index("data")
    y, x = inner // 2, inner % 2
    peer_core = (inner, 1 - core)
    peer_x = (inner + 1 - 2 * x, core)
    peer_y = (inner + 2 - 4 * y, core)
    barrier = pltpu.get_barrier_semaphore()
    me = inner * 2 + core

    def load(layer):
        return (pltpu.make_async_copy(w_in_hbm.at[layer], w_in_ref.at[layer], load_sem.at[layer % 4, 0]),
                pltpu.make_async_copy(w_out_hbm.at[layer], w_out_ref.at[layer], load_sem.at[layer % 4, 1]))

    mom_loads = (pltpu.make_async_copy(w_head_hbm, w_head_ref, mom_sem.at[0]),
                 pltpu.make_async_copy(m_head_hbm, m_head_ref, mom_sem.at[1]),
                 pltpu.make_async_copy(m_in_hbm, m_in_ref, mom_sem.at[2]),
                 pltpu.make_async_copy(m_out_hbm, m_out_ref, mom_sem.at[3]))

    small_loads = [pltpu.make_async_copy(src, dst, small_sem.at[i]) for i, (src, dst) in enumerate(
        ((x_hbm, x_ref), (label_hbm, label_ref), (rate_hbm, rate_ref), (coef_hbm, coef_ref), (x_next_hbm, x_next_ref)))]

    small_loads[0].start()
    for copy in load(0) + load(1):
        copy.start()
    for step in range(1, n_shards):
        other = (me + step) % n_shards
        pl.semaphore_signal(barrier, inc=1, device_id=(other // 2, other % 2), device_id_type=MESH)
    small_loads[0].wait()
    stream[...] = x_ref[0].astype(F32).T

    groups = [range(0, 2)] + [range(first, min(first + 3, layers)) for first in range(2, layers, 3)]
    for number, group in enumerate(groups):
        for layer in group:
            for copy in load(layer):
                copy.wait()
        if number + 1 < len(groups):
            for layer in groups[number + 1]:
                for copy in load(layer):
                    copy.start()
        else:
            for copy in small_loads[1:] + [mom_loads[0]]:
                copy.start()
        for layer in group:
            w_in[layer] = (0.5 * w_in_ref[layer]).astype(BF16)
            w_out[layer] = w_out_ref[layer].astype(BF16)
        for layer in group:
            for part in parts:
                stream_in = stream[part]
                normed, rstd = normalize(stream_in)
                x_hat[layer, part, 0:dim] = normed
                x_hat[layer, part, dim:dim + 1] = rstd
                pre_half = dot(normed.astype(BF16), w_in[layer], NN)
                pre_acts[layer, part] = pre_half
                out = (pre_half * gelu_parts(pre_half)[2]).astype(BF16)
                stream[part] = stream_in + dot(out, w_out[layer], NT)
    for copy in mom_loads[1:]:
        copy.start()

    pooled = (jnp.sum(stream[...], axis=0, keepdims=True) * (1.0 / tokens)).astype(BF16)
    for copy in small_loads[1:] + [mom_loads[0]]:
        copy.wait()
    w_head = w_head_ref[...].astype(BF16)
    pooled_rows = jnp.broadcast_to(pooled.astype(F32), (16, dim)).astype(BF16)
    logits = dot(pooled_rows, w_head, NN)
    peak = jnp.max(logits, axis=-1, keepdims=True)
    expd = jnp.exp(logits - peak)
    probs = expd / jnp.sum(expd, axis=-1, keepdims=True)
    class_ids = lax.broadcasted_iota(jnp.int32, logits.shape, 1)
    targets = jnp.where(class_ids == label_ref[...], 1.0, 0.0)
    d_logits = ((probs - targets) * (1.0 / n_shards)).astype(BF16)
    d_pooled = dot(d_logits, w_head, NT).astype(BF16).astype(F32) / tokens
    d_stream[...] = jnp.broadcast_to(d_pooled[0:1], d_stream.shape)
    head_send[...] = jnp.zeros_like(head_send)
    d_logits = d_logits.astype(F32)
    for chunk in range(8):
        wide = min(LANES, classes - chunk * LANES)
        head_send[chunk:chunk + 1, 0:wide] = d_logits[0:1, chunk * LANES:chunk * LANES + wide]
    pooled = pooled.astype(F32)
    head_send[8:9, :] = pooled[:, 0:LANES]
    head_send[9:10, 0:dim - LANES] = pooled[:, LANES:dim]
    head_recv[0] = head_send[...]

    pl.semaphore_wait(barrier, n_shards - 1)

    def head_copy(step):
        other = (me + step) % n_shards
        return pltpu.make_async_remote_copy(
            src_ref=head_send, dst_ref=head_recv.at[step], send_sem=head_send_sem.at[0],
            recv_sem=head_recv_sem.at[0], device_id=(other // 2, other % 2), device_id_type=MESH)

    for step in range(1, n_shards):
        head_copy(step).start()

    def all_head_copies():
        others = head_recv.at[pl.ds(1, n_shards - 1)]
        return pltpu.make_async_remote_copy(
            src_ref=others, dst_ref=others, send_sem=head_send_sem.at[0],
            recv_sem=head_recv_sem.at[0], device_id=peer_core, device_id_type=MESH)

    mine = half * core
    place_a, place_b = mine, mine + half // 2

    def remote(src, dst, layer, stage, device):
        near = 0 if stage in (0, 5) else 1
        return pltpu.make_async_remote_copy(
            src_ref=src, dst_ref=dst, send_sem=send_sem.at[layer, near], recv_sem=recv_sem.at[layer, stage],
            device_id=device, device_id_type=MESH)

    def copies(stage, layer):
        def grad(start, size):
            return grads.at[layer, pl.ds(start, size)]

        def total(start, size):
            return sums.at[layer, pl.ds(start, size)]

        if stage == 0:
            return [remote(grad(half * (1 - core), half), recv0.at[layer], layer, stage, peer_core)]
        if stage == 1:
            return [remote(grad(place_a + quarter * (1 - x), quarter), recv1.at[layer, 0], layer, stage, peer_x),
                    remote(grad(place_b + quarter * (1 - y), quarter), recv1.at[layer, 1], layer, stage, peer_y)]
        if stage == 2:
            return [remote(grad(place_a + quarter * x + eighth * (1 - y), eighth), recv2.at[layer, 0], layer, stage, peer_y),
                    remote(grad(place_b + quarter * y + eighth * (1 - x), eighth), recv2.at[layer, 1], layer, stage, peer_x)]
        if stage == 3:
            spot_a = total(place_a + quarter * x + eighth * y, eighth)
            spot_b = total(place_b + quarter * y + eighth * x, eighth)
            return [remote(spot_a, spot_a, layer, stage, peer_y), remote(spot_b, spot_b, layer, stage, peer_x)]
        if stage == 4:
            spot_a = total(place_a + quarter * x, quarter)
            spot_b = total(place_b + quarter * y, quarter)
            return [remote(spot_a, spot_a, layer, stage, peer_x), remote(spot_b, spot_b, layer, stage, peer_y)]
        spot = total(mine, half)
        return [remote(spot, spot, layer, stage, peer_core)]

    def add(layer, dst, start, size, other):
        dst[layer, pl.ds(start, size)] = (
            grads[layer, pl.ds(start, size)].astype(F32) + other[...].astype(F32)).astype(BF16)

    def start(stage, turn):
        for copy in copies(stage, layers - 1 - turn):
            copy.start()

    def advance(stage, turn):
        layer = layers - 1 - turn
        size = (half, 2 * quarter, 2 * eighth, 2 * eighth, 2 * quarter, half)[stage]
        spot = grads.at[layer, pl.ds(0, size)]
        remote(spot, spot, layer, stage, peer_core).wait_recv()
        if stage == 0:
            add(layer, grads, mine, half, recv0.at[layer])
        elif stage == 1:
            add(layer, grads, place_a + quarter * x, quarter, recv1.at[layer, 0])
            add(layer, grads, place_b + quarter * y, quarter, recv1.at[layer, 1])
        elif stage == 2:
            add(layer, sums, place_a + quarter * x + eighth * y, eighth, recv2.at[layer, 0])
            add(layer, sums, place_b + quarter * y + eighth * x, eighth, recv2.at[layer, 1])
        if stage < 5:
            start(stage + 1, turn)

    def run(steps):
        for step in steps:
            advance(*step)

    def run_at(index, table):
        for at, steps in enumerate(table):
            if steps:
                pl.when(index == at)(functools.partial(run, steps))

    def backward(turn, carry):
        layer = layers - 1 - turn
        for part in (slice(0, tokens),):
            branch = d_stream[part].astype(BF16)
            d_branch[part] = branch
            normed = x_hat[layer, part, 0:dim]
            acts[part] = normed.astype(BF16)
            pre_half = pre_acts[layer, part]
            square, tanh_val, twice_cdf = gelu_parts(pre_half)
            hidden[part] = (pre_half * twice_cdf).astype(BF16)
            slope = twice_cdf + ((1.0 - tanh_val * tanh_val) * pre_half) * (
                2.0 * GELU_SCALE + (24.0 * GELU_SCALE * GELU_CUBIC) * square)
            d_hidden = dot(branch, w_out[layer], NN).astype(BF16).astype(F32)
            d_pre_part = (d_hidden * slope).astype(BF16)
            d_pre[part] = d_pre_part
            d_act = dot(d_pre_part, w_in[layer], NT).astype(BF16).astype(F32)
            mean_d = jnp.mean(d_act, axis=-1, keepdims=True)
            mean_dx = jnp.mean(d_act * normed, axis=-1, keepdims=True)
            d_stream[part] = d_stream[part] + x_hat[layer, part, dim:dim + 1] * (d_act - mean_d - normed * mean_dx)
        g_in = (0.5 * dot(acts[...], d_pre[...], TN)).astype(BF16)
        g_out = dot(d_branch[...], hidden[...], TN).astype(BF16)
        for chunk in range(chunks):
            grads[layer, chunk * dim:(chunk + 1) * dim] = g_in[:, chunk * LANES:(chunk + 1) * LANES]
            grads[layer, half + chunk * dim:half + (chunk + 1) * dim] = g_out[:, chunk * LANES:(chunk + 1) * LANES]
        start(0, turn)
        run_at(turn, AFTER_BACKWARD)
        return carry

    lax.fori_loop(0, layers, backward, 0)
    last = layers - 1
    run(BEFORE_HEAD)

    rate, coef = rate_ref[...], coef_ref[...]
    all_head_copies().wait_recv()
    for copy in mom_loads[1:]:
        copy.wait()
    columns = []
    for device in range(n_shards):
        turned = head_recv[device, 8:16, :].T
        columns.append(jnp.concatenate([turned[:, 0:1], turned[0:dim - LANES, 1:2]], axis=0))
    for chunk in range(8):
        wide = min(LANES, classes - chunk * LANES)
        lanes = slice(chunk * LANES, chunk * LANES + wide)
        total_head = None
        for device in range(n_shards):
            product = columns[device] * head_recv[device, chunk:chunk + 1, 0:wide]
            product = product.astype(BF16).astype(F32)
            total_head = product if total_head is None else total_head + product
        moment = coef * m_head_ref[:, lanes] + total_head
        m_head_ref[:, lanes] = moment
        w_head_ref[:, lanes] = w_head_ref[:, lanes] - rate * moment
    stream[...] = x_next_ref[0].astype(F32).T

    run(AFTER_HEAD)

    def next_forward(layer, carry):
        run_at(layer, BEFORE_UPDATE)
        update(layer, layer, rate, coef, sums, (w_in_ref, m_in_ref, w_out_ref, m_out_ref), (w_in_ref, m_in_ref, w_out_ref, m_out_ref),
               w_in.at[layer], w_out.at[layer])
        run_at(layer, AFTER_UPDATE)
        next_block(stream, w_in.at[layer], w_out.at[layer])
        return carry

    lax.fori_loop(0, layers - LATE, next_forward, 0)
    run(AT_END)

    def finish_all(layer, carry):
        for stage, size in ((0, 2 * half), (1, 3 * half // 2)):
            spot = grads.at[layer, pl.ds(0, size)]
            remote(spot, spot, layer, stage, peer_core).wait_send()
        return carry

    lax.fori_loop(0, layers, finish_all, 0)
    all_head_copies().wait_send()


def store_kernel(rate_ref, coef_ref, w_in_ref, w_out_ref, w_head_ref, m_in_ref, m_out_ref, m_head_ref, sums, stream_ref,
                 w_in_out, w_out_out, w_head_out, m_in_out, m_out_out, m_head_out, logits_out,
                 stream, w_in_late, m_in_late, w_out_late, m_out_late, w_in, w_out, logits, early_sem, late_sem):
    layers = w_in_ref.shape[0]
    tokens, dim = stream.shape
    early = layers - LATE
    rate, coef = rate_ref[...], coef_ref[...]
    old = (w_in_ref, m_in_ref, w_out_ref, m_out_ref)
    new = (w_in_late, m_in_late, w_out_late, m_out_late)
    outs = (w_in_out, m_in_out, w_out_out, m_out_out)
    copies = [pltpu.make_async_copy(src.at[pl.ds(0, early)], dst.at[pl.ds(0, early)], early_sem.at[i])
              for i, (src, dst) in enumerate(zip(old, outs))]
    copies.append(pltpu.make_async_copy(w_head_ref, w_head_out, early_sem.at[4]))
    copies.append(pltpu.make_async_copy(m_head_ref, m_head_out, early_sem.at[5]))
    for copy in copies:
        copy.start()
    stream[...] = stream_ref[...]

    def late_copies(step):
        return [pltpu.make_async_copy(src.at[step], dst.at[early + step], late_sem.at[step, i])
                for i, (src, dst) in enumerate(zip(new, outs))]

    def late_layer(step, carry):
        update(early + step, step, rate, coef, sums, old, new, w_in, w_out)
        for copy in late_copies(step):
            copy.start()
        next_block(stream, w_in, w_out)
        return carry

    lax.fori_loop(0, LATE, late_layer, 0)
    pooled = jnp.sum(stream[...], axis=0, keepdims=True) * (1.0 / tokens)
    pooled = jnp.broadcast_to(pooled, (16, dim)).astype(BF16)
    logits[...] = dot(pooled, w_head_ref[...].astype(BF16), NN)[0:1]
    copies.append(pltpu.make_async_copy(logits, logits_out, early_sem.at[6]))
    copies[-1].start()
    for step in range(LATE):
        copies += late_copies(step)
    for copy in copies:
        copy.wait()


def solution(mesh):
    batch_spec = P(BATCH_AXES)
    repl_spec = P()
    n_shards = mesh.shape["inner"] * mesh.shape["data"]

    def device_step(x_t, labels_t, x_next, w_in, w_out, w_head, mom_in, mom_out, mom_head, learn_rate, mom_coef):
        layers, dim, mlp_dim = w_in.shape
        tokens = x_t.shape[1]
        classes = w_head.shape[1]
        half = mlp_dim // LANES * dim
        vmem = pl.BlockSpec(memory_space=pltpu.VMEM)
        hbm = pl.BlockSpec(memory_space=pl.ANY)
        shapes = [(layers, dim, mlp_dim), (layers, dim, mlp_dim), (dim, classes)] * 2
        rate, coef = learn_rate.reshape(1, 1), mom_coef.reshape(1, 1)
        results = pl.pallas_call(
            functools.partial(step_kernel, n_shards),
            out_shape=tuple(pltpu.VMEM(shape, F32) for shape in shapes) + (pltpu.VMEM((layers, 2 * half, LANES), BF16), pltpu.VMEM((tokens, dim), F32)),
            in_specs=[hbm] * 11,
            out_specs=(vmem,) * 8,
            scratch_shapes=[
                pltpu.VMEM((tokens, dim), F32),
                pltpu.VMEM((layers, tokens, dim + 1), F32),
                pltpu.VMEM((tokens, dim), BF16),
                pltpu.VMEM((layers, tokens, mlp_dim), F32),
                pltpu.VMEM((tokens, mlp_dim), BF16),
                pltpu.VMEM((tokens, dim), BF16),
                pltpu.VMEM((tokens, mlp_dim), BF16),
                pltpu.VMEM((layers, dim, mlp_dim), BF16),
                pltpu.VMEM((layers, dim, mlp_dim), BF16),
                pltpu.VMEM((layers, 2 * half, LANES), BF16),
                pltpu.VMEM((layers, half, LANES), BF16),
                pltpu.VMEM((layers, 2, half // 4, LANES), BF16),
                pltpu.VMEM((layers, 2, half // 8, LANES), BF16),
                pltpu.VMEM((16, LANES), F32),
                pltpu.VMEM((n_shards, 16, LANES), F32),
                pltpu.VMEM((1, dim, tokens), BF16),
                pltpu.VMEM((1, dim, tokens), BF16),
                pltpu.VMEM((1, 1), jnp.int32),
                pltpu.VMEM((1, 1), F32),
                pltpu.VMEM((1, 1), F32),
                pltpu.SemaphoreType.DMA((4, 2)),
                pltpu.SemaphoreType.DMA((4,)),
                pltpu.SemaphoreType.DMA((5,)),
                pltpu.SemaphoreType.DMA((layers, 2)),
                pltpu.SemaphoreType.DMA((layers, 6)),
                pltpu.SemaphoreType.DMA((1,)),
                pltpu.SemaphoreType.DMA((1,)),
            ],
            compiler_params=pltpu.CompilerParams(collective_id=0, has_side_effects=True, vmem_limit_bytes=VMEM_BYTES),
            name="step_kernel",
        )(x_t.transpose(0, 2, 1), x_next.transpose(0, 2, 1), labels_t.reshape(1, 1), rate, coef,
          w_in, w_out.transpose(0, 2, 1), w_head, mom_in, mom_out.transpose(0, 2, 1), mom_head)
        late = pltpu.VMEM((LATE, dim, mlp_dim), F32)
        w_in_new, w_out_new, w_head_new, m_in_new, m_out_new, m_head_new, logits = pl.pallas_call(
            store_kernel,
            out_shape=tuple(jax.ShapeDtypeStruct(shape, F32) for shape in shapes + [(1, classes)]),
            in_specs=[vmem] * 10,
            out_specs=(hbm,) * 7,
            scratch_shapes=[
                pltpu.VMEM((tokens, dim), F32), late, late, late, late,
                pltpu.VMEM((dim, mlp_dim), BF16), pltpu.VMEM((dim, mlp_dim), BF16), pltpu.VMEM((1, classes), F32),
                pltpu.SemaphoreType.DMA((7,)), pltpu.SemaphoreType.DMA((LATE, 4)),
            ],
            compiler_params=pltpu.CompilerParams(vmem_limit_bytes=11 * 1000 * 1000),
            name="store_kernel",
        )(rate, coef, *results)
        return (logits, w_in_new, w_out_new.transpose(0, 2, 1), w_head_new,
                m_in_new, m_out_new.transpose(0, 2, 1), m_head_new)

    return jax.shard_map(device_step, mesh=mesh, in_specs=(batch_spec, batch_spec, batch_spec) + (repl_spec,) * 8, out_specs=(batch_spec,) + (repl_spec,) * 6, check_vma=False)
```
